128 devices in a mesh: bngroup: 8 (over z, core), rep: 16 (over x, y).
Axes of the slice: x: 4, y: 4, z: 4, core: 2. Of those that a mesh axis runs over, the one named last changes fastest.
Arguments:
- images: bfloat16 [1536, 7, 7, 2048], P(('bngroup', 'rep')), may hold values from -12 to 12
- cotangent: bfloat16 [1536, 7, 7, 2048], P(('bngroup', 'rep')), may hold values from -6 to 6
- w_reduce: bfloat16 [2048, 512], replicated, may hold values from -0.125 to 0.125
- w_spatial: bfloat16 [4608, 512], replicated, may hold values from -0.09375 to 0.09375
- w_expand: bfloat16 [2048, 512], replicated, may hold values from -0.25 to 0.25
- norm_gain: float32 [3072], replicated, may hold values from 0.25 to 1.75
- norm_shift: float32 [3072], replicated, may hold values from -3 to 3
Outputs:
- output: bfloat16 [1536, 7, 7, 2048], P(('bngroup', 'rep'))
- in_grad: bfloat16 [1536, 7, 7, 2048], P(('bngroup', 'rep'))
- weight_grads: float32 [8704, 512], P('bngroup', 'rep')
- norm_grads: float32 [2, 3072], replicated
The draws below stay inside these ranges and needn't reach their ends.
All inputs are finite; a program needn't handle non-finite values.
Results may differ from the reference program's by a relative error of at most 0.007.
Values sent between devices are 32-bit elements.
A program may use at most 192 MiB of HBM per device.

```python
import jax
import jax.numpy as jnp
from jax import lax

WIDE = 2048
MID = 512
SIDE = 7
IMG_DEV = 12
IMAGES = 1536
NORM_CH = 3072
N_BNGROUP = 8
N_REP = 16


def draw_images(key, part):
    base_key, scale_key = jax.random.split(jax.random.fold_in(key, 11))
    values = jnp.clip(jax.random.normal(base_key, (IMAGES, SIDE, SIDE, WIDE), jnp.float32), -6.0, 6.0)
    scales = jnp.exp(jax.random.uniform(scale_key, (IMAGES, 1, 1, 1), jnp.float32, -0.69, 0.69))
    return (values * scales).astype(jnp.bfloat16)


def block_scale(stream_key, shape, shards, smallest, high):
    factor_of, own = 1.0, jax.random.fold_in(stream_key, 6)
    for axis_at, shards_of in shards:
        draws = jnp.exp(jax.random.uniform(jax.random.fold_in(own, axis_at), (shards_of,), jnp.float32, smallest / len(shards), high / len(shards)))
        factor_of = factor_of * jnp.repeat(draws, shape[axis_at] // shards_of).reshape([-1 if axis == axis_at else 1 for axis in range(len(shape))])
    return factor_of


def bell_draw(stream_key, extent, scale, bound, shards=(), kind=jnp.bfloat16):
    values = jax.random.normal(stream_key, extent, jnp.float32) * scale
    if len(shards) > 0:
        values = block_scale(stream_key, extent, shards, -0.22, 0.18) * values
    return jnp.clip(values, min=-bound, max=bound).astype(kind)


def setup_inputs(seed: int = 0) -> dict:
    seeds = jax.random.split(jax.random.key(seed), 8)
    return {
        "images": draw_images(jax.random.fold_in(seeds[7], 71), 0),
        "cotangent": bell_draw(seeds[1], (IMAGES, SIDE, SIDE, WIDE), 1.0, 6.0, ((0, 128),)),
        "w_reduce": bell_draw(seeds[2], (WIDE, MID), WIDE ** -0.5, 0.125),
        "w_spatial": bell_draw(seeds[3], (9 * MID, MID), (9 * MID) ** -0.5, 0.09375),
        "w_expand": bell_draw(seeds[4], (WIDE, MID), MID ** -0.5, 0.25),
        "norm_gain": jnp.clip(1.0 + 0.15 * jax.random.normal(seeds[5], (NORM_CH,), jnp.float32), 0.25, 1.75),
        "norm_shift": bell_draw(seeds[6], (NORM_CH,), 0.5, 3.0, (), jnp.float32),
    }


EPS = 0.25

def matmul(left, right):
    return jnp.dot(left, right, preferred_element_type=jnp.float32)

def contract(left, right, left_dim, right_dim):
    return lax.dot_general(left, right, (((left_dim,), (right_dim,)), ((), ())), preferred_element_type=jnp.float32)

def slope(value):
    sigma = jax.nn.sigmoid(value)
    return sigma * (1.0 + value * (1.0 - sigma))

def normalize(pre_norm, norm_gain, norm_shift):
    centre = lax.optimization_barrier(jnp.mean(pre_norm, axis=0))
    spread = lax.optimization_barrier(jnp.mean(jnp.square(pre_norm - centre), axis=0))
    inverse = lax.rsqrt(spread + EPS)
    scaled = (pre_norm - centre) * inverse
    return (scaled, inverse, norm_gain * scaled + norm_shift)

def norm_back(upstream, scaled, inverse, norm_gain):
    shift_sum = lax.optimization_barrier(jnp.sum(upstream, axis=0))
    gain_sum = lax.optimization_barrier(jnp.sum(upstream * scaled, axis=0))
    number = upstream.shape[0]
    result = norm_gain * inverse * (upstream - shift_sum / number - scaled * gain_sum / number)
    return (result.astype(jnp.bfloat16), shift_sum, gain_sum)

def unfold(field):
    length = field.shape[1]
    padded = jnp.pad(field, ((0, 0), (1, 1), (1, 1), (0, 0)))
    windows = [padded[:, row_tap:row_tap + length, col_tap:col_tap + length, :] for row_tap in range(3) for col_tap in range(3)]
    return jnp.concatenate(windows, axis=-1).reshape(-1, 9 * field.shape[3])

def fold_back(columns, images_count, length, channels):
    shaped = columns.reshape(images_count, length, length, 9, channels)
    summed = jnp.zeros((images_count, length + 2, length + 2, channels), jnp.float32)
    for row_tap in range(3):
        for col_tap in range(3):
            summed = summed + jnp.pad(shaped[:, :, :, 3 * row_tap + col_tap, :], ((0, 0), (row_tap, 2 - row_tap), (col_tap, 2 - col_tap), (0, 0)))
    return summed[:, 1:length + 1, 1:length + 1, :].reshape(-1, channels)

def block_pass(images, cotangent, w_reduce, w_spatial, w_expand, norm_gain, norm_shift):
    images_count = images.shape[0]
    length = images.shape[1]
    wide_ch = images.shape[3]
    mid_ch = w_reduce.shape[1]
    flat_in = images.reshape(-1, wide_ch)
    gain_one, gain_two, gain_three = (norm_gain[:mid_ch], norm_gain[mid_ch:2 * mid_ch], norm_gain[2 * mid_ch:])
    shift_one, shift_two, shift_three = (norm_shift[:mid_ch], norm_shift[mid_ch:2 * mid_ch], norm_shift[2 * mid_ch:])
    scaled_one, inverse_one, normed_one = normalize(matmul(flat_in, w_reduce), gain_one, shift_one)
    hidden_one = jax.nn.silu(normed_one).astype(jnp.bfloat16)
    patches = unfold(hidden_one.reshape(images_count, length, length, mid_ch))
    scaled_two, inverse_two, normed_two = normalize(matmul(patches, w_spatial), gain_two, shift_two)
    hidden_two = jax.nn.silu(normed_two).astype(jnp.bfloat16)
    scaled_three, inverse_three, normed_three = normalize(contract(hidden_two, w_expand, 1, 1), gain_three, shift_three)
    summed_in = normed_three + flat_in.astype(jnp.float32)
    output = jax.nn.silu(summed_in).astype(jnp.bfloat16)
    upstream = cotangent.reshape(-1, wide_ch).astype(jnp.float32) * slope(summed_in)
    grad_three, shift_sum_three, gain_sum_three = norm_back(upstream, scaled_three, inverse_three, gain_three)
    back_two = matmul(grad_three, w_expand) * slope(normed_two)
    grad_two, shift_sum_two, gain_sum_two = norm_back(back_two, scaled_two, inverse_two, gain_two)
    back_one = fold_back(contract(grad_two, w_spatial, 1, 1), images_count, length, mid_ch) * slope(normed_one)
    grad_one, shift_sum_one, gain_sum_one = norm_back(back_one, scaled_one, inverse_one, gain_one)
    in_grad = (upstream + contract(grad_one, w_reduce, 1, 1)).astype(jnp.bfloat16)
    weight_grads = jnp.concatenate([contract(flat_in, grad_one, 0, 0), contract(patches, grad_two, 0, 0), contract(grad_three, hidden_two, 0, 0)], axis=0)
    norm_grads = jnp.stack([jnp.concatenate([gain_sum_one, gain_sum_two, gain_sum_three]), jnp.concatenate([shift_sum_one, shift_sum_two, shift_sum_three])])
    return (output.reshape(images.shape), in_grad.reshape(images.shape), weight_grads, norm_grads)

def reference(images, cotangent, w_reduce, w_spatial, w_expand, norm_gain, norm_shift):

    def regroup(array):
        tail = array.shape[1:]
        return array.reshape((N_BNGROUP, N_REP, IMG_DEV) + tail).swapaxes(0, 1).reshape((N_REP, N_BNGROUP * IMG_DEV) + tail)

    def ungroup(array):
        tail = array.shape[2:]
        return array.reshape((N_REP, N_BNGROUP, IMG_DEV) + tail).swapaxes(0, 1).reshape((IMAGES,) + tail)

    def group_step(totals, group_items):
        output, in_grad, weight_part, norm_part = block_pass(group_items[0], group_items[1], w_reduce, w_spatial, w_expand, norm_gain, norm_shift)
        return ((totals[0] + weight_part, totals[1] + norm_part), (output, in_grad))
    start_totals = (jnp.zeros((2 * WIDE + 9 * MID, MID), jnp.float32), jnp.zeros((2, 2 * MID + WIDE), jnp.float32))
    totals, results = lax.scan(group_step, start_totals, (regroup(images), regroup(cotangent)))
    return (ungroup(results[0]), ungroup(results[1]), totals[0] / IMAGES, totals[1] / IMAGES)
```

```python
import functools

import jax
import jax.numpy as jnp
from jax import lax
from jax.experimental import pallas as pl
from jax.experimental.pallas import tpu as pltpu
from jax.sharding import PartitionSpec as P

MESH = pl.DeviceIdType.MESH
F32 = jnp.float32
BF16 = jnp.bfloat16

IMGS, SIDE, COLS = 12, 7, 8
WIDE, MID = 2048, 512
BAND = IMGS * COLS
ROWS = SIDE * BAND
REAL = IMGS * SIDE * SIDE
GROUP = 8
COUNT = float(REAL * GROUP)
IMAGES = 1536.0
EPS = 0.25
CH = 256
LANES = 2 * WIDE + 9 * MID
ZBLOCK = LANES // 4
OWN = 1152
VMEM_LIMIT = 67043328


def dot(left, right, dims=((1,), (0,))):
    return lax.dot_general(left, right, (dims, ((), ())), preferred_element_type=F32)


def sigmoid(value):
    return 0.5 * jnp.tanh(0.5 * value) + 0.5


def real_rows(value):
    rows, lanes = value.shape
    tiles = value.reshape(rows // 8, 8, lanes)
    column = lax.broadcasted_iota(jnp.int32, tiles.shape, 1)
    return jnp.where(column != 7, tiles, 0.0).reshape(rows, lanes)


def fold_rows(value):
    rows, lanes = value.shape
    return jnp.sum(value.reshape(rows // 8, 8, lanes), axis=0)


def total(folded):
    return jnp.sum(folded, axis=0, keepdims=True)


def lanes_at(j, size=CH):
    return pl.ds(pl.multiple_of(j * size, size), size)


def band_at(r):
    return pl.ds(pl.multiple_of(r * BAND, BAND), BAND)


def passes(
    x_hbm, cot_hbm, wr_hbm, ws_hbm, we_hbm, gain_ref, shift_ref,
    out_hbm, ing_hbm, wt_hbm, norm_ref,
    x, cot, wr, ws, we, pre1, taps, pre2, h2, pre3, up, g3, g2, back, g1, turned, stage, rows,
    s1, s2, s3, s4, s5, s6, load_sem, send_sem, recv_sem, stage_sem, out_sem,
):
    b = lax.axis_index("bngroup")

    def load(i, src, dst):
        copy = pltpu.make_async_copy(src, dst, load_sem.at[i])
        copy.start()
        return copy

    load_x = load(0, x_hbm, x)
    load_wr = load(1, wr_hbm, wr)
    load_ws = load(2, ws_hbm, ws)
    load_we = load(3, we_hbm, we)
    load_cot = load(4, cot_hbm, cot)

    barrier = pltpu.get_barrier_semaphore()
    for k in range(1, GROUP):
        pl.semaphore_signal(barrier, inc=1, device_id={"bngroup": (b + k) % GROUP}, device_id_type=MESH)

    zeros = jnp.zeros((BAND, 3 * MID), BF16)
    taps[0:BAND, :] = zeros
    taps[ROWS + BAND :, :] = zeros
    g2[0:BAND, :] = zeros
    g2[ROWS + BAND :, :] = zeros

    def share(e, slots):
        copies = []
        for k in range(1, GROUP):
            copy = pltpu.make_async_remote_copy(
                src_ref=slots.at[b],
                dst_ref=slots.at[b],
                send_sem=send_sem.at[e, k - 1],
                recv_sem=recv_sem.at[e, k - 1],
                device_id={"bngroup": (b + k) % GROUP},
                device_id_type=MESH,
            )
            copy.start()
            copies.append(copy)
        return copies

    def arrive(copies):
        for copy in copies:
            copy.wait()

    CEN, AMP, SHI, INV, SS, GS = range(6)
    OFF = {1: 0, 2: MID, 3: 2 * MID}
    SIZE = {1: MID, 2: MID, 3: WIDE}

    def put(row, norm, value):
        rows[row, :, OFF[norm] : OFF[norm] + SIZE[norm]] = value

    def get(row, norm, j):
        return rows[row, :, pl.ds(pl.multiple_of(OFF[norm] + j * CH, CH), CH)]

    def stats(pre, j, slots, channels):
        at = lanes_at(j)

        def add(r, acc):
            return acc + fold_rows(pre[band_at(r), at])

        mean = total(lax.fori_loop(0, SIDE, add, jnp.zeros((8, CH), F32))) / REAL

        def spread(r, acc):
            off = real_rows(pre[band_at(r), at] - mean)
            return acc + fold_rows(off * off)

        second = total(lax.fori_loop(0, SIDE, spread, jnp.zeros((8, CH), F32)))
        slots[b, :, at] = mean
        slots[b, :, pl.ds(pl.multiple_of(channels + j * CH, CH), CH)] = second

    def group_stats(slots, norm):
        c = SIZE[norm]
        mean = slots[0, :, 0:c]
        for i in range(1, GROUP):
            mean = mean + slots[i, :, 0:c]
        mean = mean / GROUP
        second = jnp.zeros((1, c), F32)
        for i in range(GROUP):
            off = slots[i, :, 0:c] - mean
            second = second + (slots[i, :, c : 2 * c] + REAL * (off * off))
        inverse = lax.rsqrt(second / COUNT + EPS)
        put(CEN, norm, mean)
        put(INV, norm, inverse)
        put(AMP, norm, gain_ref[:, OFF[norm] : OFF[norm] + c] * inverse)
        put(SHI, norm, shift_ref[:, OFF[norm] : OFF[norm] + c])

    def group_sums(slots, norm):
        c = SIZE[norm]
        sums = slots[0]
        for i in range(1, GROUP):
            sums = sums + slots[i]
        shift_sum, gain_sum = sums[:, 0:c], sums[:, c : 2 * c]
        inverse = rows[INV, :, OFF[norm] : OFF[norm] + c]
        norm_ref[:, OFF[norm] : OFF[norm] + c] = gain_sum
        norm_ref[:, 3072 + OFF[norm] : 3072 + OFF[norm] + c] = shift_sum
        put(SS, norm, shift_sum / COUNT)
        put(GS, norm, inverse * gain_sum / COUNT)

    load_x.wait()
    load_wr.wait()

    @pl.loop(0, MID // CH)
    def _(j):
        pre1[:, lanes_at(j)] = dot(x[...], wr[:, lanes_at(j)])
        stats(pre1, j, s1, MID)

    pl.semaphore_wait(barrier, GROUP - 1)
    arrive(share(0, s1))
    group_stats(s1, 1)

    @pl.loop(0, MID // CH)
    def _(j):
        cen, amp, shi = get(CEN, 1, j), get(AMP, 1, j), get(SHI, 1, j)

        @pl.loop(0, SIDE)
        def _(r):
            normed = (pre1[band_at(r), lanes_at(j)] - cen) * amp + shi
            hidden = real_rows(normed * sigmoid(normed))
            tiles = hidden.reshape(IMGS, 8, CH)
            to = pl.ds(pl.multiple_of((r + 1) * BAND, BAND), BAND)
            for tap, shifted in enumerate((pltpu.roll(tiles, 1, 1), tiles, pltpu.roll(tiles, 7, 1))):
                at = pl.ds(pl.multiple_of(tap * MID + j * CH, CH), CH)
                taps[to, at] = shifted.reshape(BAND, CH).astype(BF16)

    load_ws.wait()

    @pl.loop(0, MID // CH)
    def _(j):
        acc = dot(taps[0:ROWS, :], ws[0 : 3 * MID, lanes_at(j)])
        acc = acc + dot(taps[BAND : ROWS + BAND, :], ws[3 * MID : 6 * MID, lanes_at(j)])
        acc = acc + dot(taps[2 * BAND :, :], ws[6 * MID :, lanes_at(j)])
        pre2[:, lanes_at(j)] = real_rows(acc)
        stats(pre2, j, s2, MID)

    arrive(share(1, s2))
    group_stats(s2, 2)

    @pl.loop(0, MID // CH)
    def _(j):
        cen, amp, shi = get(CEN, 2, j), get(AMP, 2, j), get(SHI, 2, j)

        @pl.loop(0, SIDE)
        def _(r):
            normed = (pre2[band_at(r), lanes_at(j)] - cen) * amp + shi
            h2[band_at(r), lanes_at(j)] = real_rows(normed * sigmoid(normed)).astype(BF16)

    load_we.wait()

    @pl.loop(0, WIDE // CH)
    def _(j):
        pre3[:, lanes_at(j)] = dot(h2[...], we[lanes_at(j), :], ((1,), (1,)))
        stats(pre3, j, s3, WIDE)

    arrive(share(2, s3))
    group_stats(s3, 3)
    load_cot.wait()

    @pl.loop(0, WIDE // CH)
    def _(j):
        at = lanes_at(j)
        cen, amp, shi, inv = get(CEN, 3, j), get(AMP, 3, j), get(SHI, 3, j), get(INV, 3, j)

        def add(r, acc):
            band = band_at(r)
            centred = pre3[band, at] - cen
            summed = centred * amp + shi + x[band, at].astype(F32)
            sigma = sigmoid(summed)
            upstream = cot[band, at].astype(F32) * (sigma * (1.0 + summed * (1.0 - sigma)))
            cot[band, at] = (summed * sigma).astype(BF16)
            up[band, at] = upstream
            pre3[band, at] = centred
            return (acc[0] + fold_rows(upstream), acc[1] + fold_rows(upstream * centred))

        zero = jnp.zeros((8, CH), F32)
        shift_sum, gain_sum = lax.fori_loop(0, SIDE, add, (zero, zero))
        s4[b, :, at] = total(shift_sum)
        s4[b, :, pl.ds(pl.multiple_of(WIDE + j * CH, CH), CH)] = total(gain_sum) * inv

    sums = share(3, s4)
    write_out = pltpu.make_async_copy(cot, out_hbm, out_sem.at[0])
    write_out.start()
    arrive(sums)
    group_sums(s4, 3)

    @pl.loop(0, WIDE // CH)
    def _(j):
        at = lanes_at(j)
        amp, ss, gs = get(AMP, 3, j), get(SS, 3, j), get(GS, 3, j)

        @pl.loop(0, SIDE)
        def _(r):
            band = band_at(r)
            grad = amp * (up[band, at] - ss - pre3[band, at] * gs)
            g3[band, at] = real_rows(grad).astype(BF16)

    def slope_sums(pre, norm, j, slots):
        at = lanes_at(j)
        cen, amp, shi, inv = get(CEN, norm, j), get(AMP, norm, j), get(SHI, norm, j), get(INV, norm, j)

        def add(r, acc):
            band = band_at(r)
            centred = pre[band, at] - cen
            normed = centred * amp + shi
            sigma = sigmoid(normed)
            value = real_rows(back[band, at] * (sigma * (1.0 + normed * (1.0 - sigma))))
            back[band, at] = value
            return (acc[0] + fold_rows(value), acc[1] + fold_rows(value * centred))

        zero = jnp.zeros((8, CH), F32)
        shift_sum, gain_sum = lax.fori_loop(0, SIDE, add, (zero, zero))
        slots[b, :, at] = total(shift_sum)
        slots[b, :, pl.ds(pl.multiple_of(MID + j * CH, CH), CH)] = total(gain_sum) * inv

    def norm_back(pre, norm, j, r):
        at, band = lanes_at(j), band_at(r)
        cen, amp, ss, gs = get(CEN, norm, j), get(AMP, norm, j), get(SS, norm, j), get(GS, norm, j)
        return real_rows(amp * (back[band, at] - ss - (pre[band, at] - cen) * gs))

    @pl.loop(0, MID // CH)
    def _(j):
        back[:, lanes_at(j)] = dot(g3[...], we[:, lanes_at(j)])
        slope_sums(pre2, 2, j, s5)

    sums = share(4, s5)

    def weigh(first, count, place, right):
        @pl.loop(0, count)
        def _(q):
            slot = (first + q) % 2
            to = pl.ds(pl.multiple_of((place + q) * MID, MID), MID)
            copy = pltpu.make_async_copy(stage.at[slot], wt_hbm.at[:, :, :, to], stage_sem.at[slot])

            @pl.when(first + q >= 2)
            def _():
                copy.wait()

            for half in range(MID // CH):
                block = dot(turned[...], right(q, half)).reshape(16, 2, 16, CH)
                for core in range(2):
                    stage[slot, core, :, :, half * CH : (half + 1) * CH] = block[:, core]
            copy.start()

    turned[...] = h2[...].T
    weigh(0, 4, 13, lambda q, half: g3[:, pl.ds(pl.multiple_of(q * MID + half * CH, CH), CH)])

    arrive(sums)
    group_sums(s5, 2)

    @pl.loop(0, MID // CH)
    def _(j):
        @pl.loop(0, SIDE)
        def _(r):
            grad = norm_back(pre2, 2, j, r)
            tiles = grad.reshape(IMGS, 8, CH)
            to = pl.ds(pl.multiple_of((r + 1) * BAND, BAND), BAND)
            for tap, shifted in enumerate((pltpu.roll(tiles, 7, 1), tiles, pltpu.roll(tiles, 1, 1))):
                at = pl.ds(pl.multiple_of(tap * MID + j * CH, CH), CH)
                g2[to, at] = shifted.reshape(BAND, CH).astype(BF16)

    @pl.loop(0, MID // CH)
    def _(j):
        acc = None
        for row in range(3):
            for col in range(3):
                left = g2[(2 - row) * BAND : (2 - row) * BAND + ROWS, col * MID : (col + 1) * MID]
                at = pl.ds(pl.multiple_of((3 * row + col) * MID + j * CH, CH), CH)
                part = dot(left, ws[at, :], ((1,), (1,)))
                acc = part if acc is None else acc + part
        back[:, lanes_at(j)] = acc
        slope_sums(pre1, 1, j, s6)

    sums = share(5, s6)
    turned[...] = g2[BAND : ROWS + BAND, MID : 2 * MID].T
    weigh(
        4, 9, 4,
        lambda q, half: taps[
            pl.ds(pl.multiple_of((q // 3) * BAND, BAND), ROWS),
            pl.ds(pl.multiple_of((q % 3) * MID + half * CH, CH), CH),
        ],
    )
    arrive(sums)
    group_sums(s6, 1)

    @pl.loop(0, MID // CH)
    def _(j):
        @pl.loop(0, SIDE)
        def _(r):
            g1[band_at(r), lanes_at(j)] = norm_back(pre1, 1, j, r).astype(BF16)

    turned[...] = g1[...].T
    weigh(13, 4, 0, lambda q, half: x[:, pl.ds(pl.multiple_of(q * MID + half * CH, CH), CH)])

    @pl.loop(0, WIDE // CH)
    def _(j):
        at = lanes_at(j)
        g3[:, at] = (up[:, at] + dot(g1[...], wr[at, :], ((1,), (1,)))).astype(BF16)

    write_in = pltpu.make_async_copy(g3, ing_hbm, out_sem.at[1])
    write_in.start()
    for q in (15, 16):
        to = pl.ds(q * MID, MID)
        pltpu.make_async_copy(stage.at[q % 2], wt_hbm.at[:, :, :, to], stage_sem.at[q % 2]).wait()
    write_out.wait()
    write_in.wait()


def run_passes(x, cot, wr, ws, we, gain, shift):
    any_ = pl.BlockSpec(memory_space=pl.ANY)
    vmem = pl.BlockSpec(memory_space=pltpu.VMEM)
    v = pltpu.VMEM
    return pl.pallas_call(
        passes,
        out_shape=(
            jax.ShapeDtypeStruct((ROWS, WIDE), BF16),
            jax.ShapeDtypeStruct((ROWS, WIDE), BF16),
            jax.ShapeDtypeStruct((2, 16, 16, LANES), F32),
            jax.ShapeDtypeStruct((1, 6144), F32),
        ),
        in_specs=[any_] * 5 + [vmem] * 2,
        out_specs=(any_, any_, any_, vmem),
        scratch_shapes=[
            v((ROWS, WIDE), BF16),
            v((ROWS, WIDE), BF16),
            v((WIDE, MID), BF16),
            v((9 * MID, MID), BF16),
            v((WIDE, MID), BF16),
            v((ROWS, MID), F32),
            v((ROWS + 2 * BAND, 3 * MID), BF16),
            v((ROWS, MID), F32),
            v((ROWS, MID), BF16),
            v((ROWS, WIDE), F32),
            v((ROWS, WIDE), F32),
            v((ROWS, WIDE), BF16),
            v((ROWS + 2 * BAND, 3 * MID), BF16),
            v((ROWS, MID), F32),
            v((ROWS, MID), BF16),
            v((MID, ROWS), BF16),
            v((2, 2, 16, 16, MID), F32),
            v((6, 1, 3072), F32),
            v((GROUP, 1, 2 * MID), F32),
            v((GROUP, 1, 2 * MID), F32),
            v((GROUP, 1, 2 * WIDE), F32),
            v((GROUP, 1, 2 * WIDE), F32),
            v((GROUP, 1, 2 * MID), F32),
            v((GROUP, 1, 2 * MID), F32),
            pltpu.SemaphoreType.DMA((5,)),
            pltpu.SemaphoreType.DMA((6, GROUP - 1)),
            pltpu.SemaphoreType.DMA((6, GROUP - 1)),
            pltpu.SemaphoreType.DMA((2,)),
            pltpu.SemaphoreType.DMA((2,)),
        ],
        compiler_params=pltpu.CompilerParams(
            collective_id=0, has_side_effects=True, vmem_limit_bytes=VMEM_LIMIT
        ),
        cost_estimate=pl.CostEstimate(flops=18 * 10**9, bytes_accessed=4 * 10**7, transcendentals=10**7),
        name="passes",
    )(x, cot, wr, ws, we, gain, shift)


PIECES = ((0, 1024), (1024, 1024), (2048, 1024), (3072, 1280))
HALF = LANES // 2


def scatter(
    wt_hbm, norm_in, wg_ref, norm_out,
    own, other, first, second, third, fourth, last, ny, nx,
    core_send, core_recv, own_sem, send_sem, recv_sem, last_send, last_recv, norm_send, norm_recv,
):
    b, rep = lax.axis_index("bngroup"), lax.axis_index("rep")
    c = b % 2
    x, y = rep // 4, rep % 4

    def along(axis, k):
        if axis == "x":
            return {"rep": ((x + k) % 4) * 4 + y}
        return {"rep": x * 4 + (y + k) % 4}

    barrier = pltpu.get_barrier_semaphore()
    for k in range(1, GROUP):
        pl.semaphore_signal(barrier, inc=1, device_id={"bngroup": (b + k) % GROUP}, device_id_type=MESH)
    for axis in "xy":
        for k in range(1, 4):
            pl.semaphore_signal(barrier, inc=1, device_id=along(axis, k), device_id_type=MESH)

    spans = [pl.ds(color * HALF + at, size) for at, size in PIECES for color in range(2)]
    loads = []
    for i, span in enumerate(spans):
        copy = pltpu.make_async_copy(wt_hbm.at[c, :, :, :, span], own.at[:, :, :, span], own_sem.at[i])
        copy.start()
        loads.append(copy)
    pl.semaphore_wait(barrier, GROUP - 1 + 6)

    partner = {"bngroup": b + 1 - 2 * c}
    cores = []
    for i, span in enumerate(spans):
        copy = pltpu.make_async_remote_copy(
            src_ref=wt_hbm.at[1 - c, :, :, :, span],
            dst_ref=other.at[:, :, :, span],
            send_sem=core_send.at[i],
            recv_sem=core_recv.at[i],
            device_id=partner,
            device_id_type=MESH,
        )
        copy.start()
        cores.append(copy)

    def start(src, dst, device, piece, color, step, side):
        copy = pltpu.make_async_remote_copy(
            src_ref=src,
            dst_ref=dst,
            send_sem=send_sem.at[piece, color, step, side],
            recv_sem=recv_sem.at[piece, color, step, side],
            device_id=device,
            device_id_type=MESH,
        )
        copy.start()
        return copy

    def gather(step, axis, slots, mine, sem_send, sem_recv):
        copies = []
        for k in range(1, 4):
            copy = pltpu.make_async_remote_copy(
                src_ref=slots.at[mine],
                dst_ref=slots.at[mine],
                send_sem=sem_send.at[step, k - 1],
                recv_sem=sem_recv.at[step, k - 1],
                device_id=along(axis, k),
                device_id_type=MESH,
            )
            copy.start()
            copies.append(copy)
        return copies

    def sum_of(slots):
        return slots[0] + slots[1] + slots[2] + slots[3]

    ny[y] = norm_in[...]
    norm_copies = gather(0, "y", ny, y, norm_send, norm_recv)

    inflight = {}

    def stage_of(piece, step):
        at, size = PIECES[piece]
        half = size // 2
        for color in range(2):
            span = pl.ds(color * HALF + at, size)
            local = pl.ds(at, size)
            axes = "xy" if color == 0 else "yx"
            me = {"x": x, "y": y}
            outer, inner = me[axes[0]], me[axes[1]]

            def block(index, part=slice(None), span=span, color=color):
                if color == 0:
                    return own.at[index, part, :, span]
                return own.at[part, index, :, span]

            def inner_block(index, part_span, color=color, outer=outer):
                if color == 0:
                    return own.at[outer, index, :, part_span]
                return own.at[index, outer, :, part_span]

            def plus(k, base):
                return (base + k) % 4

            if step == 0:
                i = 2 * piece + color
                loads[i].wait()
                cores[i].wait()

                @pl.loop(0, 16)
                def _(n, span=span):
                    p, q = n // 4, n % 4
                    own[p, q, :, span] += other[p, q, :, span]

                opposite = plus(2, outer)
                inflight[piece, color, 0] = [
                    start(block(opposite, slice(0, 2)), first.at[color, 0, :, :, local], along(axes[0], 1), piece, color, 0, 0),
                    start(block(opposite, slice(2, 4)), first.at[color, 1, :, :, local], along(axes[0], 3), piece, color, 0, 1),
                ]
            elif step == 1:
                for copy in inflight[piece, color, 0]:
                    copy.wait()
                low = block(plus(1, outer), slice(0, 2))
                low[...] += first[color, 0, :, :, local]
                high = block(plus(3, outer), slice(2, 4))
                high[...] += first[color, 1, :, :, local]
                inflight[piece, color, 1] = [
                    start(block(plus(1, outer)), second.at[color, 0, :, :, local], along(axes[0], 1), piece, color, 1, 0),
                    start(block(plus(3, outer)), second.at[color, 1, :, :, local], along(axes[0], 3), piece, color, 1, 1),
                ]
            elif step == 2:
                for copy in inflight[piece, color, 1]:
                    copy.wait()
                mine = block(outer)
                mine[...] += second[color, 0, :, :, local] + second[color, 1, :, :, local]
                opposite = plus(2, inner)
                spans2 = [pl.ds(color * HALF + at, half), pl.ds(color * HALF + at + half, half)]
                local2 = pl.ds(at // 2, half)
                inflight[piece, color, 2] = [
                    start(inner_block(opposite, spans2[0]), third.at[color, 0, :, local2], along(axes[1], 1), piece, color, 2, 0),
                    start(inner_block(opposite, spans2[1]), third.at[color, 1, :, local2], along(axes[1], 3), piece, color, 2, 1),
                ]
            elif step == 3:
                for copy in inflight[piece, color, 2]:
                    copy.wait()
                spans2 = [pl.ds(color * HALF + at, half), pl.ds(color * HALF + at + half, half)]
                local2 = pl.ds(at // 2, half)
                low = inner_block(plus(1, inner), spans2[0])
                low[...] += third[color, 0, :, local2]
                high = inner_block(plus(3, inner), spans2[1])
                high[...] += third[color, 1, :, local2]
                inflight[piece, color, 3] = [
                    start(inner_block(plus(1, inner), span), fourth.at[color, 0, :, local], along(axes[1], 1), piece, color, 3, 0),
                    start(inner_block(plus(3, inner), span), fourth.at[color, 1, :, local], along(axes[1], 3), piece, color, 3, 1),
                ]
            else:
                for copy in inflight[piece, color, 3]:
                    copy.wait()
                mine = inner_block(inner, span)
                mine[...] += fourth[color, 0, :, local] + fourth[color, 1, :, local]

    for t in range(len(PIECES) + 4):
        for step in reversed(range(5)):
            if 0 <= t - step < len(PIECES):
                stage_of(t - step, step)

    def owned(device):
        return pl.ds(pl.multiple_of((device // 2) * ZBLOCK + (device % 2) * 1024, 128), OWN)

    finals = []
    for k in range(1, GROUP):
        peer = (b + k) % GROUP
        copy = pltpu.make_async_remote_copy(
            src_ref=own.at[x, y, :, owned(peer)],
            dst_ref=last.at[b],
            send_sem=last_send.at[k - 1],
            recv_sem=last_recv.at[k - 1],
            device_id={"bngroup": peer},
            device_id_type=MESH,
        )
        copy.start()
        finals.append(copy)
    last[b] = own[x, y, :, owned(b)]

    for copy in norm_copies:
        copy.wait()
    nx[x] = sum_of(ny)
    norm_copies = gather(1, "x", nx, x, norm_send, norm_recv)

    for copy in finals:
        copy.wait()
    parts = []
    for core in range(2):
        parts.append(last[core] + last[2 + core] + last[4 + core] + last[6 + core])
    whole = jnp.concatenate(parts, axis=0) * (1.0 / IMAGES)
    turned = pltpu.roll(whole, OWN - 64, 1)
    wg_ref[...] = jnp.where(c == 1, turned, whole)[:, : LANES // 8]
    for copy in norm_copies:
        copy.wait()
    norm_out[...] = sum_of(nx) * (1.0 / IMAGES)


def run_scatter(wt, norm):
    any_ = pl.BlockSpec(memory_space=pl.ANY)
    vmem = pl.BlockSpec(memory_space=pltpu.VMEM)
    v = pltpu.VMEM
    dma = pltpu.SemaphoreType.DMA
    n = len(PIECES)
    return pl.pallas_call(
        scatter,
        out_shape=(
            jax.ShapeDtypeStruct((32, LANES // 8), F32),
            jax.ShapeDtypeStruct((1, 6144), F32),
        ),
        in_specs=[any_, vmem],
        out_specs=(vmem, vmem),
        scratch_shapes=[
            v((4, 4, 16, LANES), F32),
            v((4, 4, 16, LANES), F32),
            v((2, 2, 2, 16, HALF), F32),
            v((2, 2, 4, 16, HALF), F32),
            v((2, 2, 16, HALF // 2), F32),
            v((2, 2, 16, HALF), F32),
            v((GROUP, 16, OWN), F32),
            v((4, 1, 6144), F32),
            v((4, 1, 6144), F32),
            dma((2 * n,)),
            dma((2 * n,)),
            dma((2 * n,)),
            dma((n, 2, 4, 2)),
            dma((n, 2, 4, 2)),
            dma((GROUP - 1,)),
            dma((GROUP - 1,)),
            dma((2, 3)),
            dma((2, 3)),
        ],
        compiler_params=pltpu.CompilerParams(
            collective_id=1, has_side_effects=True, vmem_limit_bytes=VMEM_LIMIT
        ),
        cost_estimate=pl.CostEstimate(flops=10**7, bytes_accessed=2 * 10**7, transcendentals=0),
        name="scatter",
    )(wt.reshape(2, 4, 4, 16, LANES), norm)


def to_rows(images):
    padded = jnp.pad(images, ((0, 0), (0, 0), (0, 1), (0, 0)))
    return padded.transpose(1, 0, 2, 3).reshape(ROWS, WIDE)


def from_rows(rows):
    return rows.reshape(SIDE, IMGS, COLS, WIDE)[:, :, :SIDE].transpose(1, 0, 2, 3)


def per_device(images, cotangent, w_reduce, w_spatial, w_expand, norm_gain, norm_shift):
    output, in_grad, wt, norms = run_passes(
        to_rows(images), to_rows(cotangent), w_reduce, w_spatial, w_expand,
        norm_gain.reshape(1, -1), norm_shift.reshape(1, -1),
    )
    grads, norm_grads = run_scatter(wt, norms)
    return (from_rows(output), from_rows(in_grad), grads.T, norm_grads.reshape(2, -1))


def solution(mesh):
    both = P(("bngroup", "rep"), None, None, None)
    return jax.shard_map(
        per_device,
        mesh=mesh,
        in_specs=(both, both, P(), P(), P(), P(), P()),
        out_specs=(both, both, P("bngroup", "rep"), P()),
        check_vma=False,
    )
```

```python
import jax
import jax.numpy as jnp
from jax import lax
from jax.experimental import pallas as pl
from jax.experimental.pallas import tpu as pltpu
from jax.sharding import PartitionSpec as P

MESH = pl.DeviceIdType.MESH
F32 = jnp.float32
BF16 = jnp.bfloat16

IMGS, SIDE, COLS = 12, 7, 8
WIDE, MID = 2048, 512
BAND = IMGS * COLS
ROWS = SIDE * BAND
REAL = IMGS * SIDE * SIDE
GROUP = 8
COUNT = float(REAL * GROUP)
IMAGES = 1536.0
EPS = 0.25
CH = 256
LANES = 2 * WIDE + 9 * MID
ZBLOCK = LANES // 4
OWN = 1152
VMEM_LIMIT = 67043328
SLOTS = 4

PIECES = {
    "expand": (6656, 2048, 0, 4),
    "low": (2048, 1536, 4, 3),
    "mid": (3584, 1536, 7, 3),
    "high": (5120, 1536, 10, 3),
    "reduce": (0, 2048, 13, 4),
}
SHARE = {}
_ab, _c = 0, 0
for _name, (_lane, _size, _, _) in PIECES.items():
    _n = (_size - 512) // 2
    SHARE[_name] = (_n, _ab, _c)
    _ab, _c = _ab + _n, _c + 128
AB_LANES, C_LANES = _ab, _c


def dot(left, right, dims=((1,), (0,))):
    return lax.dot_general(left, right, (dims, ((), ())), preferred_element_type=F32)


def sigmoid(value):
    return 0.5 * jnp.tanh(0.5 * value) + 0.5


def real_rows(value):
    rows, lanes = value.shape
    tiles = value.reshape(rows // 8, 8, lanes)
    column = lax.broadcasted_iota(jnp.int32, tiles.shape, 1)
    return jnp.where(column != 7, tiles, 0.0).reshape(rows, lanes)


def fold_rows(value):
    rows, lanes = value.shape
    return jnp.sum(value.reshape(rows // 8, 8, lanes), axis=0)


def total(folded):
    return jnp.sum(folded, axis=0, keepdims=True)


def lanes_at(j, size=CH):
    return pl.ds(pl.multiple_of(j * size, size), size)


def band_at(r):
    return pl.ds(pl.multiple_of(r * BAND, BAND), BAND)


def block(
    x_hbm, cot_hbm, wr_hbm, ws_hbm, we_hbm, gain_ref, shift_ref,
    out_hbm, ing_hbm, wg_ref, norm_out,
    x, cot, wa, ws, pre1, taps, pre2, h2, pre3, up, g3, g2, back, turned, stage, rows,
    s1, s2, s3, s4, s5, s6, norm, own, other, ab1, ab2, ab3, ab4, c1, c2, c3, c4, last, ny, nx,
    load_sem, send_sem, recv_sem, out_sem, core_send, core_recv,
    ab_send, ab_recv, cz_send, cz_recv, cd_send, cd_recv, last_send, last_recv, norm_send, norm_recv,
):
    b, rep = lax.axis_index("bngroup"), lax.axis_index("rep")
    z, c = b // 2, b % 2
    xx, yy = rep // 4, rep % 4

    def along(axis, k):
        if axis == "x":
            return {"rep": ((xx + k) % 4) * 4 + yy}
        if axis == "y":
            return {"rep": xx * 4 + (yy + k) % 4}
        return {"bngroup": (b + 2 * k) % GROUP}

    def load(i, src, dst):
        copy = pltpu.make_async_copy(src, dst, load_sem.at[i])
        copy.start()
        return copy

    load_x = load(0, x_hbm, x)
    load_wr = load(1, wr_hbm, wa)
    load_ws = load(2, ws_hbm, ws)
    load_cot = load(4, cot_hbm, cot)

    barrier = pltpu.get_barrier_semaphore()
    for k in range(1, GROUP):
        pl.semaphore_signal(barrier, inc=1, device_id={"bngroup": (b + k) % GROUP}, device_id_type=MESH)
    for axis in "xy":
        for k in range(1, 4):
            pl.semaphore_signal(barrier, inc=1, device_id=along(axis, k), device_id_type=MESH)

    zeros = jnp.zeros((BAND, 3 * MID), BF16)
    taps[0:BAND, :] = zeros
    taps[ROWS + BAND :, :] = zeros
    g2[0:BAND, :] = zeros
    g2[ROWS + BAND :, :] = zeros

    def share(e, slots):
        copies = []
        for k in range(1, GROUP):
            copy = pltpu.make_async_remote_copy(
                src_ref=slots.at[b],
                dst_ref=slots.at[b],
                send_sem=send_sem.at[e, k - 1],
                recv_sem=recv_sem.at[e, k - 1],
                device_id={"bngroup": (b + k) % GROUP},
                device_id_type=MESH,
            )
            copy.start()
            copies.append(copy)
        return copies

    def arrive(copies):
        for copy in copies:
            copy.wait()

    CEN, AMP, SHI, INV, SS, GS = range(6)
    OFF = {1: 0, 2: MID, 3: 2 * MID}
    SIZE = {1: MID, 2: MID, 3: WIDE}

    def put(row, which, value):
        rows[row, :, OFF[which] : OFF[which] + SIZE[which]] = value

    def get(row, which, j):
        return rows[row, :, pl.ds(pl.multiple_of(OFF[which] + j * CH, CH), CH)]

    def stats(pre, j, slots, channels):
        at = lanes_at(j)

        def add(r, acc):
            return acc + fold_rows(pre[band_at(r), at])

        mean = total(lax.fori_loop(0, SIDE, add, jnp.zeros((8, CH), F32))) / REAL

        def spread(r, acc):
            off = real_rows(pre[band_at(r), at] - mean)
            return acc + fold_rows(off * off)

        second = total(lax.fori_loop(0, SIDE, spread, jnp.zeros((8, CH), F32)))
        slots[b, :, at] = mean
        slots[b, :, pl.ds(pl.multiple_of(channels + j * CH, CH), CH)] = second

    def group_stats(slots, which):
        c = SIZE[which]
        mean = slots[0, :, 0:c]
        for i in range(1, GROUP):
            mean = mean + slots[i, :, 0:c]
        mean = mean / GROUP
        second = jnp.zeros((1, c), F32)
        for i in range(GROUP):
            off = slots[i, :, 0:c] - mean
            second = second + (slots[i, :, c : 2 * c] + REAL * (off * off))
        inverse = lax.rsqrt(second / COUNT + EPS)
        put(CEN, which, mean)
        put(INV, which, inverse)
        put(AMP, which, gain_ref[:, OFF[which] : OFF[which] + c] * inverse)
        put(SHI, which, shift_ref[:, OFF[which] : OFF[which] + c])

    def group_sums(slots, which):
        c = SIZE[which]
        sums = slots[0]
        for i in range(1, GROUP):
            sums = sums + slots[i]
        shift_sum, gain_sum = sums[:, 0:c], sums[:, c : 2 * c]
        inverse = rows[INV, :, OFF[which] : OFF[which] + c]
        norm[0:1, OFF[which] : OFF[which] + c] = gain_sum
        norm[1:2, OFF[which] : OFF[which] + c] = shift_sum
        put(SS, which, shift_sum / COUNT)
        put(GS, which, inverse * gain_sum / COUNT)

    load_x.wait()
    load_wr.wait()

    @pl.loop(0, MID // CH)
    def _(j):
        pre1[:, lanes_at(j)] = dot(x[...], wa[:, lanes_at(j)])
        stats(pre1, j, s1, MID)

    load_we = load(3, we_hbm, wa)
    pl.semaphore_wait(barrier, GROUP - 1 + 6)
    arrive(share(0, s1))
    group_stats(s1, 1)

    @pl.loop(0, MID // CH)
    def _(j):
        cen, amp, shi = get(CEN, 1, j), get(AMP, 1, j), get(SHI, 1, j)

        @pl.loop(0, SIDE)
        def _(r):
            normed = (pre1[band_at(r), lanes_at(j)] - cen) * amp + shi
            hidden = real_rows(normed * sigmoid(normed))
            tiles = hidden.reshape(IMGS, 8, CH)
            to = pl.ds(pl.multiple_of((r + 1) * BAND, BAND), BAND)
            for tap, shifted in enumerate((pltpu.roll(tiles, 1, 1), tiles, pltpu.roll(tiles, 7, 1))):
                at = pl.ds(pl.multiple_of(tap * MID + j * CH, CH), CH)
                taps[to, at] = shifted.reshape(BAND, CH).astype(BF16)

    load_ws.wait()

    @pl.loop(0, MID // CH)
    def _(j):
        acc = dot(taps[0:ROWS, :], ws[0 : 3 * MID, lanes_at(j)])
        acc = acc + dot(taps[BAND : ROWS + BAND, :], ws[3 * MID : 6 * MID, lanes_at(j)])
        acc = acc + dot(taps[2 * BAND :, :], ws[6 * MID :, lanes_at(j)])
        pre2[:, lanes_at(j)] = real_rows(acc)
        stats(pre2, j, s2, MID)

    arrive(share(1, s2))
    group_stats(s2, 2)

    @pl.loop(0, MID // CH)
    def _(j):
        cen, amp, shi = get(CEN, 2, j), get(AMP, 2, j), get(SHI, 2, j)

        @pl.loop(0, SIDE)
        def _(r):
            normed = (pre2[band_at(r), lanes_at(j)] - cen) * amp + shi
            h2[band_at(r), lanes_at(j)] = real_rows(normed * sigmoid(normed)).astype(BF16)

    load_we.wait()

    @pl.loop(0, WIDE // CH)
    def _(j):
        pre3[:, lanes_at(j)] = dot(h2[...], wa[lanes_at(j), :], ((1,), (1,)))
        stats(pre3, j, s3, WIDE)

    arrive(share(2, s3))
    group_stats(s3, 3)
    load_cot.wait()

    @pl.loop(0, WIDE // CH)
    def _(j):
        at = lanes_at(j)
        cen, amp, shi, inv = get(CEN, 3, j), get(AMP, 3, j), get(SHI, 3, j), get(INV, 3, j)

        def add(r, acc):
            band = band_at(r)
            centred = pre3[band, at] - cen
            summed = centred * amp + shi + x[band, at].astype(F32)
            sigma = sigmoid(summed)
            upstream = cot[band, at].astype(F32) * (sigma * (1.0 + summed * (1.0 - sigma)))
            cot[band, at] = (summed * sigma).astype(BF16)
            up[band, at] = upstream
            pre3[band, at] = centred
            return (acc[0] + fold_rows(upstream), acc[1] + fold_rows(upstream * centred))

        zero = jnp.zeros((8, CH), F32)
        shift_sum, gain_sum = lax.fori_loop(0, SIDE, add, (zero, zero))
        s4[b, :, at] = total(shift_sum)
        s4[b, :, pl.ds(pl.multiple_of(WIDE + j * CH, CH), CH)] = total(gain_sum) * inv

    sums = share(3, s4)
    write_out = pltpu.make_async_copy(cot, out_hbm, out_sem.at[0])
    write_out.start()
    arrive(sums)
    group_sums(s4, 3)

    @pl.loop(0, WIDE // CH)
    def _(j):
        at = lanes_at(j)
        amp, ss, gs = get(AMP, 3, j), get(SS, 3, j), get(GS, 3, j)

        @pl.loop(0, SIDE)
        def _(r):
            band = band_at(r)
            grad = amp * (up[band, at] - ss - pre3[band, at] * gs)
            g3[band, at] = real_rows(grad).astype(BF16)

    def slope_sums(pre, which, j, slots):
        at = lanes_at(j)
        cen, amp, shi, inv = get(CEN, which, j), get(AMP, which, j), get(SHI, which, j), get(INV, which, j)

        def add(r, acc):
            band = band_at(r)
            centred = pre[band, at] - cen
            normed = centred * amp + shi
            sigma = sigmoid(normed)
            value = real_rows(back[band, at] * (sigma * (1.0 + normed * (1.0 - sigma))))
            back[band, at] = value
            return (acc[0] + fold_rows(value), acc[1] + fold_rows(value * centred))

        zero = jnp.zeros((8, CH), F32)
        shift_sum, gain_sum = lax.fori_loop(0, SIDE, add, (zero, zero))
        slots[b, :, at] = total(shift_sum)
        slots[b, :, pl.ds(pl.multiple_of(MID + j * CH, CH), CH)] = total(gain_sum) * inv

    def norm_back(pre, which, j, r):
        at, band = lanes_at(j), band_at(r)
        cen, amp, ss, gs = get(CEN, which, j), get(AMP, which, j), get(SS, which, j), get(GS, which, j)
        return real_rows(amp * (back[band, at] - ss - (pre[band, at] - cen) * gs))

    @pl.loop(0, MID // CH)
    def _(j):
        back[:, lanes_at(j)] = dot(g3[...], wa[:, lanes_at(j)])
        slope_sums(pre2, 2, j, s5)

    sums = share(4, s5)
    load_wr = load(5, wr_hbm, wa)

    def turn(value):
        halves = value.T.reshape(16, 2, 16, ROWS)
        for half in range(2):
            turned[(half + c + 1) % 2] = halves[:, half].reshape(MID // 2, ROWS)

    def landing(piece, at):
        if piece == "expand":
            return pre3.at[0:256, at]
        if piece == "reduce":
            return pre3.at[256:512, at]
        return other.at[:, at]

    def to_partner(piece, i):
        lane, size, chunk, _ = PIECES[piece]
        start = lane - 2048 if piece in ("low", "mid", "high") else 0
        at = pl.ds(pl.multiple_of(start + i * MID, MID), MID)
        return pltpu.make_async_remote_copy(
            src_ref=stage.at[(chunk + i) % SLOTS],
            dst_ref=landing(piece, at),
            send_sem=core_send.at[chunk + i],
            recv_sem=core_recv.at[chunk + i],
            device_id={"bngroup": b + 1 - 2 * c},
            device_id_type=MESH,
        )

    def slot_free(n):
        pltpu.make_async_remote_copy(
            src_ref=stage.at[n % SLOTS],
            dst_ref=other.at[:, 0:MID],
            send_sem=core_send.at[n],
            recv_sem=core_recv.at[n],
            device_id={"bngroup": b + 1 - 2 * c},
            device_id_type=MESH,
        ).wait_send()

    def weigh(piece, right):
        lane, size, chunk, count = PIECES[piece]

        @pl.loop(0, count)
        def _(i):
            slot = (chunk + i) % SLOTS
            if chunk >= SLOTS:
                slot_free(chunk + i - SLOTS)
            for half in range(MID // CH):
                product = dot(turned[...].reshape(MID, ROWS), right(i, half))
                stage[slot, :, half * CH : (half + 1) * CH] = product[: MID // 2]
                at = pl.ds(pl.multiple_of(lane + i * MID + half * CH, CH), CH)
                own[:, :, :, at] = product[MID // 2 :].reshape(4, 4, 16, CH)
            if piece != "expand":
                to_partner(piece, i).start()

    flying = {}

    def send(src, dst, device, sems):
        copy = pltpu.make_async_remote_copy(
            src_ref=src, dst_ref=dst, send_sem=sems[0], recv_sem=sems[1],
            device_id=device, device_id_type=MESH,
        )
        copy.start()
        return copy

    def plus(k, base):
        return (base + k) % 4

    names = list(PIECES)

    def step(piece, n):
        lane, size, chunk, count = PIECES[piece]
        width, ab_at, c_at = SHARE[piece]
        p = names.index(piece)
        half = width // 2
        if n == 0:
            for i in range(count):
                to_partner(piece, i).wait_recv()
            start = lane - 2048 if piece in ("low", "mid", "high") else 0
            landed = landing(piece, pl.ds(start, size))

            @pl.loop(0, 16)
            def _(k):
                own[k // 4, k % 4, :, lane : lane + size] += landed[pl.ds(pl.multiple_of(k * 16, 16), 16), :]

        else:
            for copy in flying.pop((piece, n - 1)):
                copy.wait()
        copies = []
        for color in range(2):
            span = pl.ds(lane + color * width, width)
            local = pl.ds(ab_at, width)
            axes = "xy" if color == 0 else "yx"
            outer, inner = (xx, yy) if color == 0 else (yy, xx)
            parts = [pl.ds(lane + color * width + k * half, half) for k in range(2)]
            local_part = pl.ds(ab_at // 2, half)
            sems = [(ab_send.at[p, color, n, side], ab_recv.at[p, color, n, side]) for side in range(2)] if n < 4 else None

            def outer_block(index, part=slice(None), color=color, span=span):
                return own.at[index, part, :, span] if color == 0 else own.at[part, index, :, span]

            def inner_block(index, part, color=color, outer=outer):
                return own.at[outer, index, :, part] if color == 0 else own.at[index, outer, :, part]

            if n == 0:
                far = plus(2, outer)
                copies.append(send(outer_block(far, slice(0, 2)), ab1.at[color, 0, :, :, local], along(axes[0], 1), sems[0]))
                copies.append(send(outer_block(far, slice(2, 4)), ab1.at[color, 1, :, :, local], along(axes[0], 3), sems[1]))
            elif n == 1:
                low = outer_block(plus(1, outer), slice(0, 2))
                low[...] += ab1[color, 0, :, :, local]
                high = outer_block(plus(3, outer), slice(2, 4))
                high[...] += ab1[color, 1, :, :, local]
                copies.append(send(outer_block(plus(1, outer)), ab2.at[color, 0, :, :, local], along(axes[0], 1), sems[0]))
                copies.append(send(outer_block(plus(3, outer)), ab2.at[color, 1, :, :, local], along(axes[0], 3), sems[1]))
            elif n == 2:
                mine = outer_block(outer)
                mine[...] += ab2[color, 0, :, :, local] + ab2[color, 1, :, :, local]
                far = plus(2, inner)
                copies.append(send(inner_block(far, parts[0]), ab3.at[color, 0, :, local_part], along(axes[1], 1), sems[0]))
                copies.append(send(inner_block(far, parts[1]), ab3.at[color, 1, :, local_part], along(axes[1], 3), sems[1]))
            elif n == 3:
                low = inner_block(plus(1, inner), parts[0])
                low[...] += ab3[color, 0, :, local_part]
                high = inner_block(plus(3, inner), parts[1])
                high[...] += ab3[color, 1, :, local_part]
                copies.append(send(inner_block(plus(1, inner), span), ab4.at[color, 0, :, local], along(axes[1], 1), sems[0]))
                copies.append(send(inner_block(plus(3, inner), span), ab4.at[color, 1, :, local], along(axes[1], 3), sems[1]))
            else:
                mine = inner_block(inner, span)
                mine[...] += ab4[color, 0, :, local] + ab4[color, 1, :, local]

        base = lane + 2 * width
        local = pl.ds(c_at, 128)

        def tile(index):
            return pl.ds(pl.multiple_of(base + 128 * index, 128), 128)

        if n < 2:
            sems = [(cz_send.at[p, n, side], cz_recv.at[p, n, side]) for side in range(2)]
        elif n < 4:
            sems = [(cd_send.at[p, n - 2, k], cd_recv.at[p, n - 2, k]) for k in range(3)]
        if n == 0:
            far = tile(plus(2, z))
            copies.append(send(own.at[0:2, :, :, far], c1.at[0, :, :, :, local], along("z", 1), sems[0]))
            copies.append(send(own.at[2:4, :, :, far], c1.at[1, :, :, :, local], along("z", 3), sems[1]))
        elif n == 1:
            up_one, down_one = tile(plus(1, z)), tile(plus(3, z))
            own[0:2, :, :, up_one] += c1[0, :, :, :, local]
            own[2:4, :, :, down_one] += c1[1, :, :, :, local]
            copies.append(send(own.at[:, :, :, up_one], c2.at[0, :, :, :, local], along("z", 1), sems[0]))
            copies.append(send(own.at[:, :, :, down_one], c2.at[1, :, :, :, local], along("z", 3), sems[1]))
        elif n == 2:
            own[:, :, :, tile(z)] += c2[0, :, :, :, local] + c2[1, :, :, :, local]
            for k in range(1, 4):
                copies.append(send(own.at[plus(k, xx), :, :, tile(z)], c3.at[k - 1, :, :, local], along("x", k), sems[k - 1]))
        elif n == 3:
            own[xx, :, :, tile(z)] += c3[0, :, :, local] + c3[1, :, :, local] + c3[2, :, :, local]
            for k in range(1, 4):
                copies.append(send(own.at[xx, plus(k, yy), :, tile(z)], c4.at[k - 1, :, local], along("y", k), sems[k - 1]))
        else:
            mine = own[xx, yy, :, tile(z)] + c4[0, :, local] + c4[1, :, local] + c4[2, :, local]
            own[xx, yy, :, base : base + 512] = jnp.zeros((16, 512), F32)
            own[xx, yy, :, tile(z)] = mine
        if n < 4:
            flying[piece, n] = copies

    def owned(device):
        return pl.ds(pl.multiple_of((device // 2) * ZBLOCK + (device % 2) * 1024, 128), OWN)

    def to_owner(t):
        return pltpu.make_async_remote_copy(
            src_ref=own.at[xx, yy, :, owned(t)],
            dst_ref=last.at[b],
            send_sem=last_send.at[t],
            recv_sem=last_recv.at[b],
            device_id={"bngroup": t},
            device_id_type=MESH,
        )

    def from_member(t):
        return pltpu.make_async_remote_copy(
            src_ref=own.at[xx, yy, :, owned(b)],
            dst_ref=last.at[t],
            send_sem=last_send.at[t],
            recv_sem=last_recv.at[t],
            device_id={"bngroup": t},
            device_id_type=MESH,
        )

    def to_owners(targets):
        for t in targets:

            @pl.when(b != t)
            def _(t=t):
                to_owner(t).start()

    def gather(n, axis, slots, mine):
        return [
            send(slots.at[mine], slots.at[mine], along(axis, k), (norm_send.at[n, k - 1], norm_recv.at[n, k - 1]))
            for k in range(1, 4)
        ]

    def sum_of(slots):
        return slots[0] + slots[1] + slots[2] + slots[3]

    turn(h2[...])
    weigh("expand", lambda i, half: g3[:, pl.ds(pl.multiple_of(i * MID + half * CH, CH), CH)])

    arrive(sums)
    for i in range(4):
        to_partner("expand", i).start()
    group_sums(s5, 2)

    @pl.loop(0, MID // CH)
    def _(j):
        @pl.loop(0, SIDE)
        def _(r):
            grad = norm_back(pre2, 2, j, r)
            tiles = grad.reshape(IMGS, 8, CH)
            to = pl.ds(pl.multiple_of((r + 1) * BAND, BAND), BAND)
            for tap, shifted in enumerate((pltpu.roll(tiles, 7, 1), tiles, pltpu.roll(tiles, 1, 1))):
                at = pl.ds(pl.multiple_of(tap * MID + j * CH, CH), CH)
                g2[to, at] = shifted.reshape(BAND, CH).astype(BF16)

    step("expand", 0)

    for j in range(MID // CH):
        acc = None
        for row in range(3):
            for col in range(3):
                left = g2[(2 - row) * BAND : (2 - row) * BAND + ROWS, col * MID : (col + 1) * MID]
                at = pl.ds((3 * row + col) * MID + j * CH, CH)
                part = dot(left, ws[at, :], ((1,), (1,)))
                acc = part if acc is None else acc + part
        back[:, j * CH : (j + 1) * CH] = acc
        slope_sums(pre1, 1, j, s6)
        if j == 0:
            step("expand", 1)

    sums = share(5, s6)
    turn(g2[BAND : ROWS + BAND, MID : 2 * MID])

    def tap_row(row):
        return lambda i, half: taps[
            row * BAND : row * BAND + ROWS,
            pl.ds(pl.multiple_of(i * MID + half * CH, CH), CH),
        ]

    weigh("low", tap_row(0))
    step("expand", 2)
    step("low", 0)
    weigh("mid", tap_row(1))
    step("expand", 3)
    step("low", 1)
    step("mid", 0)
    weigh("high", tap_row(2))
    arrive(sums)
    group_sums(s6, 1)
    ny[yy] = norm[...]
    norm_copies = gather(0, "y", ny, yy)

    @pl.loop(0, MID // CH)
    def _(j):
        @pl.loop(0, SIDE)
        def _(r):
            h2[band_at(r), lanes_at(j)] = norm_back(pre1, 1, j, r).astype(BF16)

    step("expand", 4)
    step("low", 2)
    step("mid", 1)
    step("high", 0)
    turn(h2[...])
    weigh("reduce", lambda i, half: x[:, pl.ds(pl.multiple_of(i * MID + half * CH, CH), CH)])
    step("low", 3)
    step("mid", 2)
    step("high", 1)
    step("reduce", 0)

    load_wr.wait()

    @pl.loop(0, WIDE // CH)
    def _(j):
        at = lanes_at(j)
        g3[:, at] = (up[:, at] + dot(h2[...], wa[at, :], ((1,), (1,)))).astype(BF16)

    write_in = pltpu.make_async_copy(g3, ing_hbm, out_sem.at[1])
    write_in.start()

    step("low", 4)
    step("mid", 3)
    step("high", 2)
    step("reduce", 1)
    step("mid", 4)
    step("high", 3)
    for copy in norm_copies:
        copy.wait()
    nx[xx] = sum_of(ny)
    norm_copies = gather(1, "x", nx, xx)
    step("reduce", 2)
    step("high", 4)
    to_owners(range(2, GROUP))
    step("reduce", 3)
    step("reduce", 4)
    to_owners(range(2))
    last[b] = own[xx, yy, :, owned(b)]

    for copy in norm_copies:
        copy.wait()
    norm_out[...] = sum_of(nx) * (1.0 / IMAGES)
    write_out.wait()
    write_in.wait()
    for n in range(13, 17):
        slot_free(n)
    for t in range(GROUP):

        @pl.when(b != t)
        def _(t=t):
            to_owner(t).wait_send()
            from_member(t).wait_recv()

    parts = []
    for core in range(2):
        parts.append(last[core] + last[2 + core] + last[4 + core] + last[6 + core])
    whole = jnp.concatenate(parts, axis=0) * (1.0 / IMAGES)
    moved = pltpu.roll(whole, OWN - 64, 1)
    wg_ref[...] = jnp.where(c == 1, moved, whole)[:, : LANES // 8]


def run_block(x, cot, wr, ws, we, gain, shift):
    any_ = pl.BlockSpec(memory_space=pl.ANY)
    vmem = pl.BlockSpec(memory_space=pltpu.VMEM)
    v = pltpu.VMEM
    dma = pltpu.SemaphoreType.DMA
    pieces = len(PIECES)
    return pl.pallas_call(
        block,
        out_shape=(
            jax.ShapeDtypeStruct((ROWS, WIDE), BF16),
            jax.ShapeDtypeStruct((ROWS, WIDE), BF16),
            jax.ShapeDtypeStruct((32, LANES // 8), F32),
            jax.ShapeDtypeStruct((2, 3072), F32),
        ),
        in_specs=[any_] * 5 + [vmem] * 2,
        out_specs=(any_, any_, vmem, vmem),
        scratch_shapes=[
            v((ROWS, WIDE), BF16),
            v((ROWS, WIDE), BF16),
            v((WIDE, MID), BF16),
            v((9 * MID, MID), BF16),
            v((ROWS, MID), F32),
            v((ROWS + 2 * BAND, 3 * MID), BF16),
            v((ROWS, MID), F32),
            v((ROWS, MID), BF16),
            v((ROWS, WIDE), F32),
            v((ROWS, WIDE), F32),
            v((ROWS, WIDE), BF16),
            v((ROWS + 2 * BAND, 3 * MID), BF16),
            v((ROWS, MID), F32),
            v((2, MID // 2, ROWS), BF16),
            v((SLOTS, MID // 2, MID), F32),
            v((6, 1, 3072), F32),
            v((GROUP, 1, 2 * MID), F32),
            v((GROUP, 1, 2 * MID), F32),
            v((GROUP, 1, 2 * WIDE), F32),
            v((GROUP, 1, 2 * WIDE), F32),
            v((GROUP, 1, 2 * MID), F32),
            v((GROUP, 1, 2 * MID), F32),
            v((2, 3072), F32),
            v((4, 4, 16, LANES), F32),
            v((MID // 2, 9 * MID), F32),
            v((2, 2, 2, 16, AB_LANES), F32),
            v((2, 2, 4, 16, AB_LANES), F32),
            v((2, 2, 16, AB_LANES // 2), F32),
            v((2, 2, 16, AB_LANES), F32),
            v((2, 2, 4, 16, C_LANES), F32),
            v((2, 4, 4, 16, C_LANES), F32),
            v((3, 4, 16, C_LANES), F32),
            v((3, 16, C_LANES), F32),
            v((GROUP, 16, OWN), F32),
            v((4, 2, 3072), F32),
            v((4, 2, 3072), F32),
            dma((6,)),
            dma((6, GROUP - 1)),
            dma((6, GROUP - 1)),
            dma((2,)),
            dma((17,)),
            dma((17,)),
            dma((pieces, 2, 4, 2)),
            dma((pieces, 2, 4, 2)),
            dma((pieces, 2, 2)),
            dma((pieces, 2, 2)),
            dma((pieces, 2, 3)),
            dma((pieces, 2, 3)),
            dma((GROUP,)),
            dma((GROUP,)),
            dma((2, 3)),
            dma((2, 3)),
        ],
        compiler_params=pltpu.CompilerParams(
            collective_id=0, has_side_effects=True, vmem_limit_bytes=VMEM_LIMIT
        ),
        cost_estimate=pl.CostEstimate(flops=18 * 10**9, bytes_accessed=4 * 10**7, transcendentals=10**7),
        name="block",
    )(x, cot, wr, ws, we, gain, shift)


def to_rows(images):
    padded = jnp.pad(images, ((0, 0), (0, 0), (0, 1), (0, 0)))
    return padded.transpose(1, 0, 2, 3).reshape(ROWS, WIDE)


def from_rows(rows):
    return rows.reshape(SIDE, IMGS, COLS, WIDE)[:, :, :SIDE].transpose(1, 0, 2, 3)


def per_device(images, cotangent, w_reduce, w_spatial, w_expand, norm_gain, norm_shift):
    output, in_grad, grads, norm_grads = run_block(
        to_rows(images), to_rows(cotangent), w_reduce, w_spatial, w_expand,
        norm_gain.reshape(1, -1), norm_shift.reshape(1, -1),
    )
    return (from_rows(output), from_rows(in_grad), grads.T, norm_grads)


def solution(mesh):
    both = P(("bngroup", "rep"), None, None, None)
    return jax.shard_map(
        per_device,
        mesh=mesh,
        in_specs=(both, both, P(), P(), P(), P(), P()),
        out_specs=(both, both, P("bngroup", "rep"), P()),
        check_vma=False,
    )
```

```python
import jax
import jax.numpy as jnp
from jax import lax
from jax.experimental import pallas as pl
from jax.experimental.pallas import tpu as pltpu
from jax.sharding import PartitionSpec as P

MESH = pl.DeviceIdType.MESH
F32 = jnp.float32
BF16 = jnp.bfloat16

IMGS, SIDE, COLS = 12, 7, 8
WIDE, MID = 2048, 512
BAND = IMGS * COLS
ROWS = SIDE * BAND
REAL = IMGS * SIDE * SIDE
GROUP = 8
COUNT = float(REAL * GROUP)
IMAGES = 1536.0
EPS = 0.25
CH = 256
LANES = 2 * WIDE + 9 * MID
ZBLOCK = LANES // 4
OWN = 1152
VMEM_LIMIT = 67043328
SLOTS = 4

PIECES = {
    "expand": (6656, 2048, 0, 4),
    "low": (2048, 1536, 4, 3),
    "mid": (3584, 1536, 7, 3),
    "high": (5120, 1536, 10, 3),
    "upper": (1024, 1024, 13, 2),
    "first": (0, 1024, 15, 2),
}
LANDING = {"expand": 0, "low": 0, "mid": 1536, "high": 3072, "upper": 1024, "first": 0}
SHARE = {}
_ab, _c = 0, 0
for _name, (_lane, _size, _, _) in PIECES.items():
    _n = (_size - 512) // 2
    SHARE[_name] = (_n, _ab, _c)
    _ab, _c = _ab + _n, _c + 128
AB_LANES, C_LANES = _ab, _c


def dot(left, right, dims=((1,), (0,))):
    return lax.dot_general(left, right, (dims, ((), ())), preferred_element_type=F32)


def sigmoid(value):
    return 0.5 * jnp.tanh(0.5 * value) + 0.5


def real_rows(value):
    rows, lanes = value.shape
    tiles = value.reshape(rows // 8, 8, lanes)
    column = lax.broadcasted_iota(jnp.int32, tiles.shape, 1)
    return jnp.where(column != 7, tiles, 0.0).reshape(rows, lanes)


def fold_rows(value):
    rows, lanes = value.shape
    return jnp.sum(value.reshape(rows // 8, 8, lanes), axis=0)


def total(folded):
    return jnp.sum(folded, axis=0, keepdims=True)


def lanes_at(j, size=CH):
    return pl.ds(pl.multiple_of(j * size, size), size)


def band_at(r):
    return pl.ds(pl.multiple_of(r * BAND, BAND), BAND)


def block(
    x_hbm, cot_hbm, wr_hbm, ws_hbm, we_hbm, gain_ref, shift_ref,
    out_hbm, ing_hbm, wg_ref, norm_out,
    x, cot, wa, ws, pre1, taps, pre2, h2, pre3, up, g3, g2, back, turned, stage, rows,
    s1, s2, s3, s4, s5, s6, norm, own, other, ab1, ab2, ab3, ab4, c1, c2, c3, c4, last, ny, nx,
    load_sem, send_sem, recv_sem, out_sem, core_send, core_recv,
    ab_send, ab_recv, cz_send, cz_recv, cd_send, cd_recv, last_send, last_recv, norm_send, norm_recv, ready,
):
    b, rep = lax.axis_index("bngroup"), lax.axis_index("rep")
    z, c = b // 2, b % 2
    xx, yy = rep // 4, rep % 4

    def along(axis, k):
        if axis == "x":
            return {"rep": ((xx + k) % 4) * 4 + yy}
        if axis == "y":
            return {"rep": xx * 4 + (yy + k) % 4}
        return {"bngroup": (b + 2 * k) % GROUP}

    def load(i, src, dst):
        copy = pltpu.make_async_copy(src, dst, load_sem.at[i])
        copy.start()
        return copy

    load_x = load(0, x_hbm, x)
    load_wr = load(1, wr_hbm, wa)

    barrier = pltpu.get_barrier_semaphore()
    for k in range(1, GROUP):
        pl.semaphore_signal(barrier, inc=1, device_id={"bngroup": (b + k) % GROUP}, device_id_type=MESH)
    for axis in "xy":
        for k in range(1, 4):
            pl.semaphore_signal(barrier, inc=1, device_id=along(axis, k), device_id_type=MESH)

    zeros = jnp.zeros((BAND, 3 * MID), BF16)
    taps[0:BAND, :] = zeros
    taps[ROWS + BAND :, :] = zeros
    g2[0:BAND, :] = zeros
    g2[ROWS + BAND :, :] = zeros

    def share(e, slots):
        copies = []
        for k in range(1, GROUP):
            copy = pltpu.make_async_remote_copy(
                src_ref=slots.at[b],
                dst_ref=slots.at[b],
                send_sem=send_sem.at[e, k - 1],
                recv_sem=recv_sem.at[e, k - 1],
                device_id={"bngroup": (b + k) % GROUP},
                device_id_type=MESH,
            )
            copy.start()
            copies.append(copy)
        return copies

    def arrive(copies):
        for copy in copies:
            copy.wait()

    CEN, AMP, SHI, INV, SS, GS = range(6)
    OFF = {1: 0, 2: MID, 3: 2 * MID}
    SIZE = {1: MID, 2: MID, 3: WIDE}

    def put(row, which, value):
        rows[row, :, OFF[which] : OFF[which] + SIZE[which]] = value

    def get(row, which, j):
        return rows[row, :, pl.ds(pl.multiple_of(OFF[which] + j * CH, CH), CH)]

    def stats(pre, j, slots, channels):
        at = lanes_at(j)

        def add(r, acc):
            return acc + fold_rows(pre[band_at(r), at])

        mean = total(lax.fori_loop(0, SIDE, add, jnp.zeros((8, CH), F32))) / REAL

        def spread(r, acc):
            off = real_rows(pre[band_at(r), at] - mean)
            return acc + fold_rows(off * off)

        second = total(lax.fori_loop(0, SIDE, spread, jnp.zeros((8, CH), F32)))
        slots[b, :, at] = mean
        slots[b, :, pl.ds(pl.multiple_of(channels + j * CH, CH), CH)] = second

    def group_stats(slots, which):
        c = SIZE[which]
        mean = slots[0, :, 0:c]
        for i in range(1, GROUP):
            mean = mean + slots[i, :, 0:c]
        mean = mean / GROUP
        second = jnp.zeros((1, c), F32)
        for i in range(GROUP):
            off = slots[i, :, 0:c] - mean
            second = second + (slots[i, :, c : 2 * c] + REAL * (off * off))
        inverse = lax.rsqrt(second / COUNT + EPS)
        put(CEN, which, mean)
        put(INV, which, inverse)
        put(AMP, which, gain_ref[:, OFF[which] : OFF[which] + c] * inverse)
        put(SHI, which, shift_ref[:, OFF[which] : OFF[which] + c])

    def group_sums(slots, which):
        c = SIZE[which]
        sums = slots[0]
        for i in range(1, GROUP):
            sums = sums + slots[i]
        shift_sum, gain_sum = sums[:, 0:c], sums[:, c : 2 * c]
        inverse = rows[INV, :, OFF[which] : OFF[which] + c]
        norm[0:1, OFF[which] : OFF[which] + c] = gain_sum
        norm[1:2, OFF[which] : OFF[which] + c] = shift_sum
        put(SS, which, shift_sum / COUNT)
        put(GS, which, inverse * gain_sum / COUNT)

    load_x.wait()
    load_wr.wait()
    load_ws = load(2, ws_hbm, ws)
    load_cot = load(4, cot_hbm, cot)

    @pl.loop(0, MID // CH)
    def _(j):
        pre1[:, lanes_at(j)] = dot(x[...], wa[:, lanes_at(j)])
        stats(pre1, j, s1, MID)

    load_we = load(3, we_hbm, wa)
    pl.semaphore_wait(barrier, GROUP - 1 + 6)
    arrive(share(0, s1))
    group_stats(s1, 1)

    @pl.loop(0, MID // CH)
    def _(j):
        cen, amp, shi = get(CEN, 1, j), get(AMP, 1, j), get(SHI, 1, j)

        @pl.loop(0, SIDE)
        def _(r):
            normed = (pre1[band_at(r), lanes_at(j)] - cen) * amp + shi
            hidden = real_rows(normed * sigmoid(normed))
            tiles = hidden.reshape(IMGS, 8, CH)
            to = pl.ds(pl.multiple_of((r + 1) * BAND, BAND), BAND)
            for tap, shifted in enumerate((pltpu.roll(tiles, 1, 1), tiles, pltpu.roll(tiles, 7, 1))):
                at = pl.ds(pl.multiple_of(tap * MID + j * CH, CH), CH)
                taps[to, at] = shifted.reshape(BAND, CH).astype(BF16)

    load_ws.wait()

    @pl.loop(0, MID // CH)
    def _(j):
        acc = dot(taps[0:ROWS, :], ws[0 : 3 * MID, lanes_at(j)])
        acc = acc + dot(taps[BAND : ROWS + BAND, :], ws[3 * MID : 6 * MID, lanes_at(j)])
        acc = acc + dot(taps[2 * BAND :, :], ws[6 * MID :, lanes_at(j)])
        pre2[:, lanes_at(j)] = real_rows(acc)
        stats(pre2, j, s2, MID)

    arrive(share(1, s2))
    group_stats(s2, 2)

    @pl.loop(0, MID // CH)
    def _(j):
        cen, amp, shi = get(CEN, 2, j), get(AMP, 2, j), get(SHI, 2, j)

        @pl.loop(0, SIDE)
        def _(r):
            normed = (pre2[band_at(r), lanes_at(j)] - cen) * amp + shi
            h2[band_at(r), lanes_at(j)] = real_rows(normed * sigmoid(normed)).astype(BF16)

    load_we.wait()

    @pl.loop(0, WIDE // CH)
    def _(j):
        pre3[:, lanes_at(j)] = dot(h2[...], wa[lanes_at(j), :], ((1,), (1,)))
        stats(pre3, j, s3, WIDE)

    arrive(share(2, s3))
    group_stats(s3, 3)
    load_cot.wait()

    @pl.loop(0, WIDE // CH)
    def _(j):
        at = lanes_at(j)
        cen, amp, shi, inv = get(CEN, 3, j), get(AMP, 3, j), get(SHI, 3, j), get(INV, 3, j)

        def add(r, acc):
            band = band_at(r)
            centred = pre3[band, at] - cen
            summed = centred * amp + shi + x[band, at].astype(F32)
            sigma = sigmoid(summed)
            upstream = cot[band, at].astype(F32) * (sigma * (1.0 + summed * (1.0 - sigma)))
            cot[band, at] = (summed * sigma).astype(BF16)
            up[band, at] = upstream
            pre3[band, at] = centred
            return (acc[0] + fold_rows(upstream), acc[1] + fold_rows(upstream * centred))

        zero = jnp.zeros((8, CH), F32)
        shift_sum, gain_sum = lax.fori_loop(0, SIDE, add, (zero, zero))
        s4[b, :, at] = total(shift_sum)
        s4[b, :, pl.ds(pl.multiple_of(WIDE + j * CH, CH), CH)] = total(gain_sum) * inv

    def turn(value):
        halves = value.T.reshape(16, 2, 16, ROWS)
        for half in range(2):
            turned[(half + c + 1) % 2] = halves[:, half].reshape(MID // 2, ROWS)

    def landing(piece, at):
        if piece == "expand":
            return pre3.at[0:256, at]
        if piece in ("upper", "first"):
            return pre3.at[256:512, at]
        return other.at[:, at]

    def to_partner(piece, i):
        lane, size, chunk, _ = PIECES[piece]
        start = LANDING[piece]
        at = pl.ds(pl.multiple_of(start + i * MID, MID), MID)
        return pltpu.make_async_remote_copy(
            src_ref=stage.at[(chunk + i) % SLOTS],
            dst_ref=landing(piece, at),
            send_sem=core_send.at[chunk + i],
            recv_sem=core_recv.at[chunk + i],
            device_id={"bngroup": b + 1 - 2 * c},
            device_id_type=MESH,
        )

    def slot_free(n):
        pltpu.make_async_remote_copy(
            src_ref=stage.at[n % SLOTS],
            dst_ref=other.at[:, 0:MID],
            send_sem=core_send.at[n],
            recv_sem=core_recv.at[n],
            device_id={"bngroup": b + 1 - 2 * c},
            device_id_type=MESH,
        ).wait_send()

    def weigh(piece, right):
        lane, size, chunk, count = PIECES[piece]

        @pl.loop(0, count)
        def _(i):
            slot = (chunk + i) % SLOTS
            if chunk >= SLOTS:
                slot_free(chunk + i - SLOTS)
            for half in range(MID // CH):
                product = dot(turned[...].reshape(MID, ROWS), right(i, half))
                stage[slot, :, half * CH : (half + 1) * CH] = product[: MID // 2]
                at = pl.ds(pl.multiple_of(lane + i * MID + half * CH, CH), CH)
                own[:, :, :, at] = product[MID // 2 :].reshape(4, 4, 16, CH)
            to_partner(piece, i).start()

    flying = {}

    def send(src, dst, device, sems):
        copy = pltpu.make_async_remote_copy(
            src_ref=src, dst_ref=dst, send_sem=sems[0], recv_sem=sems[1],
            device_id=device, device_id_type=MESH,
        )
        copy.start()
        return copy

    def plus(k, base):
        return (base + k) % 4

    names = list(PIECES)

    def step(piece, n):
        lane, size, chunk, count = PIECES[piece]
        width, ab_at, c_at = SHARE[piece]
        p = names.index(piece)
        half = width // 2
        if n == 0:
            for i in range(count):
                to_partner(piece, i).wait_recv()
            start = LANDING[piece]
            landed = landing(piece, pl.ds(start, size))

            @pl.loop(0, 16)
            def _(k):
                own[k // 4, k % 4, :, lane : lane + size] += landed[pl.ds(pl.multiple_of(k * 16, 16), 16), :]

        else:
            for copy in flying.pop((piece, n - 1)):
                copy.wait()
        copies = []
        for color in range(2):
            span = pl.ds(lane + color * width, width)
            local = pl.ds(ab_at, width)
            axes = "xy" if color == 0 else "yx"
            outer, inner = (xx, yy) if color == 0 else (yy, xx)
            parts = [pl.ds(lane + color * width + k * half, half) for k in range(2)]
            local_part = pl.ds(ab_at // 2, half)
            sems = [(ab_send.at[p, color, n, side], ab_recv.at[p, color, n, side]) for side in range(2)] if n < 4 else None

            def outer_block(index, part=slice(None), color=color, span=span):
                return own.at[index, part, :, span] if color == 0 else own.at[part, index, :, span]

            def inner_block(index, part, color=color, outer=outer):
                return own.at[outer, index, :, part] if color == 0 else own.at[index, outer, :, part]

            if n == 0:
                far = plus(2, outer)
                copies.append(send(outer_block(far, slice(0, 2)), ab1.at[color, 0, :, :, local], along(axes[0], 1), sems[0]))
                copies.append(send(outer_block(far, slice(2, 4)), ab1.at[color, 1, :, :, local], along(axes[0], 3), sems[1]))
            elif n == 1:
                low = outer_block(plus(1, outer), slice(0, 2))
                low[...] += ab1[color, 0, :, :, local]
                high = outer_block(plus(3, outer), slice(2, 4))
                high[...] += ab1[color, 1, :, :, local]
                copies.append(send(outer_block(plus(1, outer)), ab2.at[color, 0, :, :, local], along(axes[0], 1), sems[0]))
                copies.append(send(outer_block(plus(3, outer)), ab2.at[color, 1, :, :, local], along(axes[0], 3), sems[1]))
            elif n == 2:
                mine = outer_block(outer)
                mine[...] += ab2[color, 0, :, :, local] + ab2[color, 1, :, :, local]
                far = plus(2, inner)
                copies.append(send(inner_block(far, parts[0]), ab3.at[color, 0, :, local_part], along(axes[1], 1), sems[0]))
                copies.append(send(inner_block(far, parts[1]), ab3.at[color, 1, :, local_part], along(axes[1], 3), sems[1]))
            elif n == 3:
                low = inner_block(plus(1, inner), parts[0])
                low[...] += ab3[color, 0, :, local_part]
                high = inner_block(plus(3, inner), parts[1])
                high[...] += ab3[color, 1, :, local_part]
                copies.append(send(inner_block(plus(1, inner), span), ab4.at[color, 0, :, local], along(axes[1], 1), sems[0]))
                copies.append(send(inner_block(plus(3, inner), span), ab4.at[color, 1, :, local], along(axes[1], 3), sems[1]))
            else:
                mine = inner_block(inner, span)
                mine[...] += ab4[color, 0, :, local] + ab4[color, 1, :, local]

        base = lane + 2 * width
        local = pl.ds(c_at, 128)

        def tile(index):
            return pl.ds(pl.multiple_of(base + 128 * index, 128), 128)

        first_axis = "x" if p % 2 == 0 else "y"
        second_axis = "y" if p % 2 == 0 else "x"
        if n < 2:
            sems = [(cz_send.at[p, n, side], cz_recv.at[p, n, side]) for side in range(2)]
        elif n < 4:
            sems = [(cd_send.at[p, n - 2, k], cd_recv.at[p, n - 2, k]) for k in range(3)]
        if n == 0:
            far = tile(plus(2, z))
            copies.append(send(own.at[0:2, :, :, far], c1.at[0, :, :, :, local], along("z", 1), sems[0]))
            copies.append(send(own.at[2:4, :, :, far], c1.at[1, :, :, :, local], along("z", 3), sems[1]))
        elif n == 1:
            up_one, down_one = tile(plus(1, z)), tile(plus(3, z))
            own[0:2, :, :, up_one] += c1[0, :, :, :, local]
            own[2:4, :, :, down_one] += c1[1, :, :, :, local]
            copies.append(send(own.at[:, :, :, up_one], c2.at[0, :, :, :, local], along("z", 1), sems[0]))
            copies.append(send(own.at[:, :, :, down_one], c2.at[1, :, :, :, local], along("z", 3), sems[1]))
        elif n == 2:
            own[:, :, :, tile(z)] += c2[0, :, :, :, local] + c2[1, :, :, :, local]
            for k in range(1, 4):
                block_of = own.at[plus(k, xx), :, :, tile(z)] if p % 2 == 0 else own.at[:, plus(k, yy), :, tile(z)]
                copies.append(send(block_of, c3.at[k - 1, :, :, local], along(first_axis, k), sems[k - 1]))
        elif n == 3:
            mine = own.at[xx, :, :, tile(z)] if p % 2 == 0 else own.at[:, yy, :, tile(z)]
            mine[...] += c3[0, :, :, local] + c3[1, :, :, local] + c3[2, :, :, local]
            for k in range(1, 4):
                block_of = own.at[xx, plus(k, yy), :, tile(z)] if p % 2 == 0 else own.at[plus(k, xx), yy, :, tile(z)]
                copies.append(send(block_of, c4.at[k - 1, :, local], along(second_axis, k), sems[k - 1]))
        else:
            mine = own[xx, yy, :, tile(z)] + c4[0, :, local] + c4[1, :, local] + c4[2, :, local]
            own[xx, yy, :, base : base + 512] = jnp.zeros((16, 512), F32)
            own[xx, yy, :, tile(z)] = mine
        if n < 4:
            flying[piece, n] = copies

    def owned(device):
        return pl.ds(pl.multiple_of((device // 2) * ZBLOCK + (device % 2) * 1024, 128), OWN)

    def to_owner(t):
        return pltpu.make_async_remote_copy(
            src_ref=own.at[xx, yy, :, owned(t)],
            dst_ref=last.at[b],
            send_sem=last_send.at[t],
            recv_sem=last_recv.at[b],
            device_id={"bngroup": t},
            device_id_type=MESH,
        )

    def from_member(t):
        return pltpu.make_async_remote_copy(
            src_ref=own.at[xx, yy, :, owned(b)],
            dst_ref=last.at[t],
            send_sem=last_send.at[t],
            recv_sem=last_recv.at[t],
            device_id={"bngroup": t},
            device_id_type=MESH,
        )

    def to_owners(targets):
        for t in targets:

            @pl.when(b != t)
            def _(t=t):
                to_owner(t).start()

    def gather(n, axis, slots, mine):
        return [
            send(slots.at[mine], slots.at[mine], along(axis, k), (norm_send.at[n, k - 1], norm_recv.at[n, k - 1]))
            for k in range(1, 4)
        ]

    def sum_of(slots):
        return slots[0] + slots[1] + slots[2] + slots[3]

    sums = share(3, s4)
    write_out = pltpu.make_async_copy(cot, out_hbm, out_sem.at[0])
    write_out.start()
    turn(h2[...])
    arrive(sums)
    group_sums(s4, 3)

    @pl.loop(0, WIDE // CH)
    def _(j):
        at = lanes_at(j)
        amp, ss, gs = get(AMP, 3, j), get(SS, 3, j), get(GS, 3, j)

        @pl.loop(0, SIDE)
        def _(r):
            band = band_at(r)
            grad = amp * (up[band, at] - ss - pre3[band, at] * gs)
            g3[band, at] = real_rows(grad).astype(BF16)

    def slope_sums(pre, which, j, slots):
        at = lanes_at(j)
        cen, amp, shi, inv = get(CEN, which, j), get(AMP, which, j), get(SHI, which, j), get(INV, which, j)

        def add(r, acc):
            band = band_at(r)
            centred = pre[band, at] - cen
            normed = centred * amp + shi
            sigma = sigmoid(normed)
            value = real_rows(back[band, at] * (sigma * (1.0 + normed * (1.0 - sigma))))
            back[band, at] = value
            return (acc[0] + fold_rows(value), acc[1] + fold_rows(value * centred))

        zero = jnp.zeros((8, CH), F32)
        shift_sum, gain_sum = lax.fori_loop(0, SIDE, add, (zero, zero))
        slots[b, :, at] = total(shift_sum)
        slots[b, :, pl.ds(pl.multiple_of(MID + j * CH, CH), CH)] = total(gain_sum) * inv

    def norm_back(pre, which, j, r):
        at, band = lanes_at(j), band_at(r)
        cen, amp, ss, gs = get(CEN, which, j), get(AMP, which, j), get(SS, which, j), get(GS, which, j)
        return real_rows(amp * (back[band, at] - ss - (pre[band, at] - cen) * gs))

    pl.semaphore_signal(ready, inc=1, device_id={"bngroup": b + 1 - 2 * c}, device_id_type=MESH)
    pl.semaphore_wait(ready, 1)
    weigh("expand", lambda i, half: g3[:, pl.ds(pl.multiple_of(i * MID + half * CH, CH), CH)])
    @pl.loop(0, MID // CH)
    def _(j):
        back[:, lanes_at(j)] = dot(g3[...], wa[:, lanes_at(j)])
        slope_sums(pre2, 2, j, s5)

    sums = share(4, s5)
    load_wr = load(5, wr_hbm, wa)

    step("expand", 0)
    arrive(sums)
    group_sums(s5, 2)

    @pl.loop(0, MID // CH)
    def _(j):
        @pl.loop(0, SIDE)
        def _(r):
            grad = norm_back(pre2, 2, j, r)
            tiles = grad.reshape(IMGS, 8, CH)
            to = pl.ds(pl.multiple_of((r + 1) * BAND, BAND), BAND)
            for tap, shifted in enumerate((pltpu.roll(tiles, 7, 1), tiles, pltpu.roll(tiles, 1, 1))):
                at = pl.ds(pl.multiple_of(tap * MID + j * CH, CH), CH)
                g2[to, at] = shifted.reshape(BAND, CH).astype(BF16)

    def tap_row(row):
        return lambda i, half: taps[
            row * BAND : row * BAND + ROWS,
            pl.ds(pl.multiple_of(i * MID + half * CH, CH), CH),
        ]

    def back_one(j):
        acc = None
        for row in range(3):
            for col in range(3):
                left = g2[(2 - row) * BAND : (2 - row) * BAND + ROWS, col * MID : (col + 1) * MID]
                at = pl.ds((3 * row + col) * MID + j * CH, CH)
                part = dot(left, ws[at, :], ((1,), (1,)))
                acc = part if acc is None else acc + part
        back[:, j * CH : (j + 1) * CH] = acc
        slope_sums(pre1, 1, j, s6)

    turn(g2[BAND : ROWS + BAND, MID : 2 * MID])
    weigh("low", tap_row(0))
    weigh("mid", tap_row(1))
    step("low", 0)
    step("expand", 1)
    weigh("high", tap_row(2))
    step("mid", 0)
    back_one(0)
    step("high", 0)
    step("low", 1)
    step("expand", 2)
    back_one(1)
    sums = share(5, s6)
    step("mid", 1)
    step("expand", 3)
    step("high", 1)
    step("low", 2)
    arrive(sums)
    group_sums(s6, 1)
    ny[yy] = norm[...]
    norm_copies = gather(0, "y", ny, yy)

    @pl.loop(0, MID // CH)
    def _(j):
        @pl.loop(0, SIDE)
        def _(r):
            h2[band_at(r), lanes_at(j)] = norm_back(pre1, 1, j, r).astype(BF16)

    turn(h2[...])
    weigh("upper", lambda i, half: x[:, pl.ds(pl.multiple_of(1024 + i * MID + half * CH, CH), CH)])
    weigh("first", lambda i, half: x[:, pl.ds(pl.multiple_of(i * MID + half * CH, CH), CH)])
    step("upper", 0)
    step("mid", 2)
    step("first", 0)
    step("high", 2)
    step("low", 3)
    step("expand", 4)

    load_wr.wait()

    @pl.loop(0, WIDE // CH)
    def _(j):
        at = lanes_at(j)
        g3[:, at] = (up[:, at] + dot(h2[...], wa[at, :], ((1,), (1,)))).astype(BF16)

    write_in = pltpu.make_async_copy(g3, ing_hbm, out_sem.at[1])
    write_in.start()

    step("upper", 1)
    step("mid", 3)
    step("first", 1)
    step("high", 3)
    step("low", 4)
    for copy in norm_copies:
        copy.wait()
    nx[xx] = sum_of(ny)
    norm_copies = gather(1, "x", nx, xx)
    step("upper", 2)
    step("mid", 4)
    step("first", 2)
    step("high", 4)
    to_owners(range(2, 8))
    step("upper", 3)
    step("first", 3)
    step("upper", 4)
    to_owners(range(1, 2))
    step("first", 4)
    to_owners(range(0, 1))
    last[b] = own[xx, yy, :, owned(b)]

    for copy in norm_copies:
        copy.wait()
    norm_out[...] = sum_of(nx) * (1.0 / IMAGES)
    write_out.wait()
    write_in.wait()
    for n in range(13, 17):
        slot_free(n)
    for t in range(GROUP):

        @pl.when(b != t)
        def _(t=t):
            to_owner(t).wait_send()
            from_member(t).wait_recv()

    parts = []
    for core in range(2):
        parts.append(last[core] + last[2 + core] + last[4 + core] + last[6 + core])
    whole = jnp.concatenate(parts, axis=0) * (1.0 / IMAGES)
    moved = pltpu.roll(whole, OWN - 64, 1)
    wg_ref[...] = jnp.where(c == 1, moved, whole)[:, : LANES // 8]


def run_block(x, cot, wr, ws, we, gain, shift):
    any_ = pl.BlockSpec(memory_space=pl.ANY)
    vmem = pl.BlockSpec(memory_space=pltpu.VMEM)
    v = pltpu.VMEM
    dma = pltpu.SemaphoreType.DMA
    pieces = len(PIECES)
    return pl.pallas_call(
        block,
        out_shape=(
            jax.ShapeDtypeStruct((ROWS, WIDE), BF16),
            jax.ShapeDtypeStruct((ROWS, WIDE), BF16),
            jax.ShapeDtypeStruct((32, LANES // 8), F32),
            jax.ShapeDtypeStruct((2, 3072), F32),
        ),
        in_specs=[any_] * 5 + [vmem] * 2,
        out_specs=(any_, any_, vmem, vmem),
        scratch_shapes=[
            v((ROWS, WIDE), BF16),
            v((ROWS, WIDE), BF16),
            v((WIDE, MID), BF16),
            v((9 * MID, MID), BF16),
            v((ROWS, MID), F32),
            v((ROWS + 2 * BAND, 3 * MID), BF16),
            v((ROWS, MID), F32),
            v((ROWS, MID), BF16),
            v((ROWS, WIDE), F32),
            v((ROWS, WIDE), F32),
            v((ROWS, WIDE), BF16),
            v((ROWS + 2 * BAND, 3 * MID), BF16),
            v((ROWS, MID), F32),
            v((2, MID // 2, ROWS), BF16),
            v((SLOTS, MID // 2, MID), F32),
            v((6, 1, 3072), F32),
            v((GROUP, 1, 2 * MID), F32),
            v((GROUP, 1, 2 * MID), F32),
            v((GROUP, 1, 2 * WIDE), F32),
            v((GROUP, 1, 2 * WIDE), F32),
            v((GROUP, 1, 2 * MID), F32),
            v((GROUP, 1, 2 * MID), F32),
            v((2, 3072), F32),
            v((4, 4, 16, LANES), F32),
            v((MID // 2, 9 * MID), F32),
            v((2, 2, 2, 16, AB_LANES), F32),
            v((2, 2, 4, 16, AB_LANES), F32),
            v((2, 2, 16, AB_LANES // 2), F32),
            v((2, 2, 16, AB_LANES), F32),
            v((2, 2, 4, 16, C_LANES), F32),
            v((2, 4, 4, 16, C_LANES), F32),
            v((3, 4, 16, C_LANES), F32),
            v((3, 16, C_LANES), F32),
            v((GROUP, 16, OWN), F32),
            v((4, 2, 3072), F32),
            v((4, 2, 3072), F32),
            dma((6,)),
            dma((6, GROUP - 1)),
            dma((6, GROUP - 1)),
            dma((2,)),
            dma((17,)),
            dma((17,)),
            dma((pieces, 2, 4, 2)),
            dma((pieces, 2, 4, 2)),
            dma((pieces, 2, 2)),
            dma((pieces, 2, 2)),
            dma((pieces, 2, 3)),
            dma((pieces, 2, 3)),
            dma((GROUP,)),
            dma((GROUP,)),
            dma((2, 3)),
            dma((2, 3)),
            pltpu.SemaphoreType.REGULAR,
        ],
        compiler_params=pltpu.CompilerParams(
            collective_id=0, has_side_effects=True, vmem_limit_bytes=VMEM_LIMIT
        ),
        cost_estimate=pl.CostEstimate(flops=18 * 10**9, bytes_accessed=4 * 10**7, transcendentals=10**7),
        name="block",
    )(x, cot, wr, ws, we, gain, shift)


def to_rows(images):
    padded = jnp.pad(images, ((0, 0), (0, 0), (0, 1), (0, 0)))
    return padded.transpose(1, 0, 2, 3).reshape(ROWS, WIDE)


def from_rows(rows):
    return rows.reshape(SIDE, IMGS, COLS, WIDE)[:, :, :SIDE].transpose(1, 0, 2, 3)


def per_device(images, cotangent, w_reduce, w_spatial, w_expand, norm_gain, norm_shift):
    output, in_grad, grads, norm_grads = run_block(
        to_rows(images), to_rows(cotangent), w_reduce, w_spatial, w_expand,
        norm_gain.reshape(1, -1), norm_shift.reshape(1, -1),
    )
    return (from_rows(output), from_rows(in_grad), grads.T, norm_grads)


def solution(mesh):
    both = P(("bngroup", "rep"), None, None, None)
    return jax.shard_map(
        per_device,
        mesh=mesh,
        in_specs=(both, both, P(), P(), P(), P(), P()),
        out_specs=(both, both, P("bngroup", "rep"), P()),
        check_vma=False,
    )
```

```python
import jax
import jax.numpy as jnp
from jax import lax
from jax.experimental import pallas as pl
from jax.experimental.pallas import tpu as pltpu
from jax.sharding import PartitionSpec as P

MESH = pl.DeviceIdType.MESH
F32 = jnp.float32
BF16 = jnp.bfloat16

IMGS, SIDE, COLS = 12, 7, 8
WIDE, MID = 2048, 512
BAND = IMGS * COLS
ROWS = SIDE * BAND
REAL = IMGS * SIDE * SIDE
GROUP = 8
COUNT = float(REAL * GROUP)
IMAGES = 1536.0
EPS = 0.25
CH = 256
LANES = 2 * WIDE + 9 * MID
ZBLOCK = LANES // 4
OWN = 1152
VMEM_LIMIT = 67043328
SLOTS = 4

PIECES = {
    "expand": (6656, 2048, 0, 4),
    "low": (2048, 1536, 4, 3),
    "mid": (3584, 1536, 7, 3),
    "high": (5120, 1536, 10, 3),
    "upper": (1024, 1024, 13, 2),
    "first": (0, 1024, 15, 2),
}
LANDING = {"expand": 0, "low": 0, "mid": 1536, "high": 3072, "upper": 1024, "first": 0}
SHARE = {}
_ab, _c = 0, 0
for _name, (_lane, _size, _, _) in PIECES.items():
    _n = (_size - 512) // 2
    SHARE[_name] = (_n, _ab, _c)
    _ab, _c = _ab + _n, _c + 128
AB_LANES, C_LANES = _ab, _c


def dot(left, right, dims=((1,), (0,))):
    return lax.dot_general(left, right, (dims, ((), ())), preferred_element_type=F32)


def sigmoid(value):
    return 0.5 * jnp.tanh(0.5 * value) + 0.5


def real_rows(value):
    rows, lanes = value.shape
    tiles = value.reshape(rows // 8, 8, lanes)
    column = lax.broadcasted_iota(jnp.int32, tiles.shape, 1)
    return jnp.where(column != 7, tiles, 0.0).reshape(rows, lanes)


def fold_rows(value):
    rows, lanes = value.shape
    return jnp.sum(value.reshape(rows // 8, 8, lanes), axis=0)


def total(folded):
    return jnp.sum(folded, axis=0, keepdims=True)


def lanes_at(j, size=CH):
    return pl.ds(pl.multiple_of(j * size, size), size)


def band_at(r):
    return pl.ds(pl.multiple_of(r * BAND, BAND), BAND)


def block(
    x_hbm, cot_hbm, wr_hbm, ws_hbm, we_hbm, gain_ref, shift_ref,
    out_hbm, ing_hbm, wg_ref, norm_out,
    x, raw, wa, ws, pre1, taps, pre2, h2, pre3, up, g3, g2, back, turned, stage, rows,
    s1, s2, s3, s4, s5, s6, norm, own, other, ab1, ab2, ab3, ab4, c1, c2, c3, c4, last, ny, nx,
    load_sem, send_sem, recv_sem, out_sem, core_send, core_recv,
    ab_send, ab_recv, c_send, c_recv, last_send, last_recv, norm_send, norm_recv, ready,
):
    b, rep = lax.axis_index("bngroup"), lax.axis_index("rep")
    z, c = b // 2, b % 2
    xx, yy = rep // 4, rep % 4

    def along(axis, k):
        if axis == "x":
            return {"rep": ((xx + k) % 4) * 4 + yy}
        if axis == "y":
            return {"rep": xx * 4 + (yy + k) % 4}
        return {"bngroup": (b + 2 * k) % GROUP}

    def load(i, src, dst):
        copy = pltpu.make_async_copy(src, dst, load_sem.at[i])
        copy.start()
        return copy

    def load_images(first, apart, images):
        return [load(first + apart * r, images.at[:, r], raw.at[r]) for r in range(SIDE)]

    def raw_rows(r, at):
        value = raw[r, :, :, at].astype(F32)
        value = jnp.concatenate([value, jnp.zeros((IMGS, 1, value.shape[2]), F32)], axis=1)
        return value.reshape(BAND, value.shape[2])

    load_x = load_images(6, 1, x_hbm)
    load_wr = load(1, wr_hbm, wa)

    barrier = pltpu.get_barrier_semaphore()
    for k in range(1, GROUP):
        pl.semaphore_signal(barrier, inc=1, device_id={"bngroup": (b + k) % GROUP}, device_id_type=MESH)
    for axis in "xy":
        for k in range(1, 4):
            pl.semaphore_signal(barrier, inc=1, device_id=along(axis, k), device_id_type=MESH)

    zeros = jnp.zeros((BAND, 3 * MID), BF16)
    taps[0:BAND, :] = zeros
    taps[ROWS + BAND :, :] = zeros
    g2[0:BAND, :] = zeros
    g2[ROWS + BAND :, :] = zeros

    partner = {"bngroup": b + 1 - 2 * c}

    def remote(src, dst, device, sems):
        return pltpu.make_async_remote_copy(
            src_ref=src, dst_ref=dst, send_sem=sems[0], recv_sem=sems[1],
            device_id=device, device_id_type=MESH,
        )

    def share(e, slots):
        sems = (send_sem.at[e], recv_sem.at[e])
        for k in range(1, GROUP):
            remote(slots.at[b], slots.at[b], {"bngroup": (b + k) % GROUP}, sems).start()
        return remote(slots.at[0 : GROUP - 1], slots.at[0 : GROUP - 1], partner, sems)

    CEN, AMP, SHI, INV, SS, GS = range(6)
    OFF = {1: 0, 2: MID, 3: 2 * MID}
    SIZE = {1: MID, 2: MID, 3: WIDE}

    def put(row, which, value):
        rows[row, :, OFF[which] : OFF[which] + SIZE[which]] = value

    def get(row, which, j):
        return rows[row, :, pl.ds(pl.multiple_of(OFF[which] + j * CH, CH), CH)]

    def stats(pre, j, slots, channels):
        at = lanes_at(j)

        def add(r, acc):
            return acc + fold_rows(pre[band_at(r), at])

        mean = total(lax.fori_loop(0, SIDE, add, jnp.zeros((8, CH), F32))) / REAL

        def spread(r, acc):
            off = real_rows(pre[band_at(r), at] - mean)
            return acc + fold_rows(off * off)

        second = total(lax.fori_loop(0, SIDE, spread, jnp.zeros((8, CH), F32)))
        slots[b, :, at] = mean
        slots[b, :, pl.ds(pl.multiple_of(channels + j * CH, CH), CH)] = second

    def group_stats(slots, which):
        c = SIZE[which]
        mean = slots[0, :, 0:c]
        for i in range(1, GROUP):
            mean = mean + slots[i, :, 0:c]
        mean = mean / GROUP
        second = jnp.zeros((1, c), F32)
        for i in range(GROUP):
            off = slots[i, :, 0:c] - mean
            second = second + (slots[i, :, c : 2 * c] + REAL * (off * off))
        inverse = lax.rsqrt(second / COUNT + EPS)
        put(CEN, which, mean)
        put(INV, which, inverse)
        put(AMP, which, gain_ref[:, OFF[which] : OFF[which] + c] * inverse)
        put(SHI, which, shift_ref[:, OFF[which] : OFF[which] + c])

    def group_sums(slots, which):
        c = SIZE[which]
        sums = slots[0]
        for i in range(1, GROUP):
            sums = sums + slots[i]
        shift_sum, gain_sum = sums[:, 0:c], sums[:, c : 2 * c]
        inverse = rows[INV, :, OFF[which] : OFF[which] + c]
        norm[0:1, OFF[which] : OFF[which] + c] = gain_sum
        norm[1:2, OFF[which] : OFF[which] + c] = shift_sum
        put(SS, which, shift_sum / COUNT)
        put(GS, which, inverse * gain_sum / COUNT)

    for r in range(SIDE):
        load_x[r].wait()

        @pl.loop(0, WIDE // CH)
        def _(j, r=r):
            x[r * BAND : (r + 1) * BAND, lanes_at(j)] = raw_rows(r, lanes_at(j)).astype(BF16)

    load_wr.wait()
    load_ws = load(2, ws_hbm, ws)
    load_images(4, 0, cot_hbm)
    @pl.loop(0, MID // CH)
    def _(j):
        pre1[:, lanes_at(j)] = dot(x[...], wa[:, lanes_at(j)])
        stats(pre1, j, s1, MID)

    load_we = load(3, we_hbm, wa)
    pl.semaphore_wait(barrier, GROUP - 1 + 6)
    share(0, s1).wait()
    group_stats(s1, 1)

    @pl.loop(0, MID // CH)
    def _(j):
        cen, amp, shi = get(CEN, 1, j), get(AMP, 1, j), get(SHI, 1, j)

        @pl.loop(0, SIDE)
        def _(r):
            normed = (pre1[band_at(r), lanes_at(j)] - cen) * amp + shi
            hidden = real_rows(normed * sigmoid(normed))
            tiles = hidden.reshape(IMGS, 8, CH)
            to = pl.ds(pl.multiple_of((r + 1) * BAND, BAND), BAND)
            for tap, shifted in enumerate((pltpu.roll(tiles, 1, 1), tiles, pltpu.roll(tiles, 7, 1))):
                at = pl.ds(pl.multiple_of(tap * MID + j * CH, CH), CH)
                taps[to, at] = shifted.reshape(BAND, CH).astype(BF16)

    load_ws.wait()

    @pl.loop(0, MID // CH)
    def _(j):
        acc = dot(taps[0:ROWS, :], ws[0 : 3 * MID, lanes_at(j)])
        acc = acc + dot(taps[BAND : ROWS + BAND, :], ws[3 * MID : 6 * MID, lanes_at(j)])
        acc = acc + dot(taps[2 * BAND :, :], ws[6 * MID :, lanes_at(j)])
        pre2[:, lanes_at(j)] = real_rows(acc)
        stats(pre2, j, s2, MID)

    sums = share(1, s2)

    @pl.loop(0, 9)
    def _(tap):
        at = pl.ds(pl.multiple_of(tap * MID, MID), MID)
        ws[at, :] = ws[at, :].T

    sums.wait()
    group_stats(s2, 2)

    @pl.loop(0, MID // CH)
    def _(j):
        cen, amp, shi = get(CEN, 2, j), get(AMP, 2, j), get(SHI, 2, j)

        @pl.loop(0, SIDE)
        def _(r):
            normed = (pre2[band_at(r), lanes_at(j)] - cen) * amp + shi
            h2[band_at(r), lanes_at(j)] = real_rows(normed * sigmoid(normed)).astype(BF16)

    load_we.wait()

    @pl.loop(0, WIDE // CH)
    def _(j):
        pre3[:, lanes_at(j)] = dot(h2[...], wa[lanes_at(j), :], ((1,), (1,)))
        stats(pre3, j, s3, WIDE)

    share(2, s3).wait()
    group_stats(s3, 3)
    pltpu.make_async_copy(raw, raw, load_sem.at[4]).wait()

    @pl.loop(0, WIDE // CH)
    def _(j):
        at = lanes_at(j)
        cen, amp, shi, inv = get(CEN, 3, j), get(AMP, 3, j), get(SHI, 3, j), get(INV, 3, j)

        def add(r, acc):
            band = band_at(r)
            centred = pre3[band, at] - cen
            summed = centred * amp + shi + x[band, at].astype(F32)
            sigma = sigmoid(summed)
            upstream = raw_rows(r, at) * (sigma * (1.0 + summed * (1.0 - sigma)))
            g3[band, at] = (summed * sigma).astype(BF16)
            up[band, at] = upstream
            pre3[band, at] = centred
            return (acc[0] + fold_rows(upstream), acc[1] + fold_rows(upstream * centred))

        zero = jnp.zeros((8, CH), F32)
        shift_sum, gain_sum = lax.fori_loop(0, SIDE, add, (zero, zero))
        s4[b, :, at] = total(shift_sum)
        s4[b, :, pl.ds(pl.multiple_of(WIDE + j * CH, CH), CH)] = total(gain_sum) * inv

    def turn(value):
        halves = value.T.reshape(16, 2, 16, ROWS)
        for half in range(2):
            turned[(half + c + 1) % 2] = halves[:, half].reshape(MID // 2, ROWS)

    def landing(piece, at):
        if piece == "expand":
            return pre3.at[0:256, at]
        if piece in ("upper", "first"):
            return pre3.at[256:512, at]
        return other.at[:, at]

    names = list(PIECES)

    def to_partner(piece, i):
        chunk = PIECES[piece][2]
        at = pl.ds(pl.multiple_of(LANDING[piece] + i * MID, MID), MID)
        slot = (chunk + i) % SLOTS
        sems = (core_send.at[slot], core_recv.at[names.index(piece)])
        return remote(stage.at[slot], landing(piece, at), partner, sems)

    def slot_free(n):
        remote(stage.at[n % SLOTS], other.at[:, 0:MID], partner, (core_send.at[n % SLOTS], core_recv.at[0])).wait_send()

    def weigh(piece, right):
        lane, size, chunk, count = PIECES[piece]

        @pl.loop(0, count)
        def _(i):
            slot = (chunk + i) % SLOTS
            if chunk >= SLOTS:
                slot_free(chunk + i - SLOTS)
            for half in range(MID // CH):
                product = dot(turned[...].reshape(MID, ROWS), right(i, half))
                stage[slot, :, half * CH : (half + 1) * CH] = product[: MID // 2]
                at = pl.ds(pl.multiple_of(lane + i * MID + half * CH, CH), CH)
                own[:, :, :, at] = product[MID // 2 :].reshape(4, 4, 16, CH)
            to_partner(piece, i).start()

    flying = {}

    def send(src, dst, device, sems):
        remote(src, dst, device, sems).start()

    def plus(k, base):
        return (base + k) % 4

    def step(piece, n):
        lane, size, chunk, count = PIECES[piece]
        width, ab_at, c_at = SHARE[piece]
        p = names.index(piece)
        half = width // 2
        if n == 0:
            landed = landing(piece, pl.ds(LANDING[piece], size))
            remote(landed, landed, partner, (core_send.at[0], core_recv.at[p])).wait_recv()

            @pl.loop(0, 16)
            def _(k):
                own[k // 4, k % 4, :, lane : lane + size] += landed[pl.ds(pl.multiple_of(k * 16, 16), 16), :]

        else:
            for copy in flying.pop((piece, n - 1)):
                copy.wait()
        if n < 4:
            ab_sems, c_sems = (ab_send.at[p, n], ab_recv.at[p, n]), (c_send.at[p, n], c_recv.at[p, n])
        for color in range(2):
            span = pl.ds(lane + color * width, width)
            local = pl.ds(ab_at, width)
            axes = "xy" if color == 0 else "yx"
            outer, inner = (xx, yy) if color == 0 else (yy, xx)
            parts = [pl.ds(lane + color * width + k * half, half) for k in range(2)]
            local_part = pl.ds(ab_at // 2, half)

            def outer_block(index, part=slice(None), color=color, span=span):
                return own.at[index, part, :, span] if color == 0 else own.at[part, index, :, span]

            def inner_block(index, part, color=color, outer=outer):
                return own.at[outer, index, :, part] if color == 0 else own.at[index, outer, :, part]

            if n == 0:
                far = plus(2, outer)
                send(outer_block(far, slice(0, 2)), ab1.at[color, 0, :, :, local], along(axes[0], 1), ab_sems)
                send(outer_block(far, slice(2, 4)), ab1.at[color, 1, :, :, local], along(axes[0], 3), ab_sems)
            elif n == 1:
                low = outer_block(plus(1, outer), slice(0, 2))
                low[...] += ab1[color, 0, :, :, local]
                high = outer_block(plus(3, outer), slice(2, 4))
                high[...] += ab1[color, 1, :, :, local]
                send(outer_block(plus(1, outer)), ab2.at[color, 0, :, :, local], along(axes[0], 1), ab_sems)
                send(outer_block(plus(3, outer)), ab2.at[color, 1, :, :, local], along(axes[0], 3), ab_sems)
            elif n == 2:
                mine = outer_block(outer)
                mine[...] += ab2[color, 0, :, :, local] + ab2[color, 1, :, :, local]
                far = plus(2, inner)
                send(inner_block(far, parts[0]), ab3.at[color, 0, :, local_part], along(axes[1], 1), ab_sems)
                send(inner_block(far, parts[1]), ab3.at[color, 1, :, local_part], along(axes[1], 3), ab_sems)
            elif n == 3:
                low = inner_block(plus(1, inner), parts[0])
                low[...] += ab3[color, 0, :, local_part]
                high = inner_block(plus(3, inner), parts[1])
                high[...] += ab3[color, 1, :, local_part]
                send(inner_block(plus(1, inner), span), ab4.at[color, 0, :, local], along(axes[1], 1), ab_sems)
                send(inner_block(plus(3, inner), span), ab4.at[color, 1, :, local], along(axes[1], 3), ab_sems)
            else:
                mine = inner_block(inner, span)
                mine[...] += ab4[color, 0, :, local] + ab4[color, 1, :, local]

        base = lane + 2 * width
        local = pl.ds(c_at, 128)

        def tile(index):
            return pl.ds(pl.multiple_of(base + 128 * index, 128), 128)

        first_axis = "x" if p % 2 == 0 else "y"
        second_axis = "y" if p % 2 == 0 else "x"
        if n == 0:
            far = tile(plus(2, z))
            send(own.at[0:2, :, :, far], c1.at[0, :, :, :, local], along("z", 1), c_sems)
            send(own.at[2:4, :, :, far], c1.at[1, :, :, :, local], along("z", 3), c_sems)
        elif n == 1:
            up_one, down_one = tile(plus(1, z)), tile(plus(3, z))
            own[0:2, :, :, up_one] += c1[0, :, :, :, local]
            own[2:4, :, :, down_one] += c1[1, :, :, :, local]
            send(own.at[:, :, :, up_one], c2.at[0, :, :, :, local], along("z", 1), c_sems)
            send(own.at[:, :, :, down_one], c2.at[1, :, :, :, local], along("z", 3), c_sems)
        elif n == 2:
            own[:, :, :, tile(z)] += c2[0, :, :, :, local] + c2[1, :, :, :, local]
            for k in range(1, 4):
                block_of = own.at[plus(k, xx), :, :, tile(z)] if p % 2 == 0 else own.at[:, plus(k, yy), :, tile(z)]
                send(block_of, c3.at[k - 1, :, :, local], along(first_axis, k), c_sems)
        elif n == 3:
            mine = own.at[xx, :, :, tile(z)] if p % 2 == 0 else own.at[:, yy, :, tile(z)]
            mine[...] += c3[0, :, :, local] + c3[1, :, :, local] + c3[2, :, :, local]
            for k in range(1, 4):
                block_of = own.at[xx, plus(k, yy), :, tile(z)] if p % 2 == 0 else own.at[plus(k, xx), yy, :, tile(z)]
                send(block_of, c4.at[k - 1, :, local], along(second_axis, k), c_sems)
        else:
            mine = own[xx, yy, :, tile(z)] + c4[0, :, local] + c4[1, :, local] + c4[2, :, local]
            own[xx, yy, :, base : base + 512] = jnp.zeros((16, 512), F32)
            own[xx, yy, :, tile(z)] = mine
        if n < 4:
            ab_local = pl.ds(ab_at // 2, half) if n == 2 else pl.ds(ab_at, width)
            ab, third = (ab1, ab2, ab3, ab4)[n], (c1, c2, c3, c4)[n]
            ab_whole = ab.at[:, :, :, :, ab_local] if n < 2 else ab.at[:, :, :, ab_local]
            c_whole = third.at[:, :, :, :, local] if n < 2 else third.at[:, :, :, local] if n == 2 else third.at[:, :, local]
            flying[piece, n] = [remote(ab_whole, ab_whole, partner, ab_sems), remote(c_whole, c_whole, partner, c_sems)]

    def owned(device):
        return pl.ds(pl.multiple_of((device // 2) * ZBLOCK + (device % 2) * 1024, 128), OWN)

    last_sems = (last_send.at[0], last_recv.at[0])

    def to_owner(t):
        return remote(own.at[xx, yy, :, owned(t)], last.at[b], {"bngroup": t}, last_sems)

    def to_owners(targets):
        for t in targets:

            @pl.when(b != t)
            def _(t=t):
                to_owner(t).start()

    def gather(n, axis, slots, mine):
        sems = (norm_send.at[n], norm_recv.at[n])
        for k in range(1, 4):
            send(slots.at[mine], slots.at[mine], along(axis, k), sems)
        return remote(slots.at[0:3], slots.at[0:3], partner, sems)

    def sum_of(slots):
        return slots[0] + slots[1] + slots[2] + slots[3]

    sums = share(3, s4)
    write_out = pltpu.make_async_copy(g3, out_hbm, out_sem.at[0])
    write_out.start()
    turn(h2[...])
    sums.wait()
    group_sums(s4, 3)
    write_out.wait()

    @pl.loop(0, WIDE // CH)
    def _(j):
        at = lanes_at(j)
        amp, ss, gs = get(AMP, 3, j), get(SS, 3, j), get(GS, 3, j)

        @pl.loop(0, SIDE)
        def _(r):
            band = band_at(r)
            grad = amp * (up[band, at] - ss - pre3[band, at] * gs)
            g3[band, at] = real_rows(grad).astype(BF16)

    def slope_sums(pre, which, j, slots):
        at = lanes_at(j)
        cen, amp, shi, inv = get(CEN, which, j), get(AMP, which, j), get(SHI, which, j), get(INV, which, j)

        def add(r, acc):
            band = band_at(r)
            centred = pre[band, at] - cen
            normed = centred * amp + shi
            sigma = sigmoid(normed)
            value = real_rows(back[band, at] * (sigma * (1.0 + normed * (1.0 - sigma))))
            back[band, at] = value
            return (acc[0] + fold_rows(value), acc[1] + fold_rows(value * centred))

        zero = jnp.zeros((8, CH), F32)
        shift_sum, gain_sum = lax.fori_loop(0, SIDE, add, (zero, zero))
        slots[b, :, at] = total(shift_sum)
        slots[b, :, pl.ds(pl.multiple_of(MID + j * CH, CH), CH)] = total(gain_sum) * inv

    def norm_back(pre, which, j, r):
        at, band = lanes_at(j), band_at(r)
        cen, amp, ss, gs = get(CEN, which, j), get(AMP, which, j), get(SS, which, j), get(GS, which, j)
        return real_rows(amp * (back[band, at] - ss - (pre[band, at] - cen) * gs))

    pl.semaphore_signal(ready, inc=1, device_id={"bngroup": b + 1 - 2 * c}, device_id_type=MESH)
    pl.semaphore_wait(ready, 1)
    weigh("expand", lambda i, half: g3[:, pl.ds(pl.multiple_of(i * MID + half * CH, CH), CH)])
    @pl.loop(0, MID // CH)
    def _(j):
        back[:, lanes_at(j)] = dot(g3[...], wa[:, lanes_at(j)])
        slope_sums(pre2, 2, j, s5)

    sums = share(4, s5)
    load_wr = load(5, wr_hbm, wa)

    step("expand", 0)
    sums.wait()
    group_sums(s5, 2)

    @pl.loop(0, MID // CH)
    def _(j):
        @pl.loop(0, SIDE)
        def _(r):
            grad = norm_back(pre2, 2, j, r)
            tiles = grad.reshape(IMGS, 8, CH)
            to = pl.ds(pl.multiple_of((r + 1) * BAND, BAND), BAND)
            for tap, shifted in enumerate((pltpu.roll(tiles, 7, 1), tiles, pltpu.roll(tiles, 1, 1))):
                at = pl.ds(pl.multiple_of(tap * MID + j * CH, CH), CH)
                g2[to, at] = shifted.reshape(BAND, CH).astype(BF16)

    def tap_row(row):
        return lambda i, half: taps[
            row * BAND : row * BAND + ROWS,
            pl.ds(pl.multiple_of(i * MID + half * CH, CH), CH),
        ]

    def back_one(j):
        acc = None
        for row in range(3):
            left = g2[(2 - row) * BAND : (2 - row) * BAND + ROWS, :]
            part = dot(left, ws[3 * MID * row : 3 * MID * (row + 1), j * CH : (j + 1) * CH])
            acc = part if acc is None else acc + part
        back[:, j * CH : (j + 1) * CH] = acc
        slope_sums(pre1, 1, j, s6)

    def input_gradient(quarter):
        @pl.loop(2 * quarter, 2 * quarter + 2)
        def _(j):
            at = lanes_at(j)
            g3[:, at] = (up[:, at] + dot(h2[...], wa[at, :], ((1,), (1,)))).astype(BF16)

    turn(g2[BAND : ROWS + BAND, MID : 2 * MID])
    weigh("low", tap_row(0))
    step("expand", 1)
    weigh("mid", tap_row(1))
    step("low", 0)
    weigh("high", tap_row(2))
    step("mid", 0)
    back_one(0)
    step("high", 0)
    step("expand", 2)
    step("low", 1)
    back_one(1)
    sums = share(5, s6)
    step("mid", 1)
    step("high", 1)
    step("expand", 3)
    step("low", 2)
    sums.wait()
    group_sums(s6, 1)
    ny[yy] = norm[...]
    norm_copies = gather(0, "y", ny, yy)

    @pl.loop(0, MID // CH)
    def _(j):
        @pl.loop(0, SIDE)
        def _(r):
            h2[band_at(r), lanes_at(j)] = norm_back(pre1, 1, j, r).astype(BF16)

    turn(h2[...])
    weigh("upper", lambda i, half: x[:, pl.ds(pl.multiple_of(1024 + i * MID + half * CH, CH), CH)])
    weigh("first", lambda i, half: x[:, pl.ds(pl.multiple_of(i * MID + half * CH, CH), CH)])
    step("upper", 0)
    step("mid", 2)
    step("first", 0)
    load_wr.wait()
    input_gradient(0)
    step("high", 2)
    step("expand", 4)
    step("upper", 1)
    input_gradient(1)
    step("low", 3)
    step("first", 1)
    input_gradient(2)
    step("mid", 3)
    step("upper", 2)
    step("low", 4)
    step("high", 3)
    input_gradient(3)
    write_in = pltpu.make_async_copy(g3, ing_hbm, out_sem.at[1])
    write_in.start()
    step("first", 2)
    norm_copies.wait()
    nx[xx] = sum_of(ny)
    norm_copies = gather(1, "x", nx, xx)
    step("mid", 4)
    step("upper", 3)
    step("high", 4)
    to_owners(range(2, GROUP))
    step("first", 3)
    step("upper", 4)
    to_owners(range(1, 2))
    step("first", 4)
    to_owners(range(1))
    last[b] = own[xx, yy, :, owned(b)]

    norm_copies.wait()
    norm_out[...] = sum_of(nx) * (1.0 / IMAGES)
    write_in.wait()
    for n in range(13, 17):
        slot_free(n)
    remote(last.at[0 : GROUP - 1], last.at[0 : GROUP - 1], partner, last_sems).wait()

    parts = []
    for core in range(2):
        parts.append(last[core] + last[2 + core] + last[4 + core] + last[6 + core])
    whole = jnp.concatenate(parts, axis=0) * (1.0 / IMAGES)
    moved = pltpu.roll(whole, OWN - 64, 1)
    wg_ref[...] = jnp.where(c == 1, moved, whole)[:, : LANES // 8]


def run_block(x, cot, wr, ws, we, gain, shift):
    any_ = pl.BlockSpec(memory_space=pl.ANY)
    vmem = pl.BlockSpec(memory_space=pltpu.VMEM)
    v = pltpu.VMEM
    dma = pltpu.SemaphoreType.DMA
    pieces = len(PIECES)
    return pl.pallas_call(
        block,
        out_shape=(
            jax.ShapeDtypeStruct((ROWS, WIDE), BF16),
            jax.ShapeDtypeStruct((ROWS, WIDE), BF16),
            jax.ShapeDtypeStruct((32, LANES // 8), F32),
            jax.ShapeDtypeStruct((2, 3072), F32),
        ),
        in_specs=[any_] * 5 + [vmem] * 2,
        out_specs=(any_, any_, vmem, vmem),
        scratch_shapes=[
            v((ROWS, WIDE), BF16),
            v((SIDE, IMGS, SIDE, WIDE), BF16),
            v((WIDE, MID), BF16),
            v((9 * MID, MID), BF16),
            v((ROWS, MID), F32),
            v((ROWS + 2 * BAND, 3 * MID), BF16),
            v((ROWS, MID), F32),
            v((ROWS, MID), BF16),
            v((ROWS, WIDE), F32),
            v((ROWS, WIDE), F32),
            v((ROWS, WIDE), BF16),
            v((ROWS + 2 * BAND, 3 * MID), BF16),
            v((ROWS, MID), F32),
            v((2, MID // 2, ROWS), BF16),
            v((SLOTS, MID // 2, MID), F32),
            v((6, 1, 3072), F32),
            v((GROUP, 1, 2 * MID), F32),
            v((GROUP, 1, 2 * MID), F32),
            v((GROUP, 1, 2 * WIDE), F32),
            v((GROUP, 1, 2 * WIDE), F32),
            v((GROUP, 1, 2 * MID), F32),
            v((GROUP, 1, 2 * MID), F32),
            v((2, 3072), F32),
            v((4, 4, 16, LANES), F32),
            v((MID // 2, 9 * MID), F32),
            v((2, 2, 2, 16, AB_LANES), F32),
            v((2, 2, 4, 16, AB_LANES), F32),
            v((2, 2, 16, AB_LANES // 2), F32),
            v((2, 2, 16, AB_LANES), F32),
            v((2, 2, 4, 16, C_LANES), F32),
            v((2, 4, 4, 16, C_LANES), F32),
            v((3, 4, 16, C_LANES), F32),
            v((3, 16, C_LANES), F32),
            v((GROUP, 16, OWN), F32),
            v((4, 2, 3072), F32),
            v((4, 2, 3072), F32),
            dma((6 + SIDE,)),
            dma((6,)),
            dma((6,)),
            dma((2,)),
            dma((SLOTS,)),
            dma((pieces,)),
            dma((pieces, 4)),
            dma((pieces, 4)),
            dma((pieces, 4)),
            dma((pieces, 4)),
            dma((1,)),
            dma((1,)),
            dma((2,)),
            dma((2,)),
            pltpu.SemaphoreType.REGULAR,
        ],
        compiler_params=pltpu.CompilerParams(
            collective_id=0, has_side_effects=True, vmem_limit_bytes=VMEM_LIMIT
        ),
        cost_estimate=pl.CostEstimate(flops=18 * 10**9, bytes_accessed=4 * 10**7, transcendentals=10**7),
        name="block",
    )(x, cot, wr, ws, we, gain, shift)


def from_rows(rows):
    return rows.reshape(SIDE, IMGS, COLS, WIDE)[:, :, :SIDE].transpose(1, 0, 2, 3)


def per_device(images, cotangent, w_reduce, w_spatial, w_expand, norm_gain, norm_shift):
    output, in_grad, grads, norm_grads = run_block(
        images, cotangent, w_reduce, w_spatial, w_expand,
        norm_gain.reshape(1, -1), norm_shift.reshape(1, -1),
    )
    return (from_rows(output), from_rows(in_grad), grads.T, norm_grads)


def solution(mesh):
    both = P(("bngroup", "rep"), None, None, None)
    return jax.shard_map(
        per_device,
        mesh=mesh,
        in_specs=(both, both, P(), P(), P(), P(), P()),
        out_specs=(both, both, P("bngroup", "rep"), P()),
        check_vma=False,
    )
```

```python
import jax
import jax.numpy as jnp
from jax import lax
from jax.experimental import pallas as pl
from jax.experimental.pallas import tpu as pltpu
from jax.sharding import PartitionSpec as P

MESH = pl.DeviceIdType.MESH
F32 = jnp.float32
BF16 = jnp.bfloat16

IMGS, SIDE, COLS = 12, 7, 8
WIDE, MID = 2048, 512
BAND = IMGS * COLS
ROWS = SIDE * BAND
REAL = IMGS * SIDE * SIDE
GROUP = 8
COUNT = float(REAL * GROUP)
IMAGES = 1536.0
EPS = 0.25
CH = 256
LANES = 2 * WIDE + 9 * MID
ZBLOCK = LANES // 4
OWN = 1152
VMEM_LIMIT = 67043328
SLOTS = 4

PIECES = {
    "expand": (6656, 1024, 0, 2),
    "extra": (7680, 1024, 2, 2),
    "low": (2048, 1536, 4, 3),
    "mid": (3584, 1536, 7, 3),
    "high": (5120, 1536, 10, 3),
    "upper": (1024, 1024, 13, 2),
    "first": (0, 1024, 15, 2),
}
LANDING = {"expand": 0, "extra": 1024, "low": 0, "mid": 1536, "high": 3072, "upper": 1024, "first": 0}
THIRD = {"expand": 1, "low": 1, "mid": 1, "high": 1, "upper": 1, "first": 1}
DIRECT = ("upper", "first",)
SHARE = {}
_ab, _c, _d = 0, 0, 0
for _name, (_lane, _size, _, _) in PIECES.items():
    _n = (_size - 512 * THIRD.get(_name, 0)) // 2
    SHARE[_name] = (_n, _ab, _c, _d)
    _ab, _c, _d = _ab + _n, _c + 128 * THIRD.get(_name, 0), _d + (_n if _name in DIRECT else 0)
EVEN = (0, 2, 4, 6)
D_LANES = _d
AB_LANES, C_LANES = _ab, _c


def dot(left, right, dims=((1,), (0,))):
    return lax.dot_general(left, right, (dims, ((), ())), preferred_element_type=F32)


def sigmoid(value):
    return 0.5 * jnp.tanh(0.5 * value) + 0.5


def real_rows(value):
    rows, lanes = value.shape
    tiles = value.reshape(rows // 8, 8, lanes)
    column = lax.broadcasted_iota(jnp.int32, tiles.shape, 1)
    return jnp.where(column != 7, tiles, 0.0).reshape(rows, lanes)


def fold_rows(value):
    rows, lanes = value.shape
    return jnp.sum(value.reshape(rows // 8, 8, lanes), axis=0)


def total(folded):
    return jnp.sum(folded, axis=0, keepdims=True)


def lanes_at(j, size=CH):
    return pl.ds(pl.multiple_of(j * size, size), size)


def band_at(r):
    return pl.ds(pl.multiple_of(r * BAND, BAND), BAND)


def block(
    x_hbm, cot_hbm, wr_hbm, ws_hbm, we_hbm, gain_ref, shift_ref,
    out_hbm, ing_hbm, wg_ref, norm_out,
    x, raw, wa, ws, pre1, taps, pre2, h2, pre3, up, g3, g2, back, turned, stage, rows,
    s1, s2, s3, s4, s5, s6, norm, own, other, ab1, ab2, ab3, ab4, straight, c1, c2, c3, c4, last, ny, nx,
    load_sem, send_sem, recv_sem, out_sem, core_send, core_recv,
    ab_send, ab_recv, c_send, c_recv, last_send, last_recv, norm_send, norm_recv, ready,
):
    b, rep = lax.axis_index("bngroup"), lax.axis_index("rep")
    z, c = b // 2, b % 2
    xx, yy = rep // 4, rep % 4

    def along(axis, k):
        if axis == "x":
            return {"rep": ((xx + k) % 4) * 4 + yy}
        if axis == "y":
            return {"rep": xx * 4 + (yy + k) % 4}
        return {"bngroup": (b + 2 * k) % GROUP}

    def load(i, src, dst):
        copy = pltpu.make_async_copy(src, dst, load_sem.at[i])
        copy.start()
        return copy

    def load_images(first, apart, images):
        return [load(first + apart * r, images.at[:, r], raw.at[r]) for r in range(SIDE)]

    def raw_rows(r, at):
        value = raw[r, :, :, at].astype(F32)
        value = jnp.concatenate([value, jnp.zeros((IMGS, 1, value.shape[2]), F32)], axis=1)
        return value.reshape(BAND, value.shape[2])

    load_x = load_images(6, 1, x_hbm)
    load_wr = load(1, wr_hbm, wa)

    barrier = pltpu.get_barrier_semaphore()
    for k in range(1, GROUP):
        pl.semaphore_signal(barrier, inc=1, device_id={"bngroup": (b + k) % GROUP}, device_id_type=MESH)
    for axis in "xy":
        for k in range(1, 4):
            pl.semaphore_signal(barrier, inc=1, device_id=along(axis, k), device_id_type=MESH)

    zeros = jnp.zeros((BAND, 3 * MID), BF16)
    taps[0:BAND, :] = zeros
    taps[ROWS + BAND :, :] = zeros
    g2[0:BAND, :] = zeros
    g2[ROWS + BAND :, :] = zeros

    partner = {"bngroup": b + 1 - 2 * c}

    def remote(src, dst, device, sems):
        return pltpu.make_async_remote_copy(
            src_ref=src, dst_ref=dst, send_sem=sems[0], recv_sem=sems[1],
            device_id=device, device_id_type=MESH,
        )

    def share(e, slots):
        sems = (send_sem.at[e], recv_sem.at[e])
        for k in range(1, GROUP):
            remote(slots.at[b], slots.at[b], {"bngroup": (b + k) % GROUP}, sems).start()
        return remote(slots.at[0 : GROUP - 1], slots.at[0 : GROUP - 1], partner, sems)

    CEN, AMP, SHI, INV, SS, GS = range(6)
    OFF = {1: 0, 2: MID, 3: 2 * MID}
    SIZE = {1: MID, 2: MID, 3: WIDE}

    def put(row, which, value):
        rows[row, :, OFF[which] : OFF[which] + SIZE[which]] = value

    def get(row, which, j):
        return rows[row, :, pl.ds(pl.multiple_of(OFF[which] + j * CH, CH), CH)]

    def stats(value, j, slots, channels):
        about = total(value[0:8]) / 7.0
        off = real_rows(value - about)
        first, second = total(fold_rows(off)) / REAL, total(fold_rows(off * off))
        slots[b, :, lanes_at(j)] = about + first
        at = pl.ds(pl.multiple_of(channels + j * CH, CH), CH)
        slots[b, :, at] = jnp.maximum(second - REAL * (first * first), 0.0)

    def group_stats(slots, which):
        c = SIZE[which]
        mean = slots[0, :, 0:c]
        for i in range(1, GROUP):
            mean = mean + slots[i, :, 0:c]
        mean = mean / GROUP
        second = jnp.zeros((1, c), F32)
        for i in range(GROUP):
            off = slots[i, :, 0:c] - mean
            second = second + (slots[i, :, c : 2 * c] + REAL * (off * off))
        inverse = lax.rsqrt(second / COUNT + EPS)
        put(CEN, which, mean)
        put(INV, which, inverse)
        put(AMP, which, gain_ref[:, OFF[which] : OFF[which] + c] * inverse)
        put(SHI, which, shift_ref[:, OFF[which] : OFF[which] + c])

    def group_sums(slots, which):
        c = SIZE[which]
        sums = slots[0]
        for i in range(1, GROUP):
            sums = sums + slots[i]
        shift_sum, gain_sum = sums[:, 0:c], sums[:, c : 2 * c]
        inverse = rows[INV, :, OFF[which] : OFF[which] + c]
        norm[0:1, OFF[which] : OFF[which] + c] = gain_sum
        norm[1:2, OFF[which] : OFF[which] + c] = shift_sum
        put(SS, which, shift_sum / COUNT)
        put(GS, which, inverse * gain_sum / COUNT)

    for r in range(SIDE):
        load_x[r].wait()

        @pl.loop(0, WIDE // CH)
        def _(j, r=r):
            x[r * BAND : (r + 1) * BAND, lanes_at(j)] = raw_rows(r, lanes_at(j)).astype(BF16)

    load_wr.wait()
    load_ws = load(2, ws_hbm, ws)
    load_images(4, 0, cot_hbm)
    @pl.loop(0, MID // CH)
    def _(j):
        value = dot(x[...], wa[:, lanes_at(j)])
        pre1[:, lanes_at(j)] = value
        stats(value, j, s1, MID)

    load_we = load(3, we_hbm, wa)
    pl.semaphore_wait(barrier, GROUP - 1 + 6)
    share(0, s1).wait()
    group_stats(s1, 1)

    @pl.loop(0, MID // CH)
    def _(j):
        cen, amp, shi = get(CEN, 1, j), get(AMP, 1, j), get(SHI, 1, j)

        @pl.loop(0, SIDE)
        def _(r):
            normed = (pre1[band_at(r), lanes_at(j)] - cen) * amp + shi
            hidden = real_rows(normed * sigmoid(normed))
            tiles = hidden.reshape(IMGS, 8, CH)
            to = pl.ds(pl.multiple_of((r + 1) * BAND, BAND), BAND)
            for tap, shifted in enumerate((pltpu.roll(tiles, 1, 1), tiles, pltpu.roll(tiles, 7, 1))):
                at = pl.ds(pl.multiple_of(tap * MID + j * CH, CH), CH)
                taps[to, at] = shifted.reshape(BAND, CH).astype(BF16)

    load_ws.wait()

    @pl.loop(0, MID // CH)
    def _(j):
        acc = dot(taps[0:ROWS, :], ws[0 : 3 * MID, lanes_at(j)])
        acc = acc + dot(taps[BAND : ROWS + BAND, :], ws[3 * MID : 6 * MID, lanes_at(j)])
        acc = acc + dot(taps[2 * BAND :, :], ws[6 * MID :, lanes_at(j)])
        value = real_rows(acc)
        pre2[:, lanes_at(j)] = value
        stats(value, j, s2, MID)

    sums = share(1, s2)

    @pl.loop(0, 9)
    def _(tap):
        at = pl.ds(pl.multiple_of(tap * MID, MID), MID)
        ws[at, :] = ws[at, :].T

    sums.wait()
    group_stats(s2, 2)

    @pl.loop(0, MID // CH)
    def _(j):
        cen, amp, shi = get(CEN, 2, j), get(AMP, 2, j), get(SHI, 2, j)

        @pl.loop(0, SIDE)
        def _(r):
            normed = (pre2[band_at(r), lanes_at(j)] - cen) * amp + shi
            h2[band_at(r), lanes_at(j)] = real_rows(normed * sigmoid(normed)).astype(BF16)

    load_we.wait()

    @pl.loop(0, WIDE // CH)
    def _(j):
        value = dot(h2[...], wa[lanes_at(j), :], ((1,), (1,)))
        pre3[:, lanes_at(j)] = value
        stats(value, j, s3, WIDE)

    share(2, s3).wait()
    group_stats(s3, 3)
    pltpu.make_async_copy(raw, raw, load_sem.at[4]).wait()

    @pl.loop(0, WIDE // CH)
    def _(j):
        at = lanes_at(j)
        cen, amp, shi, inv = get(CEN, 3, j), get(AMP, 3, j), get(SHI, 3, j), get(INV, 3, j)

        def add(r, acc):
            band = band_at(r)
            centred = pre3[band, at] - cen
            summed = centred * amp + shi + x[band, at].astype(F32)
            sigma = sigmoid(summed)
            value = summed * sigma
            upstream = raw_rows(r, at) * (sigma + value * (1.0 - sigma))
            g3[band, at] = value.astype(BF16)
            up[band, at] = upstream
            pre3[band, at] = centred
            return (acc[0] + fold_rows(upstream), acc[1] + fold_rows(upstream * centred))

        zero = jnp.zeros((8, CH), F32)
        shift_sum, gain_sum = lax.fori_loop(0, SIDE, add, (zero, zero))
        s4[b, :, at] = total(shift_sum)
        s4[b, :, pl.ds(pl.multiple_of(WIDE + j * CH, CH), CH)] = total(gain_sum) * inv

    def turn(value):
        halves = value.T.reshape(16, 2, 16, ROWS)
        for half in range(2):
            turned[(half + c + 1) % 2] = halves[:, half].reshape(MID // 2, ROWS)

    def landing(piece, at):
        if piece in ("expand", "extra"):
            return pre3.at[0:256, at]
        if piece in ("upper", "first"):
            return pre3.at[256:512, at]
        return other.at[:, at]

    names = list(PIECES)

    def to_partner(piece, i):
        chunk = PIECES[piece][2]
        at = pl.ds(pl.multiple_of(LANDING[piece] + i * MID, MID), MID)
        slot = (chunk + i) % SLOTS
        sems = (core_send.at[slot], core_recv.at[names.index(piece)])
        return remote(stage.at[slot], landing(piece, at), partner, sems)

    def slot_free(n):
        remote(stage.at[n % SLOTS], other.at[:, 0:MID], partner, (core_send.at[n % SLOTS], core_recv.at[0])).wait_send()

    def weigh(piece, right):
        lane, size, chunk, count = PIECES[piece]

        @pl.loop(0, count)
        def _(i):
            slot = (chunk + i) % SLOTS
            if chunk >= SLOTS:
                slot_free(chunk + i - SLOTS)
            for half in range(MID // CH):
                product = dot(turned[...].reshape(MID, ROWS), right(i, half))
                stage[slot, :, half * CH : (half + 1) * CH] = product[: MID // 2]
                at = pl.ds(pl.multiple_of(lane + i * MID + half * CH, CH), CH)
                own[:, :, :, at] = product[MID // 2 :].reshape(4, 4, 16, CH)
            to_partner(piece, i).start()

    flying = {}

    def send(src, dst, device, sems):
        remote(src, dst, device, sems).start()

    def plus(k, base):
        return (base + k) % 4

    def step(piece, n):
        lane, size, chunk, count = PIECES[piece]
        width, ab_at, c_at, d_at = SHARE[piece]
        direct = piece in DIRECT
        p = names.index(piece)
        half = width // 2
        if n == 0:
            landed = landing(piece, pl.ds(LANDING[piece], size))
            remote(landed, landed, partner, (core_send.at[0], core_recv.at[p])).wait_recv()

            @pl.loop(0, 16)
            def _(k):
                own[k // 4, k % 4, :, lane : lane + size] += landed[pl.ds(pl.multiple_of(k * 16, 16), 16), :]

        else:
            flying.pop((piece, n - 1)).wait()
        if n < 4:
            sems = (ab_send.at[p], ab_recv.at[p, n])
        for color in range(2):
            span = pl.ds(lane + color * width, width)
            local = pl.ds(ab_at, width)
            axes = "xy" if color == 0 else "yx"
            outer, inner = (xx, yy) if color == 0 else (yy, xx)
            parts = [pl.ds(lane + color * width + k * half, half) for k in range(2)]
            local_part = pl.ds(ab_at // 2, half)

            def outer_block(index, part=slice(None), color=color, span=span):
                return own.at[index, part, :, span] if color == 0 else own.at[part, index, :, span]

            def inner_block(index, part, color=color, outer=outer):
                return own.at[outer, index, :, part] if color == 0 else own.at[index, outer, :, part]

            if n == 0:
                far = plus(2, outer)
                send(outer_block(far, slice(0, 2)), ab1.at[color, 0, :, :, local], along(axes[0], 1), sems)
                send(outer_block(far, slice(2, 4)), ab1.at[color, 1, :, :, local], along(axes[0], 3), sems)
            elif n == 1:
                low = outer_block(plus(1, outer), slice(0, 2))
                low[...] += ab1[color, 0, :, :, local]
                high = outer_block(plus(3, outer), slice(2, 4))
                high[...] += ab1[color, 1, :, :, local]
                send(outer_block(plus(1, outer)), ab2.at[color, 0, :, :, local], along(axes[0], 1), sems)
                send(outer_block(plus(3, outer)), ab2.at[color, 1, :, :, local], along(axes[0], 3), sems)
            elif n == 2:
                mine = outer_block(outer)
                mine[...] += ab2[color, 0, :, :, local] + ab2[color, 1, :, :, local]
                if direct:
                    for k in range(1, 4):
                        send(inner_block(plus(k, inner), span), straight.at[color, k - 1, :, pl.ds(d_at, width)], along(axes[1], k), sems)
                    continue
                far = plus(2, inner)
                send(inner_block(far, parts[0]), ab3.at[color, 0, :, local_part], along(axes[1], 1), sems)
                send(inner_block(far, parts[1]), ab3.at[color, 1, :, local_part], along(axes[1], 3), sems)
            elif direct:
                if n == 3:
                    at = pl.ds(d_at, width)
                    mine = inner_block(inner, span)
                    mine[...] += straight[color, 0, :, at] + straight[color, 1, :, at] + straight[color, 2, :, at]
            elif n == 3:
                low = inner_block(plus(1, inner), parts[0])
                low[...] += ab3[color, 0, :, local_part]
                high = inner_block(plus(3, inner), parts[1])
                high[...] += ab3[color, 1, :, local_part]
                send(inner_block(plus(1, inner), span), ab4.at[color, 0, :, local], along(axes[1], 1), sems)
                send(inner_block(plus(3, inner), span), ab4.at[color, 1, :, local], along(axes[1], 3), sems)
            else:
                mine = inner_block(inner, span)
                mine[...] += ab4[color, 0, :, local] + ab4[color, 1, :, local]
        if n < (3 if direct else 4):
            if direct and n == 2:
                ab = straight.at[:, :, :, pl.ds(d_at, width)]
            elif n == 2:
                ab = ab3.at[:, :, :, pl.ds(ab_at // 2, half)]
            elif n == 3:
                ab = ab4.at[:, :, :, pl.ds(ab_at, width)]
            else:
                ab = (ab1, ab2)[n].at[:, :, :, :, pl.ds(ab_at, width)]
            flying[piece, n] = remote(ab, ab, partner, sems)

    def third_step(piece, n):
        lane = PIECES[piece][0]
        width, _, c_at, _ = SHARE[piece]
        p = names.index(piece)
        base = lane + 2 * width
        tiles = 128 * THIRD[piece]
        local = pl.ds(c_at, tiles)
        if n > 0:
            flying.pop((piece, n - 1, "third")).wait()
        if n < 4:
            sems = (c_send.at[p], c_recv.at[p, n])

        def tile(index):
            return pl.ds(pl.multiple_of(base + tiles * index, 128), tiles)

        first_axis = "x" if p in EVEN else "y"
        second_axis = "y" if p in EVEN else "x"
        if n == 0:
            far = tile(plus(2, z))
            send(own.at[0:2, :, :, far], c1.at[0, :, :, :, local], along("z", 1), sems)
            send(own.at[2:4, :, :, far], c1.at[1, :, :, :, local], along("z", 3), sems)
        elif n == 1:
            up_one, down_one = tile(plus(1, z)), tile(plus(3, z))
            own[0:2, :, :, up_one] += c1[0, :, :, :, local]
            own[2:4, :, :, down_one] += c1[1, :, :, :, local]
            send(own.at[:, :, :, up_one], c2.at[0, :, :, :, local], along("z", 1), sems)
            send(own.at[:, :, :, down_one], c2.at[1, :, :, :, local], along("z", 3), sems)
        elif n == 2:
            own[:, :, :, tile(z)] += c2[0, :, :, :, local] + c2[1, :, :, :, local]
            for k in range(1, 4):
                block_of = own.at[plus(k, xx), :, :, tile(z)] if p in EVEN else own.at[:, plus(k, yy), :, tile(z)]
                send(block_of, c3.at[k - 1, :, :, local], along(first_axis, k), sems)
        elif n == 3:
            mine = own.at[xx, :, :, tile(z)] if p in EVEN else own.at[:, yy, :, tile(z)]
            mine[...] += c3[0, :, :, local] + c3[1, :, :, local] + c3[2, :, :, local]
            for k in range(1, 4):
                block_of = own.at[xx, plus(k, yy), :, tile(z)] if p in EVEN else own.at[plus(k, xx), yy, :, tile(z)]
                send(block_of, c4.at[k - 1, :, local], along(second_axis, k), sems)
        else:
            mine = own[xx, yy, :, tile(z)] + c4[0, :, local] + c4[1, :, local] + c4[2, :, local]
            own[xx, yy, :, base : base + 4 * tiles] = jnp.zeros((16, 4 * tiles), F32)
            own[xx, yy, :, tile(z)] = mine
        if n < 4:
            whole = (c1, c2, c3, c4)[n]
            whole = whole.at[:, :, :, :, local] if n < 2 else whole.at[:, :, :, local] if n == 2 else whole.at[:, :, local]
            flying[piece, n, "third"] = remote(whole, whole, partner, sems)

    def owned(device):
        return pl.ds(pl.multiple_of((device // 2) * ZBLOCK + (device % 2) * 1024, 128), OWN)

    last_sems = (last_send.at[0], last_recv.at[0])

    def to_owner(t):
        return remote(own.at[xx, yy, :, owned(t)], last.at[b], {"bngroup": t}, last_sems)

    def to_owners(targets):
        for t in targets:

            @pl.when(b != t)
            def _(t=t):
                to_owner(t).start()

    def gather(n, axis, slots, mine):
        sems = (norm_send.at[n], norm_recv.at[n])
        for k in range(1, 4):
            send(slots.at[mine], slots.at[mine], along(axis, k), sems)
        return remote(slots.at[0:3], slots.at[0:3], partner, sems)

    def sum_of(slots):
        return slots[0] + slots[1] + slots[2] + slots[3]

    sums = share(3, s4)
    write_out = pltpu.make_async_copy(g3, out_hbm, out_sem.at[0])
    write_out.start()
    turn(h2[...])
    sums.wait()
    group_sums(s4, 3)
    write_out.wait()

    @pl.loop(0, WIDE // CH)
    def _(j):
        at = lanes_at(j)
        amp, ss, gs = get(AMP, 3, j), get(SS, 3, j), get(GS, 3, j)

        @pl.loop(0, SIDE)
        def _(r):
            band = band_at(r)
            grad = amp * (up[band, at] - ss - pre3[band, at] * gs)
            g3[band, at] = real_rows(grad).astype(BF16)

    def slope_sums(pre, which, j, slots):
        at = lanes_at(j)
        cen, amp, shi, inv = get(CEN, which, j), get(AMP, which, j), get(SHI, which, j), get(INV, which, j)

        def add(r, acc):
            band = band_at(r)
            centred = pre[band, at] - cen
            normed = centred * amp + shi
            sigma = sigmoid(normed)
            value = real_rows(back[band, at] * (sigma * (1.0 + normed * (1.0 - sigma))))
            back[band, at] = value
            return (acc[0] + fold_rows(value), acc[1] + fold_rows(value * centred))

        zero = jnp.zeros((8, CH), F32)
        shift_sum, gain_sum = lax.fori_loop(0, SIDE, add, (zero, zero))
        slots[b, :, at] = total(shift_sum)
        slots[b, :, pl.ds(pl.multiple_of(MID + j * CH, CH), CH)] = total(gain_sum) * inv

    def norm_back(pre, which, j, r):
        at, band = lanes_at(j), band_at(r)
        cen, amp, ss, gs = get(CEN, which, j), get(AMP, which, j), get(SS, which, j), get(GS, which, j)
        return real_rows(amp * (back[band, at] - ss - (pre[band, at] - cen) * gs))

    @pl.loop(0, MID // CH)
    def _(j):
        back[:, lanes_at(j)] = dot(g3[...], wa[:, lanes_at(j)])
        slope_sums(pre2, 2, j, s5)

    load_wr = load(5, wr_hbm, wa)

    sums = share(4, s5)
    pl.semaphore_signal(ready, inc=1, device_id=partner, device_id_type=MESH)
    pl.semaphore_wait(ready, 1)
    weigh("expand", lambda i, half: g3[:, pl.ds(pl.multiple_of(i * MID + half * CH, CH), CH)])
    weigh("extra", lambda i, half: g3[:, pl.ds(pl.multiple_of(1024 + i * MID + half * CH, CH), CH)])
    step("expand", 0)
    sums.wait()
    group_sums(s5, 2)
    @pl.loop(0, MID // CH)
    def _(j):
        @pl.loop(0, SIDE)
        def _(r):
            grad = norm_back(pre2, 2, j, r)
            tiles = grad.reshape(IMGS, 8, CH)
            to = pl.ds(pl.multiple_of((r + 1) * BAND, BAND), BAND)
            for tap, shifted in enumerate((pltpu.roll(tiles, 7, 1), tiles, pltpu.roll(tiles, 1, 1))):
                at = pl.ds(pl.multiple_of(tap * MID + j * CH, CH), CH)
                g2[to, at] = shifted.reshape(BAND, CH).astype(BF16)

    def tap_row(row):
        return lambda i, half: taps[
            row * BAND : row * BAND + ROWS,
            pl.ds(pl.multiple_of(i * MID + half * CH, CH), CH),
        ]

    def back_one(j):
        acc = None
        for row in range(3):
            left = g2[(2 - row) * BAND : (2 - row) * BAND + ROWS, :]
            part = dot(left, ws[3 * MID * row : 3 * MID * (row + 1), j * CH : (j + 1) * CH])
            acc = part if acc is None else acc + part
        back[:, j * CH : (j + 1) * CH] = acc
        slope_sums(pre1, 1, j, s6)

    def input_gradient(quarter):
        @pl.loop(2 * quarter, 2 * quarter + 2)
        def _(j):
            at = lanes_at(j)
            g3[:, at] = (up[:, at] + dot(h2[...], wa[at, :], ((1,), (1,)))).astype(BF16)

    turn(g2[BAND : ROWS + BAND, MID : 2 * MID])
    weigh("low", tap_row(0))
    step("extra", 0)
    weigh("mid", tap_row(1))
    step("expand", 1)
    step("low", 0)
    third_step("expand", 0)
    third_step("low", 0)
    weigh("high", tap_row(2))
    step("mid", 0)
    third_step("mid", 0)
    step("extra", 1)
    back_one(0)
    step("low", 1)
    third_step("low", 1)
    step("high", 0)
    back_one(1)
    sums = share(5, s6)
    step("extra", 2)
    step("mid", 1)
    step("expand", 2)
    third_step("mid", 1)
    third_step("high", 0)
    third_step("expand", 1)
    step("low", 2)
    sums.wait()
    group_sums(s6, 1)
    ny[yy] = norm[...]
    norm_copies = gather(0, "y", ny, yy)

    @pl.loop(0, MID // CH)
    def _(j):
        @pl.loop(0, SIDE)
        def _(r):
            h2[band_at(r), lanes_at(j)] = norm_back(pre1, 1, j, r).astype(BF16)

    step("extra", 3)
    step("high", 1)
    third_step("low", 2)
    turn(h2[...])
    weigh("upper", lambda i, half: x[:, pl.ds(pl.multiple_of(1024 + i * MID + half * CH, CH), CH)])
    third_step("mid", 2)
    weigh("first", lambda i, half: x[:, pl.ds(pl.multiple_of(i * MID + half * CH, CH), CH)])
    step("upper", 0)
    third_step("upper", 0)
    load_wr.wait()
    input_gradient(0)
    third_step("high", 1)
    step("expand", 3)
    step("mid", 2)
    step("first", 0)
    step("high", 2)
    third_step("first", 0)
    third_step("upper", 1)
    step("low", 3)
    third_step("expand", 2)
    third_step("mid", 3)
    input_gradient(1)
    step("mid", 3)
    third_step("low", 3)
    third_step("high", 2)
    input_gradient(2)
    step("expand", 4)
    step("first", 1)
    step("low", 4)
    step("extra", 4)
    norm_copies.wait()
    nx[xx] = sum_of(ny)
    norm_copies = gather(1, "x", nx, xx)
    step("upper", 1)
    third_step("first", 1)
    step("high", 3)
    third_step("upper", 2)
    third_step("mid", 4)
    step("mid", 4)
    third_step("high", 3)
    third_step("low", 4)
    to_owners(range(2, 4))
    third_step("expand", 3)
    third_step("first", 2)
    step("upper", 2)
    third_step("high", 4)
    third_step("expand", 4)
    step("high", 4)
    to_owners(range(4, GROUP))
    third_step("upper", 3)
    step("first", 2)
    third_step("first", 3)
    step("upper", 3)
    third_step("upper", 4)
    to_owners(range(1, 2))
    step("first", 3)
    third_step("first", 4)
    to_owners(range(1))
    input_gradient(3)
    write_in = pltpu.make_async_copy(g3, ing_hbm, out_sem.at[1])
    write_in.start()
    last[b] = own[xx, yy, :, owned(b)]

    norm_copies.wait()
    norm_out[...] = sum_of(nx) * (1.0 / IMAGES)
    write_in.wait()
    for n in range(13, 17):
        slot_free(n)
    remote(last.at[0 : GROUP - 1], last.at[0 : GROUP - 1], partner, last_sems).wait()

    parts = []
    for core in range(2):
        parts.append(last[core] + last[2 + core] + last[4 + core] + last[6 + core])
    whole = jnp.concatenate(parts, axis=0) * (1.0 / IMAGES)
    moved = pltpu.roll(whole, OWN - 64, 1)
    wg_ref[...] = jnp.where(c == 1, moved, whole)[:, : LANES // 8]


def run_block(x, cot, wr, ws, we, gain, shift):
    any_ = pl.BlockSpec(memory_space=pl.ANY)
    vmem = pl.BlockSpec(memory_space=pltpu.VMEM)
    v = pltpu.VMEM
    dma = pltpu.SemaphoreType.DMA
    pieces = len(PIECES)
    return pl.pallas_call(
        block,
        out_shape=(
            jax.ShapeDtypeStruct((ROWS, WIDE), BF16),
            jax.ShapeDtypeStruct((ROWS, WIDE), BF16),
            jax.ShapeDtypeStruct((32, LANES // 8), F32),
            jax.ShapeDtypeStruct((2, 3072), F32),
        ),
        in_specs=[any_] * 5 + [vmem] * 2,
        out_specs=(any_, any_, vmem, vmem),
        scratch_shapes=[
            v((ROWS, WIDE), BF16),
            v((SIDE, IMGS, SIDE, WIDE), BF16),
            v((WIDE, MID), BF16),
            v((9 * MID, MID), BF16),
            v((ROWS, MID), F32),
            v((ROWS + 2 * BAND, 3 * MID), BF16),
            v((ROWS, MID), F32),
            v((ROWS, MID), BF16),
            v((ROWS, WIDE), F32),
            v((ROWS, WIDE), F32),
            v((ROWS, WIDE), BF16),
            v((ROWS + 2 * BAND, 3 * MID), BF16),
            v((ROWS, MID), F32),
            v((2, MID // 2, ROWS), BF16),
            v((SLOTS, MID // 2, MID), F32),
            v((6, 1, 3072), F32),
            v((GROUP, 1, 2 * MID), F32),
            v((GROUP, 1, 2 * MID), F32),
            v((GROUP, 1, 2 * WIDE), F32),
            v((GROUP, 1, 2 * WIDE), F32),
            v((GROUP, 1, 2 * MID), F32),
            v((GROUP, 1, 2 * MID), F32),
            v((2, 3072), F32),
            v((4, 4, 16, LANES), F32),
            v((MID // 2, 9 * MID), F32),
            v((2, 2, 2, 16, AB_LANES), F32),
            v((2, 2, 4, 16, AB_LANES), F32),
            v((2, 2, 16, AB_LANES // 2), F32),
            v((2, 2, 16, AB_LANES), F32),
            v((2, 3, 16, D_LANES), F32),
            v((2, 2, 4, 16, C_LANES), F32),
            v((2, 4, 4, 16, C_LANES), F32),
            v((3, 4, 16, C_LANES), F32),
            v((3, 16, C_LANES), F32),
            v((GROUP, 16, OWN), F32),
            v((4, 2, 3072), F32),
            v((4, 2, 3072), F32),
            dma((6 + SIDE,)),
            dma((6,)),
            dma((6,)),
            dma((2,)),
            dma((SLOTS,)),
            dma((pieces,)),
            dma((pieces,)),
            dma((pieces, 4)),
            dma((pieces,)),
            dma((pieces, 4)),
            dma((1,)),
            dma((1,)),
            dma((2,)),
            dma((2,)),
            pltpu.SemaphoreType.REGULAR,
        ],
        compiler_params=pltpu.CompilerParams(
            collective_id=0, has_side_effects=True, vmem_limit_bytes=VMEM_LIMIT
        ),
        cost_estimate=pl.CostEstimate(flops=18 * 10**9, bytes_accessed=4 * 10**7, transcendentals=10**7),
        name="block",
    )(x, cot, wr, ws, we, gain, shift)


def from_rows(rows):
    return rows.reshape(SIDE, IMGS, COLS, WIDE)[:, :, :SIDE].transpose(1, 0, 2, 3)


def per_device(images, cotangent, w_reduce, w_spatial, w_expand, norm_gain, norm_shift):
    output, in_grad, grads, norm_grads = run_block(
        images, cotangent, w_reduce, w_spatial, w_expand,
        norm_gain.reshape(1, -1), norm_shift.reshape(1, -1),
    )
    return (from_rows(output), from_rows(in_grad), grads.T, norm_grads)


def solution(mesh):
    both = P(("bngroup", "rep"), None, None, None)
    return jax.shard_map(
        per_device,
        mesh=mesh,
        in_specs=(both, both, P(), P(), P(), P(), P()),
        out_specs=(both, both, P("bngroup", "rep"), P()),
        check_vma=False,
    )
```

```python
import jax
import jax.numpy as jnp
from jax import lax
from jax.experimental import pallas as pl
from jax.experimental.pallas import tpu as pltpu
from jax.sharding import PartitionSpec as P

MESH = pl.DeviceIdType.MESH
F32 = jnp.float32
BF16 = jnp.bfloat16

IMGS, SIDE, COLS = 12, 7, 8
WIDE, MID = 2048, 512
QUARTERS = 4
BAND = IMGS * COLS
ROWS = SIDE * BAND
REAL = IMGS * SIDE * SIDE
GROUP = 8
COUNT = float(REAL * GROUP)
IMAGES = 1536.0
EPS = 0.25
CH = 256
LANES = 2 * WIDE + 9 * MID
ZBLOCK = LANES // 4
OWN = 1152
VMEM_LIMIT = 67043328
SLOTS = 4

PIECES = {
    "expand": (6656, 1024, 0, 2),
    "extra": (7680, 1024, 2, 2),
    "low": (2048, 1536, 4, 3),
    "mid": (3584, 1536, 7, 3),
    "high": (5120, 1536, 10, 3),
    "upper": (1024, 1024, 13, 2),
    "first": (0, 1024, 15, 2),
}
LANDING = {"expand": 0, "extra": 1024, "low": 0, "mid": 1536, "high": 3072, "upper": 1024, "first": 0}
THIRD = {"expand": 1, "low": 1, "mid": 1, "high": 1, "upper": 1, "first": 1}
DIRECT = ("upper", "first",)
SHARE = {}
_ab, _c, _d = 0, 0, 0
for _name, (_lane, _size, _, _) in PIECES.items():
    _n = (_size - 512 * THIRD.get(_name, 0)) // 2
    SHARE[_name] = (_n, _ab, _c, _d)
    _ab, _c, _d = _ab + _n, _c + 128 * THIRD.get(_name, 0), _d + (_n if _name in DIRECT else 0)
EVEN = (0, 2, 4, 6)
D_LANES = _d
AB_LANES, C_LANES = _ab, _c


def dot(left, right, dims=((1,), (0,))):
    return lax.dot_general(left, right, (dims, ((), ())), preferred_element_type=F32)


def sigmoid(value):
    return 0.5 * jnp.tanh(0.5 * value) + 0.5


def real_rows(value):
    rows, lanes = value.shape
    tiles = value.reshape(rows // 8, 8, lanes)
    column = lax.broadcasted_iota(jnp.int32, tiles.shape, 1)
    return jnp.where(column != 7, tiles, 0.0).reshape(rows, lanes)


def fold_rows(value):
    rows, lanes = value.shape
    return jnp.sum(value.reshape(rows // 8, 8, lanes), axis=0)


def total(folded):
    return jnp.sum(folded, axis=0, keepdims=True)


def lanes_at(j, size=CH):
    return pl.ds(pl.multiple_of(j * size, size), size)


def band_at(r):
    return pl.ds(pl.multiple_of(r * BAND, BAND), BAND)


def block(
    x_hbm, cot_hbm, wr_hbm, ws_hbm, we_hbm, gain_ref, shift_ref,
    out_hbm, ing_hbm, wg_ref, norm_out,
    x, raw, wa, ws, pre1, taps, pre2, h2, pre3, up, g3, g2, back, turned, stage, rows,
    s1, s2, s3, s4, s5, s6, norm, own, other, ab1, ab2, ab3, ab4, straight, c1, c2, c3, c4, last, ny, nx,
    load_sem, send_sem, recv_sem, out_sem, core_send, core_recv,
    ab_send, ab_recv, c_send, c_recv, last_send, last_recv, norm_send, norm_recv, ready,
):
    b, rep = lax.axis_index("bngroup"), lax.axis_index("rep")
    z, c = b // 2, b % 2
    xx, yy = rep // 4, rep % 4

    def along(axis, k):
        if axis == "x":
            return {"rep": ((xx + k) % 4) * 4 + yy}
        if axis == "y":
            return {"rep": xx * 4 + (yy + k) % 4}
        return {"bngroup": (b + 2 * k) % GROUP}

    def load(i, src, dst):
        copy = pltpu.make_async_copy(src, dst, load_sem.at[i])
        copy.start()
        return copy

    def load_images(first, apart, images):
        return [load(first + apart * r, images.at[:, r], raw.at[r]) for r in range(SIDE)]

    def raw_rows(r, at):
        value = raw[r, :, :, at].astype(F32)
        value = jnp.concatenate([value, jnp.zeros((IMGS, 1, value.shape[2]), F32)], axis=1)
        return value.reshape(BAND, value.shape[2])

    load_x = load_images(6, 1, x_hbm)
    load_wr = load(1, wr_hbm, wa)

    barrier = pltpu.get_barrier_semaphore()
    for k in range(1, GROUP):
        pl.semaphore_signal(barrier, inc=1, device_id={"bngroup": (b + k) % GROUP}, device_id_type=MESH)
    for axis in "xy":
        for k in range(1, 4):
            pl.semaphore_signal(barrier, inc=1, device_id=along(axis, k), device_id_type=MESH)

    zeros = jnp.zeros((BAND, 3 * MID), BF16)
    taps[0:BAND, :] = zeros
    taps[ROWS + BAND :, :] = zeros
    g2[0:BAND, :] = zeros
    g2[ROWS + BAND :, :] = zeros

    partner = {"bngroup": b + 1 - 2 * c}

    def remote(src, dst, device, sems):
        return pltpu.make_async_remote_copy(
            src_ref=src, dst_ref=dst, send_sem=sems[0], recv_sem=sems[1],
            device_id=device, device_id_type=MESH,
        )

    def share(e, slots):
        sems = (send_sem.at[e], recv_sem.at[e])
        for k in range(1, GROUP):
            remote(slots.at[b], slots.at[b], {"bngroup": (b + k) % GROUP}, sems).start()
        return remote(slots.at[0 : GROUP - 1], slots.at[0 : GROUP - 1], partner, sems)

    CEN, AMP, SHI, INV, SS, GS = range(6)
    OFF = {1: 0, 2: MID, 3: 2 * MID}

    def put(row, off, value):
        rows[row, :, off : off + value.shape[1]] = value

    def get(row, which, j):
        return rows[row, :, pl.ds(pl.multiple_of(OFF[which] + j * CH, CH), CH)]

    def stats(value, j, slots, channels):
        about = total(value[0:8]) / 7.0
        off = real_rows(value - about)
        first, second = total(fold_rows(off)) / REAL, total(fold_rows(off * off))
        slots[b, :, lanes_at(j)] = about + first
        at = pl.ds(pl.multiple_of(channels + j * CH, CH), CH)
        slots[b, :, at] = jnp.maximum(second - REAL * (first * first), 0.0)

    def group_stats(slots, which, start=0, c=MID):
        off_at = OFF[which] + start
        mean = slots[0, :, 0:c]
        for i in range(1, GROUP):
            mean = mean + slots[i, :, 0:c]
        mean = mean / GROUP
        second = jnp.zeros((1, c), F32)
        for i in range(GROUP):
            off = slots[i, :, 0:c] - mean
            second = second + (slots[i, :, c : 2 * c] + REAL * (off * off))
        inverse = lax.rsqrt(second / COUNT + EPS)
        put(CEN, off_at, mean)
        put(INV, off_at, inverse)
        put(AMP, off_at, gain_ref[:, off_at : off_at + c] * inverse)
        put(SHI, off_at, shift_ref[:, off_at : off_at + c])

    def group_sums(slots, which, start=0, c=MID):
        off_at = OFF[which] + start
        sums = slots[0]
        for i in range(1, GROUP):
            sums = sums + slots[i]
        shift_sum, gain_sum = sums[:, 0:c], sums[:, c : 2 * c]
        inverse = rows[INV, :, off_at : off_at + c]
        norm[0:1, off_at : off_at + c] = gain_sum
        norm[1:2, off_at : off_at + c] = shift_sum
        put(SS, off_at, shift_sum / COUNT)
        put(GS, off_at, inverse * gain_sum / COUNT)

    for r in range(SIDE):
        load_x[r].wait()

        @pl.loop(0, WIDE // CH)
        def _(j, r=r):
            x[r * BAND : (r + 1) * BAND, lanes_at(j)] = raw_rows(r, lanes_at(j)).astype(BF16)

    load_wr.wait()
    load_ws = load(2, ws_hbm, ws)
    load_images(4, 0, cot_hbm)
    @pl.loop(0, MID // CH)
    def _(j):
        value = dot(x[...], wa[:, lanes_at(j)])
        pre1[:, lanes_at(j)] = value
        stats(value, j, s1, MID)

    load_we = load(3, we_hbm, wa)
    pl.semaphore_wait(barrier, GROUP - 1 + 6)
    share(0, s1).wait()
    group_stats(s1, 1)

    @pl.loop(0, MID // CH)
    def _(j):
        cen, amp, shi = get(CEN, 1, j), get(AMP, 1, j), get(SHI, 1, j)

        @pl.loop(0, SIDE)
        def _(r):
            normed = (pre1[band_at(r), lanes_at(j)] - cen) * amp + shi
            hidden = real_rows(normed * sigmoid(normed))
            tiles = hidden.reshape(IMGS, 8, CH)
            to = pl.ds(pl.multiple_of((r + 1) * BAND, BAND), BAND)
            for tap, shifted in enumerate((pltpu.roll(tiles, 1, 1), tiles, pltpu.roll(tiles, 7, 1))):
                at = pl.ds(pl.multiple_of(tap * MID + j * CH, CH), CH)
                taps[to, at] = shifted.reshape(BAND, CH).astype(BF16)

    load_ws.wait()

    @pl.loop(0, MID // CH)
    def _(j):
        acc = dot(taps[0:ROWS, :], ws[0 : 3 * MID, lanes_at(j)])
        acc = acc + dot(taps[BAND : ROWS + BAND, :], ws[3 * MID : 6 * MID, lanes_at(j)])
        acc = acc + dot(taps[2 * BAND :, :], ws[6 * MID :, lanes_at(j)])
        value = real_rows(acc)
        pre2[:, lanes_at(j)] = value
        stats(value, j, s2, MID)

    sums = share(1, s2)

    @pl.loop(0, 9)
    def _(tap):
        at = pl.ds(pl.multiple_of(tap * MID, MID), MID)
        ws[at, :] = ws[at, :].T

    sums.wait()
    group_stats(s2, 2)

    @pl.loop(0, MID // CH)
    def _(j):
        cen, amp, shi = get(CEN, 2, j), get(AMP, 2, j), get(SHI, 2, j)

        @pl.loop(0, SIDE)
        def _(r):
            normed = (pre2[band_at(r), lanes_at(j)] - cen) * amp + shi
            h2[band_at(r), lanes_at(j)] = real_rows(normed * sigmoid(normed)).astype(BF16)

    load_we.wait()

    exchanged = []
    for q in range(QUARTERS):

        @pl.loop(2 * q, 2 * q + 2)
        def _(j, q=q):
            value = dot(h2[...], wa[lanes_at(j), :], ((1,), (1,)))
            pre3[:, lanes_at(j)] = value
            stats(value, j - 2 * q, s3.at[q], MID)

        exchanged.append(share(6 + q, s3.at[q]))

    pltpu.make_async_copy(raw, raw, load_sem.at[4]).wait()

    written, sums = [], []
    for q in range(QUARTERS):
        exchanged[q].wait()
        group_stats(s3.at[q], 3, q * MID)

        @pl.loop(2 * q, 2 * q + 2)
        def _(j, q=q):
            at = lanes_at(j)
            cen, amp, shi, inv = get(CEN, 3, j), get(AMP, 3, j), get(SHI, 3, j), get(INV, 3, j)

            def add(r, acc):
                band = band_at(r)
                centred = pre3[band, at] - cen
                summed = centred * amp + shi + x[band, at].astype(F32)
                sigma = sigmoid(summed)
                value = summed * sigma
                upstream = raw_rows(r, at) * (sigma + value * (1.0 - sigma))
                g3[band, at] = value.astype(BF16)
                up[band, at] = upstream
                pre3[band, at] = centred
                return (acc[0] + fold_rows(upstream), acc[1] + fold_rows(upstream * centred))

            zero = jnp.zeros((8, CH), F32)
            shift_sum, gain_sum = lax.fori_loop(0, SIDE, add, (zero, zero))
            s4[q, b, :, lanes_at(j - 2 * q)] = total(shift_sum)
            s4[q, b, :, pl.ds(pl.multiple_of(MID + (j - 2 * q) * CH, CH), CH)] = total(gain_sum) * inv

        sums.append(share(6 + QUARTERS + q, s4.at[q]))
        at = pl.ds(q * MID, MID)
        copy = pltpu.make_async_copy(g3.at[:, at], out_hbm.at[:, at], out_sem.at[q])
        copy.start()
        written.append(copy)

    def turn(value):
        halves = value.T.reshape(16, 2, 16, ROWS)
        for half in range(2):
            turned[(half + c + 1) % 2] = halves[:, half].reshape(MID // 2, ROWS)

    def landing(piece, at):
        if piece in ("expand", "extra"):
            return pre3.at[0:256, at]
        if piece in ("upper", "first"):
            return pre3.at[256:512, at]
        return other.at[:, at]

    names = list(PIECES)

    def to_partner(piece, i):
        chunk = PIECES[piece][2]
        at = pl.ds(pl.multiple_of(LANDING[piece] + i * MID, MID), MID)
        slot = (chunk + i) % SLOTS
        sems = (core_send.at[slot], core_recv.at[names.index(piece)])
        return remote(stage.at[slot], landing(piece, at), partner, sems)

    def slot_free(n):
        remote(stage.at[n % SLOTS], other.at[:, 0:MID], partner, (core_send.at[n % SLOTS], core_recv.at[0])).wait_send()

    def weigh(piece, right):
        lane, size, chunk, count = PIECES[piece]

        @pl.loop(0, count)
        def _(i):
            slot = (chunk + i) % SLOTS
            if chunk >= SLOTS:
                slot_free(chunk + i - SLOTS)
            for half in range(MID // CH):
                product = dot(turned[...].reshape(MID, ROWS), right(i, half))
                stage[slot, :, half * CH : (half + 1) * CH] = product[: MID // 2]
                at = pl.ds(pl.multiple_of(lane + i * MID + half * CH, CH), CH)
                own[:, :, :, at] = product[MID // 2 :].reshape(4, 4, 16, CH)
            to_partner(piece, i).start()

    flying = {}

    def send(src, dst, device, sems):
        remote(src, dst, device, sems).start()

    def plus(k, base):
        return (base + k) % 4

    def step(piece, n):
        lane, size, chunk, count = PIECES[piece]
        width, ab_at, c_at, d_at = SHARE[piece]
        direct = piece in DIRECT
        p = names.index(piece)
        half = width // 2
        if n == 0:
            landed = landing(piece, pl.ds(LANDING[piece], size))
            remote(landed, landed, partner, (core_send.at[0], core_recv.at[p])).wait_recv()

            @pl.loop(0, 16)
            def _(k):
                own[k // 4, k % 4, :, lane : lane + size] += landed[pl.ds(pl.multiple_of(k * 16, 16), 16), :]

        else:
            flying.pop((piece, n - 1)).wait()
        if n < 4:
            sems = (ab_send.at[p], ab_recv.at[p, n])
        for color in range(2):
            span = pl.ds(lane + color * width, width)
            local = pl.ds(ab_at, width)
            axes = "xy" if color == 0 else "yx"
            outer, inner = (xx, yy) if color == 0 else (yy, xx)
            parts = [pl.ds(lane + color * width + k * half, half) for k in range(2)]
            local_part = pl.ds(ab_at // 2, half)

            def outer_block(index, part=slice(None), color=color, span=span):
                return own.at[index, part, :, span] if color == 0 else own.at[part, index, :, span]

            def inner_block(index, part, color=color, outer=outer):
                return own.at[outer, index, :, part] if color == 0 else own.at[index, outer, :, part]

            if n == 0:
                far = plus(2, outer)
                send(outer_block(far, slice(0, 2)), ab1.at[color, 0, :, :, local], along(axes[0], 1), sems)
                send(outer_block(far, slice(2, 4)), ab1.at[color, 1, :, :, local], along(axes[0], 3), sems)
            elif n == 1:
                low = outer_block(plus(1, outer), slice(0, 2))
                low[...] += ab1[color, 0, :, :, local]
                high = outer_block(plus(3, outer), slice(2, 4))
                high[...] += ab1[color, 1, :, :, local]
                send(outer_block(plus(1, outer)), ab2.at[color, 0, :, :, local], along(axes[0], 1), sems)
                send(outer_block(plus(3, outer)), ab2.at[color, 1, :, :, local], along(axes[0], 3), sems)
            elif n == 2:
                mine = outer_block(outer)
                mine[...] += ab2[color, 0, :, :, local] + ab2[color, 1, :, :, local]
                if direct:
                    for k in range(1, 4):
                        send(inner_block(plus(k, inner), span), straight.at[color, k - 1, :, pl.ds(d_at, width)], along(axes[1], k), sems)
                    continue
                far = plus(2, inner)
                send(inner_block(far, parts[0]), ab3.at[color, 0, :, local_part], along(axes[1], 1), sems)
                send(inner_block(far, parts[1]), ab3.at[color, 1, :, local_part], along(axes[1], 3), sems)
            elif direct:
                if n == 3:
                    at = pl.ds(d_at, width)
                    mine = inner_block(inner, span)
                    mine[...] += straight[color, 0, :, at] + straight[color, 1, :, at] + straight[color, 2, :, at]
            elif n == 3:
                low = inner_block(plus(1, inner), parts[0])
                low[...] += ab3[color, 0, :, local_part]
                high = inner_block(plus(3, inner), parts[1])
                high[...] += ab3[color, 1, :, local_part]
                send(inner_block(plus(1, inner), span), ab4.at[color, 0, :, local], along(axes[1], 1), sems)
                send(inner_block(plus(3, inner), span), ab4.at[color, 1, :, local], along(axes[1], 3), sems)
            else:
                mine = inner_block(inner, span)
                mine[...] += ab4[color, 0, :, local] + ab4[color, 1, :, local]
        if n < (3 if direct else 4):
            if direct and n == 2:
                ab = straight.at[:, :, :, pl.ds(d_at, width)]
            elif n == 2:
                ab = ab3.at[:, :, :, pl.ds(ab_at // 2, half)]
            elif n == 3:
                ab = ab4.at[:, :, :, pl.ds(ab_at, width)]
            else:
                ab = (ab1, ab2)[n].at[:, :, :, :, pl.ds(ab_at, width)]
            flying[piece, n] = remote(ab, ab, partner, sems)

    def third_step(piece, n):
        lane = PIECES[piece][0]
        width, _, c_at, _ = SHARE[piece]
        p = names.index(piece)
        base = lane + 2 * width
        tiles = 128 * THIRD[piece]
        local = pl.ds(c_at, tiles)
        if n > 0:
            flying.pop((piece, n - 1, "third")).wait()
        if n < 4:
            sems = (c_send.at[p], c_recv.at[p, n])

        def tile(index):
            return pl.ds(pl.multiple_of(base + tiles * index, 128), tiles)

        first_axis = "x" if p in EVEN else "y"
        second_axis = "y" if p in EVEN else "x"
        if n == 0:
            far = tile(plus(2, z))
            send(own.at[0:2, :, :, far], c1.at[0, :, :, :, local], along("z", 1), sems)
            send(own.at[2:4, :, :, far], c1.at[1, :, :, :, local], along("z", 3), sems)
        elif n == 1:
            up_one, down_one = tile(plus(1, z)), tile(plus(3, z))
            own[0:2, :, :, up_one] += c1[0, :, :, :, local]
            own[2:4, :, :, down_one] += c1[1, :, :, :, local]
            send(own.at[:, :, :, up_one], c2.at[0, :, :, :, local], along("z", 1), sems)
            send(own.at[:, :, :, down_one], c2.at[1, :, :, :, local], along("z", 3), sems)
        elif n == 2:
            own[:, :, :, tile(z)] += c2[0, :, :, :, local] + c2[1, :, :, :, local]
            for k in range(1, 4):
                block_of = own.at[plus(k, xx), :, :, tile(z)] if p in EVEN else own.at[:, plus(k, yy), :, tile(z)]
                send(block_of, c3.at[k - 1, :, :, local], along(first_axis, k), sems)
        elif n == 3:
            mine = own.at[xx, :, :, tile(z)] if p in EVEN else own.at[:, yy, :, tile(z)]
            mine[...] += c3[0, :, :, local] + c3[1, :, :, local] + c3[2, :, :, local]
            for k in range(1, 4):
                block_of = own.at[xx, plus(k, yy), :, tile(z)] if p in EVEN else own.at[plus(k, xx), yy, :, tile(z)]
                send(block_of, c4.at[k - 1, :, local], along(second_axis, k), sems)
        else:
            mine = own[xx, yy, :, tile(z)] + c4[0, :, local] + c4[1, :, local] + c4[2, :, local]
            own[xx, yy, :, base : base + 4 * tiles] = jnp.zeros((16, 4 * tiles), F32)
            own[xx, yy, :, tile(z)] = mine
        if n < 4:
            whole = (c1, c2, c3, c4)[n]
            whole = whole.at[:, :, :, :, local] if n < 2 else whole.at[:, :, :, local] if n == 2 else whole.at[:, :, local]
            flying[piece, n, "third"] = remote(whole, whole, partner, sems)

    def owned(device):
        return pl.ds(pl.multiple_of((device // 2) * ZBLOCK + (device % 2) * 1024, 128), OWN)

    last_sems = (last_send.at[0], last_recv.at[0])

    def to_owner(t):
        return remote(own.at[xx, yy, :, owned(t)], last.at[b], {"bngroup": t}, last_sems)

    def to_owners(targets):
        for t in targets:

            @pl.when(b != t)
            def _(t=t):
                to_owner(t).start()

    def gather(n, axis, slots, mine):
        sems = (norm_send.at[n], norm_recv.at[n])
        for k in range(1, 4):
            send(slots.at[mine], slots.at[mine], along(axis, k), sems)
        return remote(slots.at[0:3], slots.at[0:3], partner, sems)

    def sum_of(slots):
        return slots[0] + slots[1] + slots[2] + slots[3]

    def grad_three(q):
        sums[q].wait()
        group_sums(s4.at[q], 3, q * MID)
        written[q].wait()

        @pl.loop(2 * q, 2 * q + 2)
        def _(j):
            at = lanes_at(j)
            amp, ss, gs = get(AMP, 3, j), get(SS, 3, j), get(GS, 3, j)

            @pl.loop(0, SIDE)
            def _(r):
                band = band_at(r)
                grad = amp * (up[band, at] - ss - pre3[band, at] * gs)
                g3[band, at] = real_rows(grad).astype(BF16)

    def tell_partner():
        pl.semaphore_signal(ready, inc=1, device_id=partner, device_id_type=MESH)

    def slope_sums(pre, which, j, slots):
        at = lanes_at(j)
        cen, amp, shi, inv = get(CEN, which, j), get(AMP, which, j), get(SHI, which, j), get(INV, which, j)

        def add(r, acc):
            band = band_at(r)
            centred = pre[band, at] - cen
            normed = centred * amp + shi
            sigma = sigmoid(normed)
            value = real_rows(back[band, at] * (sigma * (1.0 + normed * (1.0 - sigma))))
            back[band, at] = value
            return (acc[0] + fold_rows(value), acc[1] + fold_rows(value * centred))

        zero = jnp.zeros((8, CH), F32)
        shift_sum, gain_sum = lax.fori_loop(0, SIDE, add, (zero, zero))
        slots[b, :, at] = total(shift_sum)
        slots[b, :, pl.ds(pl.multiple_of(MID + j * CH, CH), CH)] = total(gain_sum) * inv

    def norm_back(pre, which, j, r):
        at, band = lanes_at(j), band_at(r)
        cen, amp, ss, gs = get(CEN, which, j), get(AMP, which, j), get(SS, which, j), get(GS, which, j)
        return real_rows(amp * (back[band, at] - ss - (pre[band, at] - cen) * gs))

    turn(h2[...])
    grad_three(0)
    grad_three(1)
    tell_partner()
    pl.semaphore_wait(ready, 1)
    weigh("expand", lambda i, half: g3[:, pl.ds(pl.multiple_of(i * MID + half * CH, CH), CH)])
    grad_three(2)
    grad_three(3)
    tell_partner()
    @pl.loop(0, MID // CH)
    def _(j):
        back[:, lanes_at(j)] = dot(g3[...], wa[:, lanes_at(j)])
        slope_sums(pre2, 2, j, s5)

    load_wr = load(5, wr_hbm, wa)

    sums = share(4, s5)
    pl.semaphore_wait(ready, 1)
    weigh("extra", lambda i, half: g3[:, pl.ds(pl.multiple_of(1024 + i * MID + half * CH, CH), CH)])
    step("expand", 0)
    sums.wait()
    group_sums(s5, 2)
    @pl.loop(0, MID // CH)
    def _(j):
        @pl.loop(0, SIDE)
        def _(r):
            grad = norm_back(pre2, 2, j, r)
            tiles = grad.reshape(IMGS, 8, CH)
            to = pl.ds(pl.multiple_of((r + 1) * BAND, BAND), BAND)
            for tap, shifted in enumerate((pltpu.roll(tiles, 7, 1), tiles, pltpu.roll(tiles, 1, 1))):
                at = pl.ds(pl.multiple_of(tap * MID + j * CH, CH), CH)
                g2[to, at] = shifted.reshape(BAND, CH).astype(BF16)

    def tap_row(row):
        return lambda i, half: taps[
            row * BAND : row * BAND + ROWS,
            pl.ds(pl.multiple_of(i * MID + half * CH, CH), CH),
        ]

    def back_one(j):
        acc = None
        for row in range(3):
            left = g2[(2 - row) * BAND : (2 - row) * BAND + ROWS, :]
            part = dot(left, ws[3 * MID * row : 3 * MID * (row + 1), j * CH : (j + 1) * CH])
            acc = part if acc is None else acc + part
        back[:, j * CH : (j + 1) * CH] = acc
        slope_sums(pre1, 1, j, s6)

    def input_gradient(quarter):
        @pl.loop(2 * quarter, 2 * quarter + 2)
        def _(j):
            at = lanes_at(j)
            g3[:, at] = (up[:, at] + dot(h2[...], wa[at, :], ((1,), (1,)))).astype(BF16)

    turn(g2[BAND : ROWS + BAND, MID : 2 * MID])
    weigh("low", tap_row(0))
    step("extra", 0)
    weigh("mid", tap_row(1))
    step("expand", 1)
    step("low", 0)
    third_step("expand", 0)
    third_step("low", 0)
    weigh("high", tap_row(2))
    step("mid", 0)
    third_step("mid", 0)
    step("extra", 1)
    back_one(0)
    step("low", 1)
    third_step("low", 1)
    step("high", 0)
    back_one(1)
    sums = share(5, s6)
    step("extra", 2)
    step("mid", 1)
    step("expand", 2)
    third_step("mid", 1)
    third_step("high", 0)
    third_step("expand", 1)
    step("low", 2)
    sums.wait()
    group_sums(s6, 1)
    ny[yy] = norm[...]
    norm_copies = gather(0, "y", ny, yy)

    @pl.loop(0, MID // CH)
    def _(j):
        @pl.loop(0, SIDE)
        def _(r):
            h2[band_at(r), lanes_at(j)] = norm_back(pre1, 1, j, r).astype(BF16)

    step("extra", 3)
    step("high", 1)
    third_step("low", 2)
    turn(h2[...])
    weigh("upper", lambda i, half: x[:, pl.ds(pl.multiple_of(1024 + i * MID + half * CH, CH), CH)])
    third_step("mid", 2)
    weigh("first", lambda i, half: x[:, pl.ds(pl.multiple_of(i * MID + half * CH, CH), CH)])
    step("upper", 0)
    third_step("upper", 0)
    load_wr.wait()
    input_gradient(0)
    third_step("high", 1)
    step("expand", 3)
    step("mid", 2)
    step("first", 0)
    step("high", 2)
    third_step("first", 0)
    third_step("upper", 1)
    step("low", 3)
    third_step("expand", 2)
    third_step("mid", 3)
    input_gradient(1)
    step("mid", 3)
    third_step("low", 3)
    third_step("high", 2)
    input_gradient(2)
    step("expand", 4)
    step("first", 1)
    step("low", 4)
    step("extra", 4)
    norm_copies.wait()
    nx[xx] = sum_of(ny)
    norm_copies = gather(1, "x", nx, xx)
    step("upper", 1)
    third_step("first", 1)
    step("high", 3)
    third_step("upper", 2)
    third_step("mid", 4)
    step("mid", 4)
    third_step("high", 3)
    third_step("low", 4)
    to_owners(range(2, 4))
    third_step("expand", 3)
    third_step("first", 2)
    step("upper", 2)
    third_step("high", 4)
    third_step("expand", 4)
    step("high", 4)
    to_owners(range(4, GROUP))
    third_step("upper", 3)
    step("first", 2)
    third_step("first", 3)
    step("upper", 3)
    third_step("upper", 4)
    to_owners(range(1, 2))
    step("first", 3)
    third_step("first", 4)
    to_owners(range(1))
    input_gradient(3)
    write_in = pltpu.make_async_copy(g3, ing_hbm, out_sem.at[QUARTERS])
    write_in.start()
    last[b] = own[xx, yy, :, owned(b)]

    norm_copies.wait()
    norm_out[...] = sum_of(nx) * (1.0 / IMAGES)
    write_in.wait()
    for n in range(13, 17):
        slot_free(n)
    remote(last.at[0 : GROUP - 1], last.at[0 : GROUP - 1], partner, last_sems).wait()

    parts = []
    for core in range(2):
        parts.append(last[core] + last[2 + core] + last[4 + core] + last[6 + core])
    whole = jnp.concatenate(parts, axis=0) * (1.0 / IMAGES)
    moved = pltpu.roll(whole, OWN - 64, 1)
    wg_ref[...] = jnp.where(c == 1, moved, whole)[:, : LANES // 8]


def run_block(x, cot, wr, ws, we, gain, shift):
    any_ = pl.BlockSpec(memory_space=pl.ANY)
    vmem = pl.BlockSpec(memory_space=pltpu.VMEM)
    v = pltpu.VMEM
    dma = pltpu.SemaphoreType.DMA
    pieces = len(PIECES)
    return pl.pallas_call(
        block,
        out_shape=(
            jax.ShapeDtypeStruct((ROWS, WIDE), BF16),
            jax.ShapeDtypeStruct((ROWS, WIDE), BF16),
            jax.ShapeDtypeStruct((32, LANES // 8), F32),
            jax.ShapeDtypeStruct((2, 3072), F32),
        ),
        in_specs=[any_] * 5 + [vmem] * 2,
        out_specs=(any_, any_, vmem, vmem),
        scratch_shapes=[
            v((ROWS, WIDE), BF16),
            v((SIDE, IMGS, SIDE, WIDE), BF16),
            v((WIDE, MID), BF16),
            v((9 * MID, MID), BF16),
            v((ROWS, MID), F32),
            v((ROWS + 2 * BAND, 3 * MID), BF16),
            v((ROWS, MID), F32),
            v((ROWS, MID), BF16),
            v((ROWS, WIDE), F32),
            v((ROWS, WIDE), F32),
            v((ROWS, WIDE), BF16),
            v((ROWS + 2 * BAND, 3 * MID), BF16),
            v((ROWS, MID), F32),
            v((2, MID // 2, ROWS), BF16),
            v((SLOTS, MID // 2, MID), F32),
            v((6, 1, 3072), F32),
            v((GROUP, 1, 2 * MID), F32),
            v((GROUP, 1, 2 * MID), F32),
            v((QUARTERS, GROUP, 1, 2 * MID), F32),
            v((QUARTERS, GROUP, 1, 2 * MID), F32),
            v((GROUP, 1, 2 * MID), F32),
            v((GROUP, 1, 2 * MID), F32),
            v((2, 3072), F32),
            v((4, 4, 16, LANES), F32),
            v((MID // 2, 9 * MID), F32),
            v((2, 2, 2, 16, AB_LANES), F32),
            v((2, 2, 4, 16, AB_LANES), F32),
            v((2, 2, 16, AB_LANES // 2), F32),
            v((2, 2, 16, AB_LANES), F32),
            v((2, 3, 16, D_LANES), F32),
            v((2, 2, 4, 16, C_LANES), F32),
            v((2, 4, 4, 16, C_LANES), F32),
            v((3, 4, 16, C_LANES), F32),
            v((3, 16, C_LANES), F32),
            v((GROUP, 16, OWN), F32),
            v((4, 2, 3072), F32),
            v((4, 2, 3072), F32),
            dma((6 + SIDE,)),
            dma((6 + 2 * QUARTERS,)),
            dma((6 + 2 * QUARTERS,)),
            dma((QUARTERS + 1,)),
            dma((SLOTS,)),
            dma((pieces,)),
            dma((pieces,)),
            dma((pieces, 4)),
            dma((pieces,)),
            dma((pieces, 4)),
            dma((1,)),
            dma((1,)),
            dma((2,)),
            dma((2,)),
            pltpu.SemaphoreType.REGULAR,
        ],
        compiler_params=pltpu.CompilerParams(
            collective_id=0, has_side_effects=True, vmem_limit_bytes=VMEM_LIMIT
        ),
        cost_estimate=pl.CostEstimate(flops=18 * 10**9, bytes_accessed=4 * 10**7, transcendentals=10**7),
        name="block",
    )(x, cot, wr, ws, we, gain, shift)


def from_rows(rows):
    return rows.reshape(SIDE, IMGS, COLS, WIDE)[:, :, :SIDE].transpose(1, 0, 2, 3)


def per_device(images, cotangent, w_reduce, w_spatial, w_expand, norm_gain, norm_shift):
    output, in_grad, grads, norm_grads = run_block(
        images, cotangent, w_reduce, w_spatial, w_expand,
        norm_gain.reshape(1, -1), norm_shift.reshape(1, -1),
    )
    return (from_rows(output), from_rows(in_grad), grads.T, norm_grads)


def solution(mesh):
    both = P(("bngroup", "rep"), None, None, None)
    return jax.shard_map(
        per_device,
        mesh=mesh,
        in_specs=(both, both, P(), P(), P(), P(), P()),
        out_specs=(both, both, P("bngroup", "rep"), P()),
        check_vma=False,
    )
```

```python
import jax
import jax.numpy as jnp
from jax import lax
from jax.experimental import pallas as pl
from jax.experimental.pallas import tpu as pltpu
from jax.sharding import PartitionSpec as P

MESH = pl.DeviceIdType.MESH
F32 = jnp.float32
BF16 = jnp.bfloat16

IMGS, SIDE, COLS = 12, 7, 8
WIDE, MID = 2048, 512
QUARTERS = 4
BAND = IMGS * COLS
ROWS = SIDE * BAND
REAL = IMGS * SIDE * SIDE
GROUP = 8
COUNT = float(REAL * GROUP)
IMAGES = 1536.0
EPS = 0.25
CH = 256
LANES = 2 * WIDE + 9 * MID
ZBLOCK = LANES // 4
OWN = 1152
VMEM_LIMIT = 67043328
SLOTS = 4

PIECES = {
    "expand": (6656, 1024, 0, 2),
    "extra": (7680, 1024, 2, 2),
    "low": (2048, 1536, 4, 3),
    "mid": (3584, 1536, 7, 3),
    "high": (5120, 1536, 10, 3),
    "upper": (1024, 1024, 13, 2),
    "first": (0, 1024, 15, 2),
}
LANDING = {"expand": 0, "extra": 1024, "low": 0, "mid": 1536, "high": 3072, "upper": 1024, "first": 0}
THIRD = {"expand": 1, "low": 1, "mid": 1, "high": 1, "upper": 1, "first": 1}
DIRECT = ("upper", "first",)
SHARE = {}
_ab, _c, _d = 0, 0, 0
for _name, (_lane, _size, _, _) in PIECES.items():
    _n = (_size - 512 * THIRD.get(_name, 0)) // 2
    SHARE[_name] = (_n, _ab, _c, _d)
    _ab, _c, _d = _ab + _n, _c + 128 * THIRD.get(_name, 0), _d + (_n if _name in DIRECT else 0)
EVEN = (0, 2, 4, 6)
D_LANES = _d
AB_LANES, C_LANES = _ab, _c


def dot(left, right, dims=((1,), (0,))):
    return lax.dot_general(left, right, (dims, ((), ())), preferred_element_type=F32)


def sigmoid(value):
    return 0.5 * jnp.tanh(0.5 * value) + 0.5


def real_rows(value):
    rows, lanes = value.shape
    tiles = value.reshape(rows // 8, 8, lanes)
    column = lax.broadcasted_iota(jnp.int32, tiles.shape, 1)
    return jnp.where(column != 7, tiles, 0.0).reshape(rows, lanes)


def fold_rows(value):
    rows, lanes = value.shape
    return jnp.sum(value.reshape(rows // 8, 8, lanes), axis=0)


def total(folded):
    return jnp.sum(folded, axis=0, keepdims=True)


def lanes_at(j, size=CH):
    return pl.ds(pl.multiple_of(j * size, size), size)


def band_at(r):
    return pl.ds(pl.multiple_of(r * BAND, BAND), BAND)


def block(
    x_hbm, cot_hbm, wr_hbm, ws_hbm, we_hbm, gain_ref, shift_ref,
    out_hbm, ing_hbm, wg_ref, norm_out,
    x, raw, wa, ws, pre1, taps, pre2, h2, pre3, up, g3, g2, back, turned, stage, rows,
    s1, s2, s3, s4, s5, s6, norm, own, other, ab1, ab2, ab3, ab4, straight, c1, c2, c3, c4, last, ny, nx,
    load_sem, send_sem, recv_sem, out_sem, core_send, core_recv,
    ab_send, ab_recv, c_send, c_recv, last_send, last_recv, norm_send, norm_recv, ready,
):
    b, rep = lax.axis_index("bngroup"), lax.axis_index("rep")
    z, c = b // 2, b % 2
    xx, yy = rep // 4, rep % 4

    def along(axis, k):
        if axis == "x":
            return {"rep": ((xx + k) % 4) * 4 + yy}
        if axis == "y":
            return {"rep": xx * 4 + (yy + k) % 4}
        return {"bngroup": (b + 2 * k) % GROUP}

    def load(i, src, dst):
        copy = pltpu.make_async_copy(src, dst, load_sem.at[i])
        copy.start()
        return copy

    def load_images(first, apart, images):
        return [load(first + apart * r, images.at[:, r], raw.at[r]) for r in range(SIDE)]

    def raw_rows(r, at):
        value = raw[r, :, :, at].astype(F32)
        value = jnp.concatenate([value, jnp.zeros((IMGS, 1, value.shape[2]), F32)], axis=1)
        return value.reshape(BAND, value.shape[2])

    load_x = load_images(6, 1, x_hbm)
    load_wr = load(1, wr_hbm, wa)

    barrier = pltpu.get_barrier_semaphore()
    for k in range(1, GROUP):
        pl.semaphore_signal(barrier, inc=1, device_id={"bngroup": (b + k) % GROUP}, device_id_type=MESH)
    for axis in "xy":
        for k in range(1, 4):
            pl.semaphore_signal(barrier, inc=1, device_id=along(axis, k), device_id_type=MESH)

    zeros = jnp.zeros((BAND, 3 * MID), BF16)
    taps[0:BAND, :] = zeros
    taps[ROWS + BAND :, :] = zeros
    g2[0:BAND, :] = zeros
    g2[ROWS + BAND :, :] = zeros

    partner = {"bngroup": b + 1 - 2 * c}

    def remote(src, dst, device, sems):
        return pltpu.make_async_remote_copy(
            src_ref=src, dst_ref=dst, send_sem=sems[0], recv_sem=sems[1],
            device_id=device, device_id_type=MESH,
        )

    def share(e, slots):
        sems = (send_sem.at[e], recv_sem.at[e])
        for k in range(1, GROUP):
            remote(slots.at[b], slots.at[b], {"bngroup": (b + k) % GROUP}, sems).start()
        return remote(slots.at[0 : GROUP - 1], slots.at[0 : GROUP - 1], partner, sems)

    CEN, AMP, SHI, INV, SS, GS = range(6)
    OFF = {1: 0, 2: MID, 3: 2 * MID}

    def put(row, off, value):
        rows[row, :, off : off + value.shape[1]] = value

    def get(row, which, j):
        return rows[row, :, pl.ds(pl.multiple_of(OFF[which] + j * CH, CH), CH)]

    def stats(value, j, slots, channels):
        about = total(value[0:8]) / 7.0
        off = real_rows(value - about)
        first, second = total(fold_rows(off)) / REAL, total(fold_rows(off * off))
        slots[b, :, lanes_at(j)] = about + first
        at = pl.ds(pl.multiple_of(channels + j * CH, CH), CH)
        slots[b, :, at] = jnp.maximum(second - REAL * (first * first), 0.0)

    def group_stats(slots, which, start=0, c=MID):
        off_at = OFF[which] + start
        mean = slots[0, :, 0:c]
        for i in range(1, GROUP):
            mean = mean + slots[i, :, 0:c]
        mean = mean / GROUP
        second = jnp.zeros((1, c), F32)
        for i in range(GROUP):
            off = slots[i, :, 0:c] - mean
            second = second + (slots[i, :, c : 2 * c] + REAL * (off * off))
        inverse = lax.rsqrt(second / COUNT + EPS)
        put(CEN, off_at, mean)
        put(INV, off_at, inverse)
        put(AMP, off_at, gain_ref[:, off_at : off_at + c] * inverse)
        put(SHI, off_at, shift_ref[:, off_at : off_at + c])

    def group_sums(slots, which, start=0, c=MID):
        off_at = OFF[which] + start
        sums = slots[0]
        for i in range(1, GROUP):
            sums = sums + slots[i]
        shift_sum, gain_sum = sums[:, 0:c], sums[:, c : 2 * c]
        inverse = rows[INV, :, off_at : off_at + c]
        norm[0:1, off_at : off_at + c] = gain_sum
        norm[1:2, off_at : off_at + c] = shift_sum
        put(SS, off_at, shift_sum / COUNT)
        put(GS, off_at, inverse * gain_sum / COUNT)

    for r in range(SIDE):
        load_x[r].wait()

        @pl.loop(0, WIDE // CH)
        def _(j, r=r):
            x[r * BAND : (r + 1) * BAND, lanes_at(j)] = raw_rows(r, lanes_at(j)).astype(BF16)

    load_wr.wait()
    load_ws = load(2, ws_hbm, ws)
    load_images(4, 0, cot_hbm)
    @pl.loop(0, MID // CH)
    def _(j):
        value = dot(x[...], wa[:, lanes_at(j)])
        pre1[:, lanes_at(j)] = value
        stats(value, j, s1, MID)

    load_we = load(3, we_hbm, wa)
    pl.semaphore_wait(barrier, GROUP - 1 + 6)
    share(0, s1).wait()
    group_stats(s1, 1)

    @pl.loop(0, MID // CH)
    def _(j):
        cen, amp, shi = get(CEN, 1, j), get(AMP, 1, j), get(SHI, 1, j)

        @pl.loop(0, SIDE)
        def _(r):
            normed = (pre1[band_at(r), lanes_at(j)] - cen) * amp + shi
            hidden = real_rows(normed * sigmoid(normed))
            tiles = hidden.reshape(IMGS, 8, CH)
            to = pl.ds(pl.multiple_of((r + 1) * BAND, BAND), BAND)
            for tap, shifted in enumerate((pltpu.roll(tiles, 1, 1), tiles, pltpu.roll(tiles, 7, 1))):
                at = pl.ds(pl.multiple_of(tap * MID + j * CH, CH), CH)
                taps[to, at] = shifted.reshape(BAND, CH).astype(BF16)

    load_ws.wait()

    @pl.loop(0, MID // CH)
    def _(j):
        acc = dot(taps[0:ROWS, :], ws[0 : 3 * MID, lanes_at(j)])
        acc = acc + dot(taps[BAND : ROWS + BAND, :], ws[3 * MID : 6 * MID, lanes_at(j)])
        acc = acc + dot(taps[2 * BAND :, :], ws[6 * MID :, lanes_at(j)])
        value = real_rows(acc)
        pre2[:, lanes_at(j)] = value
        stats(value, j, s2, MID)

    sums = share(1, s2)

    @pl.loop(0, 9)
    def _(tap):
        at = pl.ds(pl.multiple_of(tap * MID, MID), MID)
        ws[at, :] = ws[at, :].T

    sums.wait()
    group_stats(s2, 2)

    @pl.loop(0, MID // CH)
    def _(j):
        cen, amp, shi = get(CEN, 2, j), get(AMP, 2, j), get(SHI, 2, j)

        @pl.loop(0, SIDE)
        def _(r):
            normed = (pre2[band_at(r), lanes_at(j)] - cen) * amp + shi
            h2[band_at(r), lanes_at(j)] = real_rows(normed * sigmoid(normed)).astype(BF16)

    load_we.wait()

    exchanged = []
    for q in range(QUARTERS):

        @pl.loop(2 * q, 2 * q + 2)
        def _(j, q=q):
            value = dot(h2[...], wa[lanes_at(j), :], ((1,), (1,)))
            pre3[:, lanes_at(j)] = value
            stats(value, j - 2 * q, s3.at[q], MID)

        exchanged.append(share(6 + q, s3.at[q]))

    pltpu.make_async_copy(raw, raw, load_sem.at[4]).wait()

    written, sums = [], []
    for q in range(QUARTERS):
        exchanged[q].wait()
        group_stats(s3.at[q], 3, q * MID)

        @pl.loop(2 * q, 2 * q + 2)
        def _(j, q=q):
            at = lanes_at(j)
            cen, amp, shi, inv = get(CEN, 3, j), get(AMP, 3, j), get(SHI, 3, j), get(INV, 3, j)

            def add(r, acc):
                band = band_at(r)
                centred = pre3[band, at] - cen
                summed = centred * amp + shi + x[band, at].astype(F32)
                sigma = sigmoid(summed)
                value = summed * sigma
                upstream = raw_rows(r, at) * (sigma + value * (1.0 - sigma))
                g3[band, at] = value.astype(BF16)
                up[band, at] = upstream
                pre3[band, at] = centred
                return (acc[0] + fold_rows(upstream), acc[1] + fold_rows(upstream * centred))

            zero = jnp.zeros((8, CH), F32)
            shift_sum, gain_sum = lax.fori_loop(0, SIDE, add, (zero, zero))
            s4[q, b, :, lanes_at(j - 2 * q)] = total(shift_sum)
            s4[q, b, :, pl.ds(pl.multiple_of(MID + (j - 2 * q) * CH, CH), CH)] = total(gain_sum) * inv

        sums.append(share(6 + QUARTERS + q, s4.at[q]))
        at = pl.ds(q * MID, MID)
        copy = pltpu.make_async_copy(g3.at[:, at], out_hbm.at[:, at], out_sem.at[q])
        copy.start()
        written.append(copy)

    def turn(value):
        halves = value.T.reshape(16, 2, 16, ROWS)
        for half in range(2):
            turned[(half + c + 1) % 2] = halves[:, half].reshape(MID // 2, ROWS)

    def landing(piece, at):
        if piece in ("expand", "extra"):
            return pre3.at[0:256, at]
        if piece in ("upper", "first"):
            return pre3.at[256:512, at]
        return other.at[:, at]

    names = list(PIECES)

    def to_partner(piece, i):
        chunk = PIECES[piece][2]
        at = pl.ds(pl.multiple_of(LANDING[piece] + i * MID, MID), MID)
        slot = (chunk + i) % SLOTS
        sems = (core_send.at[slot], core_recv.at[names.index(piece)])
        return remote(stage.at[slot], landing(piece, at), partner, sems)

    def slot_free(n):
        remote(stage.at[n % SLOTS], other.at[:, 0:MID], partner, (core_send.at[n % SLOTS], core_recv.at[0])).wait_send()

    def weigh(piece, right):
        lane, size, chunk, count = PIECES[piece]

        @pl.loop(0, count)
        def _(i):
            slot = (chunk + i) % SLOTS
            if chunk >= SLOTS:
                slot_free(chunk + i - SLOTS)
            for half in range(MID // CH):
                product = dot(turned[...].reshape(MID, ROWS), right(i, half))
                stage[slot, :, half * CH : (half + 1) * CH] = product[: MID // 2]
                at = pl.ds(pl.multiple_of(lane + i * MID + half * CH, CH), CH)
                own[:, :, :, at] = product[MID // 2 :].reshape(4, 4, 16, CH)
            to_partner(piece, i).start()

    flying = {}

    def send(src, dst, device, sems):
        remote(src, dst, device, sems).start()

    def plus(k, base):
        return (base + k) % 4

    def step(piece, n):
        lane, size, chunk, count = PIECES[piece]
        width, ab_at, c_at, d_at = SHARE[piece]
        direct = piece in DIRECT
        p = names.index(piece)
        half = width // 2
        if n == 0:
            landed = landing(piece, pl.ds(LANDING[piece], size))
            remote(landed, landed, partner, (core_send.at[0], core_recv.at[p])).wait_recv()

            @pl.loop(0, 16)
            def _(k):
                own[k // 4, k % 4, :, lane : lane + size] += landed[pl.ds(pl.multiple_of(k * 16, 16), 16), :]

        else:
            flying.pop((piece, n - 1)).wait()
        if n < 4:
            sems = (ab_send.at[p], ab_recv.at[p, n])
        for color in range(2):
            span = pl.ds(lane + color * width, width)
            local = pl.ds(ab_at, width)
            axes = "xy" if color == 0 else "yx"
            outer, inner = (xx, yy) if color == 0 else (yy, xx)
            parts = [pl.ds(lane + color * width + k * half, half) for k in range(2)]
            local_part = pl.ds(ab_at // 2, half)

            def outer_block(index, part=slice(None), color=color, span=span):
                return own.at[index, part, :, span] if color == 0 else own.at[part, index, :, span]

            def inner_block(index, part, color=color, outer=outer):
                return own.at[outer, index, :, part] if color == 0 else own.at[index, outer, :, part]

            if n == 0:
                far = plus(2, outer)
                send(outer_block(far, slice(0, 2)), ab1.at[color, 0, :, :, local], along(axes[0], 1), sems)
                send(outer_block(far, slice(2, 4)), ab1.at[color, 1, :, :, local], along(axes[0], 3), sems)
            elif n == 1:
                low = outer_block(plus(1, outer), slice(0, 2))
                low[...] += ab1[color, 0, :, :, local]
                high = outer_block(plus(3, outer), slice(2, 4))
                high[...] += ab1[color, 1, :, :, local]
                send(outer_block(plus(1, outer)), ab2.at[color, 0, :, :, local], along(axes[0], 1), sems)
                send(outer_block(plus(3, outer)), ab2.at[color, 1, :, :, local], along(axes[0], 3), sems)
            elif n == 2:
                mine = outer_block(outer)
                mine[...] += ab2[color, 0, :, :, local] + ab2[color, 1, :, :, local]
                if direct:
                    for k in range(1, 4):
                        send(inner_block(plus(k, inner), span), straight.at[color, k - 1, :, pl.ds(d_at, width)], along(axes[1], k), sems)
                    continue
                far = plus(2, inner)
                send(inner_block(far, parts[0]), ab3.at[color, 0, :, local_part], along(axes[1], 1), sems)
                send(inner_block(far, parts[1]), ab3.at[color, 1, :, local_part], along(axes[1], 3), sems)
            elif direct:
                if n == 3:
                    at = pl.ds(d_at, width)
                    mine = inner_block(inner, span)
                    mine[...] += straight[color, 0, :, at] + straight[color, 1, :, at] + straight[color, 2, :, at]
            elif n == 3:
                low = inner_block(plus(1, inner), parts[0])
                low[...] += ab3[color, 0, :, local_part]
                high = inner_block(plus(3, inner), parts[1])
                high[...] += ab3[color, 1, :, local_part]
                send(inner_block(plus(1, inner), span), ab4.at[color, 0, :, local], along(axes[1], 1), sems)
                send(inner_block(plus(3, inner), span), ab4.at[color, 1, :, local], along(axes[1], 3), sems)
            else:
                mine = inner_block(inner, span)
                mine[...] += ab4[color, 0, :, local] + ab4[color, 1, :, local]
        if n < (3 if direct else 4):
            if direct and n == 2:
                ab = straight.at[:, :, :, pl.ds(d_at, width)]
            elif n == 2:
                ab = ab3.at[:, :, :, pl.ds(ab_at // 2, half)]
            elif n == 3:
                ab = ab4.at[:, :, :, pl.ds(ab_at, width)]
            else:
                ab = (ab1, ab2)[n].at[:, :, :, :, pl.ds(ab_at, width)]
            flying[piece, n] = remote(ab, ab, partner, sems)

    def third_step(piece, n):
        lane = PIECES[piece][0]
        width, _, c_at, _ = SHARE[piece]
        p = names.index(piece)
        base = lane + 2 * width
        tiles = 128 * THIRD[piece]
        local = pl.ds(c_at, tiles)
        if n > 0:
            flying.pop((piece, n - 1, "third")).wait()
        if n < 4:
            sems = (c_send.at[p], c_recv.at[p, n])

        def tile(index):
            return pl.ds(pl.multiple_of(base + tiles * index, 128), tiles)

        first_axis = "x" if p in EVEN else "y"
        second_axis = "y" if p in EVEN else "x"
        if n == 0:
            far = tile(plus(2, z))
            send(own.at[0:2, :, :, far], c1.at[0, :, :, :, local], along("z", 1), sems)
            send(own.at[2:4, :, :, far], c1.at[1, :, :, :, local], along("z", 3), sems)
        elif n == 1:
            up_one, down_one = tile(plus(1, z)), tile(plus(3, z))
            own[0:2, :, :, up_one] += c1[0, :, :, :, local]
            own[2:4, :, :, down_one] += c1[1, :, :, :, local]
            send(own.at[:, :, :, up_one], c2.at[0, :, :, :, local], along("z", 1), sems)
            send(own.at[:, :, :, down_one], c2.at[1, :, :, :, local], along("z", 3), sems)
        elif n == 2:
            own[:, :, :, tile(z)] += c2[0, :, :, :, local] + c2[1, :, :, :, local]
            for k in range(1, 4):
                block_of = own.at[plus(k, xx), :, :, tile(z)] if p in EVEN else own.at[:, plus(k, yy), :, tile(z)]
                send(block_of, c3.at[k - 1, :, :, local], along(first_axis, k), sems)
        elif n == 3:
            mine = own.at[xx, :, :, tile(z)] if p in EVEN else own.at[:, yy, :, tile(z)]
            mine[...] += c3[0, :, :, local] + c3[1, :, :, local] + c3[2, :, :, local]
            for k in range(1, 4):
                block_of = own.at[xx, plus(k, yy), :, tile(z)] if p in EVEN else own.at[plus(k, xx), yy, :, tile(z)]
                send(block_of, c4.at[k - 1, :, local], along(second_axis, k), sems)
        else:
            mine = own[xx, yy, :, tile(z)] + c4[0, :, local] + c4[1, :, local] + c4[2, :, local]
            own[xx, yy, :, base : base + 4 * tiles] = jnp.zeros((16, 4 * tiles), F32)
            own[xx, yy, :, tile(z)] = mine
        if n < 4:
            whole = (c1, c2, c3, c4)[n]
            whole = whole.at[:, :, :, :, local] if n < 2 else whole.at[:, :, :, local] if n == 2 else whole.at[:, :, local]
            flying[piece, n, "third"] = remote(whole, whole, partner, sems)

    def owned(device):
        return pl.ds(pl.multiple_of((device // 2) * ZBLOCK + (device % 2) * 1024, 128), OWN)

    last_sems = (last_send.at[0], last_recv.at[0])

    def to_owner(t):
        return remote(own.at[xx, yy, :, owned(t)], last.at[b], {"bngroup": t}, last_sems)

    def to_owners(targets):
        for t in targets:

            @pl.when(b != t)
            def _(t=t):
                to_owner(t).start()

    def gather(n, axis, slots, mine):
        sems = (norm_send.at[n], norm_recv.at[n])
        for k in range(1, 4):
            send(slots.at[mine], slots.at[mine], along(axis, k), sems)
        return remote(slots.at[0:3], slots.at[0:3], partner, sems)

    def sum_of(slots):
        return slots[0] + slots[1] + slots[2] + slots[3]

    def grad_three(q):
        sums[q].wait()
        group_sums(s4.at[q], 3, q * MID)
        written[q].wait()

        @pl.loop(2 * q, 2 * q + 2)
        def _(j):
            at = lanes_at(j)
            amp, ss, gs = get(AMP, 3, j), get(SS, 3, j), get(GS, 3, j)

            @pl.loop(0, SIDE)
            def _(r):
                band = band_at(r)
                grad = amp * (up[band, at] - ss - pre3[band, at] * gs)
                g3[band, at] = real_rows(grad).astype(BF16)

    def tell_partner():
        pl.semaphore_signal(ready, inc=1, device_id=partner, device_id_type=MESH)

    def slope_sums(pre, which, j, slots):
        at = lanes_at(j)
        cen, amp, shi, inv = get(CEN, which, j), get(AMP, which, j), get(SHI, which, j), get(INV, which, j)

        def add(r, acc):
            band = band_at(r)
            centred = pre[band, at] - cen
            normed = centred * amp + shi
            sigma = sigmoid(normed)
            value = real_rows(back[band, at] * (sigma * (1.0 + normed * (1.0 - sigma))))
            back[band, at] = value
            return (acc[0] + fold_rows(value), acc[1] + fold_rows(value * centred))

        zero = jnp.zeros((8, CH), F32)
        shift_sum, gain_sum = lax.fori_loop(0, SIDE, add, (zero, zero))
        slots[b, :, at] = total(shift_sum)
        slots[b, :, pl.ds(pl.multiple_of(MID + j * CH, CH), CH)] = total(gain_sum) * inv

    def norm_back(pre, which, j, r):
        at, band = lanes_at(j), band_at(r)
        cen, amp, ss, gs = get(CEN, which, j), get(AMP, which, j), get(SS, which, j), get(GS, which, j)
        return real_rows(amp * (back[band, at] - ss - (pre[band, at] - cen) * gs))

    turn(h2[...])
    grad_three(0)
    grad_three(1)
    tell_partner()
    pl.semaphore_wait(ready, 1)
    weigh("expand", lambda i, half: g3[:, pl.ds(pl.multiple_of(i * MID + half * CH, CH), CH)])
    grad_three(2)
    grad_three(3)
    tell_partner()
    @pl.loop(0, MID // CH)
    def _(j):
        back[:, lanes_at(j)] = dot(g3[...], wa[:, lanes_at(j)])
        slope_sums(pre2, 2, j, s5)

    load_wr = load(5, wr_hbm, wa)

    sums = share(4, s5)
    pl.semaphore_wait(ready, 1)
    weigh("extra", lambda i, half: g3[:, pl.ds(pl.multiple_of(1024 + i * MID + half * CH, CH), CH)])
    step("expand", 0)
    third_step("expand", 0)
    step("extra", 0)
    sums.wait()
    group_sums(s5, 2)
    @pl.loop(0, MID // CH)
    def _(j):
        @pl.loop(0, SIDE)
        def _(r):
            grad = norm_back(pre2, 2, j, r)
            tiles = grad.reshape(IMGS, 8, CH)
            to = pl.ds(pl.multiple_of((r + 1) * BAND, BAND), BAND)
            for tap, shifted in enumerate((pltpu.roll(tiles, 7, 1), tiles, pltpu.roll(tiles, 1, 1))):
                at = pl.ds(pl.multiple_of(tap * MID + j * CH, CH), CH)
                g2[to, at] = shifted.reshape(BAND, CH).astype(BF16)

    def tap_row(row):
        return lambda i, half: taps[
            row * BAND : row * BAND + ROWS,
            pl.ds(pl.multiple_of(i * MID + half * CH, CH), CH),
        ]

    def back_one(j):
        acc = None
        for row in range(3):
            left = g2[(2 - row) * BAND : (2 - row) * BAND + ROWS, :]
            part = dot(left, ws[3 * MID * row : 3 * MID * (row + 1), j * CH : (j + 1) * CH])
            acc = part if acc is None else acc + part
        back[:, j * CH : (j + 1) * CH] = acc
        slope_sums(pre1, 1, j, s6)

    def input_gradient(quarter):
        @pl.loop(2 * quarter, 2 * quarter + 2)
        def _(j):
            at = lanes_at(j)
            g3[:, at] = (up[:, at] + dot(h2[...], wa[at, :], ((1,), (1,)))).astype(BF16)

    turn(g2[BAND : ROWS + BAND, MID : 2 * MID])
    weigh("low", tap_row(0))
    step("expand", 1)
    weigh("mid", tap_row(1))
    step("low", 0)
    third_step("low", 0)
    step("extra", 1)
    weigh("high", tap_row(2))
    third_step("expand", 1)
    step("mid", 0)
    step("expand", 2)
    back_one(0)
    step("low", 1)
    third_step("mid", 0)
    third_step("low", 1)
    step("high", 0)
    back_one(1)
    step("expand", 3)
    sums = share(5, s6)
    third_step("expand", 2)
    third_step("high", 0)
    step("mid", 1)
    third_step("mid", 1)
    step("high", 1)
    step("extra", 2)
    step("low", 2)
    sums.wait()
    group_sums(s6, 1)
    ny[yy] = norm[...]
    norm_copies = gather(0, "y", ny, yy)

    @pl.loop(0, MID // CH)
    def _(j):
        @pl.loop(0, SIDE)
        def _(r):
            h2[band_at(r), lanes_at(j)] = norm_back(pre1, 1, j, r).astype(BF16)

    third_step("high", 1)
    turn(h2[...])
    weigh("upper", lambda i, half: x[:, pl.ds(pl.multiple_of(1024 + i * MID + half * CH, CH), CH)])
    third_step("expand", 3)
    weigh("first", lambda i, half: x[:, pl.ds(pl.multiple_of(i * MID + half * CH, CH), CH)])
    third_step("low", 2)
    third_step("mid", 2)
    step("upper", 0)
    third_step("upper", 0)
    step("first", 0)
    norm_copies.wait()
    nx[xx] = sum_of(ny)
    norm_copies = gather(1, "x", nx, xx)
    step("mid", 2)
    third_step("first", 0)
    step("extra", 3)
    step("low", 3)
    third_step("expand", 4)
    step("high", 2)
    third_step("upper", 1)
    step("expand", 4)
    third_step("low", 3)
    third_step("high", 2)
    third_step("mid", 3)
    third_step("first", 1)
    step("upper", 1)
    step("mid", 3)
    load_wr.wait()
    input_gradient(0)
    step("first", 1)
    third_step("upper", 2)
    step("high", 3)
    input_gradient(1)
    step("low", 4)
    third_step("high", 3)
    third_step("first", 2)
    third_step("mid", 4)
    step("mid", 4)
    third_step("low", 4)
    to_owners(range(2, 4))
    input_gradient(2)
    step("upper", 2)
    step("extra", 4)
    third_step("upper", 3)
    step("high", 4)
    third_step("high", 4)
    step("first", 2)
    to_owners(range(4, GROUP))
    third_step("first", 3)
    step("upper", 3)
    third_step("upper", 4)
    to_owners(range(1, 2))
    step("first", 3)
    third_step("first", 4)
    to_owners(range(1))
    input_gradient(3)
    write_in = pltpu.make_async_copy(g3, ing_hbm, out_sem.at[QUARTERS])
    write_in.start()
    last[b] = own[xx, yy, :, owned(b)]

    norm_copies.wait()
    norm_out[...] = sum_of(nx) * (1.0 / IMAGES)
    write_in.wait()
    for n in range(13, 17):
        slot_free(n)
    remote(last.at[0 : GROUP - 1], last.at[0 : GROUP - 1], partner, last_sems).wait()

    parts = []
    for core in range(2):
        parts.append(last[core] + last[2 + core] + last[4 + core] + last[6 + core])
    whole = jnp.concatenate(parts, axis=0) * (1.0 / IMAGES)
    moved = pltpu.roll(whole, OWN - 64, 1)
    wg_ref[...] = jnp.where(c == 1, moved, whole)[:, : LANES // 8]


def run_block(x, cot, wr, ws, we, gain, shift):
    any_ = pl.BlockSpec(memory_space=pl.ANY)
    vmem = pl.BlockSpec(memory_space=pltpu.VMEM)
    v = pltpu.VMEM
    dma = pltpu.SemaphoreType.DMA
    pieces = len(PIECES)
    return pl.pallas_call(
        block,
        out_shape=(
            jax.ShapeDtypeStruct((ROWS, WIDE), BF16),
            jax.ShapeDtypeStruct((ROWS, WIDE), BF16),
            jax.ShapeDtypeStruct((32, LANES // 8), F32),
            jax.ShapeDtypeStruct((2, 3072), F32),
        ),
        in_specs=[any_] * 5 + [vmem] * 2,
        out_specs=(any_, any_, vmem, vmem),
        scratch_shapes=[
            v((ROWS, WIDE), BF16),
            v((SIDE, IMGS, SIDE, WIDE), BF16),
            v((WIDE, MID), BF16),
            v((9 * MID, MID), BF16),
            v((ROWS, MID), F32),
            v((ROWS + 2 * BAND, 3 * MID), BF16),
            v((ROWS, MID), F32),
            v((ROWS, MID), BF16),
            v((ROWS, WIDE), F32),
            v((ROWS, WIDE), F32),
            v((ROWS, WIDE), BF16),
            v((ROWS + 2 * BAND, 3 * MID), BF16),
            v((ROWS, MID), F32),
            v((2, MID // 2, ROWS), BF16),
            v((SLOTS, MID // 2, MID), F32),
            v((6, 1, 3072), F32),
            v((GROUP, 1, 2 * MID), F32),
            v((GROUP, 1, 2 * MID), F32),
            v((QUARTERS, GROUP, 1, 2 * MID), F32),
            v((QUARTERS, GROUP, 1, 2 * MID), F32),
            v((GROUP, 1, 2 * MID), F32),
            v((GROUP, 1, 2 * MID), F32),
            v((2, 3072), F32),
            v((4, 4, 16, LANES), F32),
            v((MID // 2, 9 * MID), F32),
            v((2, 2, 2, 16, AB_LANES), F32),
            v((2, 2, 4, 16, AB_LANES), F32),
            v((2, 2, 16, AB_LANES // 2), F32),
            v((2, 2, 16, AB_LANES), F32),
            v((2, 3, 16, D_LANES), F32),
            v((2, 2, 4, 16, C_LANES), F32),
            v((2, 4, 4, 16, C_LANES), F32),
            v((3, 4, 16, C_LANES), F32),
            v((3, 16, C_LANES), F32),
            v((GROUP, 16, OWN), F32),
            v((4, 2, 3072), F32),
            v((4, 2, 3072), F32),
            dma((6 + SIDE,)),
            dma((6 + 2 * QUARTERS,)),
            dma((6 + 2 * QUARTERS,)),
            dma((QUARTERS + 1,)),
            dma((SLOTS,)),
            dma((pieces,)),
            dma((pieces,)),
            dma((pieces, 4)),
            dma((pieces,)),
            dma((pieces, 4)),
            dma((1,)),
            dma((1,)),
            dma((2,)),
            dma((2,)),
            pltpu.SemaphoreType.REGULAR,
        ],
        compiler_params=pltpu.CompilerParams(
            collective_id=0, has_side_effects=True, vmem_limit_bytes=VMEM_LIMIT
        ),
        cost_estimate=pl.CostEstimate(flops=18 * 10**9, bytes_accessed=4 * 10**7, transcendentals=10**7),
        name="block",
    )(x, cot, wr, ws, we, gain, shift)


def from_rows(rows):
    return rows.reshape(SIDE, IMGS, COLS, WIDE)[:, :, :SIDE].transpose(1, 0, 2, 3)


def per_device(images, cotangent, w_reduce, w_spatial, w_expand, norm_gain, norm_shift):
    output, in_grad, grads, norm_grads = run_block(
        images, cotangent, w_reduce, w_spatial, w_expand,
        norm_gain.reshape(1, -1), norm_shift.reshape(1, -1),
    )
    return (from_rows(output), from_rows(in_grad), grads.T, norm_grads)


def solution(mesh):
    both = P(("bngroup", "rep"), None, None, None)
    return jax.shard_map(
        per_device,
        mesh=mesh,
        in_specs=(both, both, P(), P(), P(), P(), P()),
        out_specs=(both, both, P("bngroup", "rep"), P()),
        check_vma=False,
    )
```
